32 devices in a mesh: range: 8 (over z, y), depth: 4 (over x, core).
Axes of the slice: x: 2, y: 2, z: 4, core: 2. Of those that a mesh axis runs over, the one named last changes fastest.
Arguments:
- pressure: float32 [4096, 1024], P('depth', 'range'), may hold values from -6 to 6
- vel_range: float32 [4096, 1024], P('depth', 'range'), may hold values from -3 to 3
- vel_depth: float32 [4096, 1024], P('depth', 'range'), may hold values from -3 to 3
- sound_speed: float32 [4096, 1024], P('depth', 'range'), may hold values from 0.5 to 1.1
- density: float32 [4096, 1024], P('depth', 'range'), may hold values from 1 to 3
- ahead_speed: float32 [4096, 64], P('depth'), may hold values from 0.5 to 1.1
- ahead_density: float32 [4096, 64], P('depth'), may hold values from 1 to 3
- shifts: int32 [4], replicated, may hold values from 1 to 16, as said below
- sources: int32 [8, 2], replicated, may hold values from 0 to 4095, as said below
- wavelet: float32 [8, 4], replicated, may hold values from -12 to 12
Outputs:
- pressure_out: float32 [4096, 1024], P('depth', 'range')
- range_out: float32 [4096, 1024], P('depth', 'range')
- depth_out: float32 [4096, 1024], P('depth', 'range')
The draws below stay inside these ranges and needn't reach their ends.
Inputs may be any that keep to these rules, and one draw needn't show every extreme that they name: `shifts`: every draw has a step that advances by exactly 16 columns. `sources`: column 0 is a depth index below 4096, column 1 a range index below 1024.
All inputs are finite; a program needn't handle non-finite values.
Results may differ from the reference program's by a relative error of at most 0.0003.
Values sent between devices are 32-bit elements; how exact they have to be, the bound alone decides.
No kernel may reach another device: no remote copies, remote signals or barrier semaphores. Data moves between devices by JAX's collectives and lax.ppermute only.
A program may use at most 64 MiB of HBM per device.

```python
import math
import jax
import jax.numpy as jnp
from jax import lax

SMAX = 16
ITERS = 4
NSRC = 8
NZ = 4096
NR = 1024
AHEAD = 64


def draw_shifts(key, part):
    first, second = jax.random.split(jax.random.fold_in(key, 11))
    base = jax.random.randint(first, (ITERS,), 1, SMAX + 1)
    chosen = jax.random.randint(second, (), 0, ITERS)
    return jnp.where(jnp.arange(ITERS) == chosen, SMAX, base).astype(jnp.int32)


def draw_sources(key, part):
    first, second, third = jax.random.split(jax.random.fold_in(key, 23), 3)
    depth_index = jax.random.randint(first, (NSRC,), 0, NZ)
    range_index = jax.random.randint(second, (NSRC,), 0, NR)
    order = jax.random.permutation(third, NSRC)
    slots = jnp.arange(NSRC, dtype=jnp.int32)
    depth_index = jnp.where(slots == order[0], NZ - 1, depth_index)
    depth_index = jnp.where(slots == order[2], 0, depth_index)
    range_index = jnp.where(slots == order[1], NR - 1, range_index)
    return jnp.stack([depth_index, range_index], 1).astype(jnp.int32)


def level_of(own_key, dims, cuts, smallest, top_value):
    factor_of = 1.0
    for dim, blocks in cuts:
        draws = jax.random.uniform(jax.random.fold_in(jax.random.fold_in(own_key, 6), dim), (blocks,), jnp.float32, smallest / len(cuts), top_value / len(cuts))
        factor_of = factor_of * jnp.repeat(jnp.exp(draws), dims[dim] // blocks).reshape((-1,) + (1,) * (len(dims) - 1 - dim))
    return factor_of


def bell_draw(rng, shape, width, reach, cuts=(), kind=jnp.bfloat16):
    loudness = level_of(rng, shape, cuts, -0.22, 0.18) if cuts else 1.0
    entries = jax.random.normal(rng, shape, jnp.float32) * width * loudness
    return jnp.minimum(jnp.maximum(entries, -reach), reach).astype(kind)


def setup_inputs(seed: int = 0) -> dict:
    seeds = jax.random.split(jax.random.key(seed), 11)
    return {
        "pressure": bell_draw(seeds[0], (NZ, NR), 1.0, 6.0, ((0, 4), (1, 8)), jnp.float32),
        "vel_range": bell_draw(seeds[1], (NZ, NR), 0.5, 3.0, ((0, 4), (1, 8)), jnp.float32),
        "vel_depth": bell_draw(seeds[2], (NZ, NR), 0.5, 3.0, ((0, 4), (1, 8)), jnp.float32),
        "sound_speed": jnp.clip(0.5 + 0.6 * jax.random.uniform(seeds[3], (NZ, NR), jnp.float32) ** level_of(seeds[3], (NZ, NR), ((0, 4), (1, 8)), -0.2, 0.2), 0.5, 1.1),
        "density": jnp.clip(jnp.exp(math.log(3.0) - 1.0986123 * jax.random.uniform(seeds[4], (NZ, NR), jnp.float32) ** level_of(seeds[4], (NZ, NR), ((0, 4), (1, 8)), -0.2, 0.2)), 1.0, 3.0),
        "ahead_speed": jnp.clip(0.5 + 0.6 * jax.random.uniform(seeds[5], (NZ, AHEAD), jnp.float32) ** level_of(seeds[5], (NZ, AHEAD), ((0, 4),), -0.2, 0.2), 0.5, 1.1),
        "ahead_density": jnp.clip(jnp.exp(math.log(3.0) - 1.0986123 * jax.random.uniform(seeds[6], (NZ, AHEAD), jnp.float32) ** level_of(seeds[6], (NZ, AHEAD), ((0, 4),), -0.2, 0.2)), 1.0, 3.0),
        "shifts": draw_shifts(jax.random.fold_in(seeds[10], 71), 0),
        "sources": draw_sources(jax.random.fold_in(seeds[10], 71), 0),
        "wavelet": bell_draw(seeds[9], (NSRC, ITERS), 3.0, 12.0, (), jnp.float32),
    }


TIME_STEP = 0.6


def reference(pressure, vel_range, vel_depth, sound_speed, density, ahead_speed, ahead_density, shifts, sources, wavelet):
    offset = jnp.int32(0)
    for segment in range(ITERS):
        p_right = jnp.concatenate([pressure[:, 1:], jnp.zeros_like(pressure[:, :1])], 1)
        rho_right = jnp.concatenate([density[:, 1:], density[:, -1:]], 1)
        vel_range = vel_range - TIME_STEP * (2.0 / (density + rho_right)) * (p_right - pressure)
        p_lower = jnp.concatenate([pressure[1:], jnp.zeros_like(pressure[:1])], 0)
        rho_lower = jnp.concatenate([density[1:], density[-1:]], 0)
        vel_depth = vel_depth - TIME_STEP * (2.0 / (density + rho_lower)) * (p_lower - pressure)
        range_left = jnp.concatenate([jnp.zeros_like(vel_range[:, :1]), vel_range[:, :-1]], 1)
        depth_upper = jnp.concatenate([jnp.zeros_like(vel_depth[:1]), vel_depth[:-1]], 0)
        stiffness = density * sound_speed * sound_speed
        pressure = pressure - TIME_STEP * stiffness * ((vel_range - range_left) + (vel_depth - depth_upper))
        amplitude = wavelet[:, segment]
        depth_onehot = (sources[:, 0][:, None] == jnp.arange(NZ, dtype=jnp.int32)[None, :]).astype(pressure.dtype)
        range_onehot = ((sources[:, 1] - offset)[:, None] == jnp.arange(NR, dtype=jnp.int32)[None, :]).astype(pressure.dtype)
        pressure = pressure + jnp.dot((depth_onehot * amplitude[:, None]).T, range_onehot, precision=lax.Precision.HIGHEST)
        advance_by = shifts[segment].astype(jnp.int32)
        zero_strip = jnp.zeros((NZ, SMAX), pressure.dtype)
        new_speed = lax.dynamic_slice_in_dim(ahead_speed, offset, SMAX, 1)
        new_density = lax.dynamic_slice_in_dim(ahead_density, offset, SMAX, 1)

        def advance(values, incoming):
            return lax.dynamic_slice_in_dim(jnp.concatenate([values, incoming], 1), advance_by, NR, 1)

        pressure = advance(pressure, zero_strip)
        vel_range = advance(vel_range, zero_strip)
        vel_depth = advance(vel_depth, zero_strip)
        sound_speed = advance(sound_speed, new_speed)
        density = advance(density, new_density)
        offset = offset + advance_by
    return pressure, vel_range, vel_depth
```

```python
import functools

import jax
import jax.numpy as jnp
from jax import lax
from jax.experimental import pallas as pl
from jax.experimental.pallas import tpu as pltpu
from jax.sharding import PartitionSpec as P

ITERS = 4
TIME_STEP = 0.6
LANES = 128
TILE = 8
MARGIN = 16
SKEW = 4
WIDTH = 42
GROUPS = 6
BLOCK = 64

FAR = 1 << 20


def lane_ids(rows):
    return lax.broadcasted_iota(jnp.int32, (rows, LANES), 1)


def between(lanes, low, high):
    return jnp.logical_and(lanes >= low, lanes < high)


def roll(x, by):
    return pltpu.roll(x, by % LANES, 1)


def for_rows(start, stop, fn, size=BLOCK):
    whole = (stop - start) // size

    def step(i, carry):
        fn(pl.multiple_of(start + i * size, TILE), size)
        return carry

    if whole > 1:
        lax.fori_loop(0, whole, step, 0)
    elif whole == 1:
        fn(start, size)
    if start + whole * size < stop:
        fn(start + whole * size, stop - start - whole * size)


def offsets_of(shifts):
    found = [jnp.int32(0)]
    for t in range(ITERS):
        found.append(found[-1] + shifts[t])
    return found


def set_coefs(n, c, rho, ax, az, stiff):
    def coefs(r, k):
        here = pl.ds(r, k)
        dense, speed = rho[here, :], c[here, :]
        ax[here, :] = (2.0 * TIME_STEP) / (dense + roll(dense, -1))
        az[here, :] = (2.0 * TIME_STEP) / (dense + rho[pl.ds(r + 1, k), :])
        stiff[here, :] = TIME_STEP * (dense * speed * speed)

    for_rows(0, n - TILE, coefs)


def inject(field, sources, wavelet, t, local_row, first_col, last_lane):
    rows = lax.broadcasted_iota(jnp.int32, (TILE, LANES), 0)
    lanes = lane_ids(TILE)
    for k in range(sources.shape[0]):
        row, inside = local_row(sources[k, 0])
        lane = sources[k, 1] - first_col
        good = jnp.logical_and(inside, jnp.logical_and(lane >= 0, lane <= last_lane))
        row = jnp.where(good, row, 0)
        amount = jnp.where(good, wavelet[k, t], 0.0)
        at = pl.ds(pl.multiple_of((row // TILE) * TILE, TILE), TILE)
        here = jnp.logical_and(rows == row % TILE, lanes == lane)
        field[at, :] = field[at, :] + jnp.where(here, amount, 0.0)


def left_steps(n, fields, coefs, stages, shifts, sources, wavelet, local_row):
    ax, az, stiff = coefs
    ps, us, ws = stages
    offsets = offsets_of(shifts)
    place = lax.axis_index("range")
    for t in range(ITERS):
        p, u, w = fields if t == 0 else (ps.at[t - 1], us.at[t - 1], ws.at[t - 1])
        u_new, w_new, p_new = us.at[t], ws.at[t], ps.at[t]
        wall = jnp.where(place == 0, offsets[t], -1)

        def speeds(r, k):
            here = pl.ds(r, k)
            now = p[here, :]
            u_new[here, :] = u[here, :] - ax[here, :] * (roll(now, -1) - now)
            w_new[here, :] = w[here, :] - az[here, :] * (p[pl.ds(r + 1, k), :] - now)

        def press(r, k):
            here = pl.ds(r, k)
            fast = u_new[here, :]
            left = jnp.where(lane_ids(k) == wall, 0.0, roll(fast, 1))
            down = w_new[here, :] - w_new[pl.ds(r - 1, k), :]
            p_new[here, :] = p[here, :] - stiff[here, :] * ((fast - left) + down)

        for_rows(0, n - TILE, speeds)
        for_rows(TILE, n - TILE, press)
        inject(p_new, sources, wavelet, t, local_row, place * LANES, LANES - 1)


def slanted(r, k, p0, stages, stiff, rho):
    ps, us, ws = stages
    here = pl.ds(r, k)
    lanes = lane_ids(k)

    def pick(parts):
        found = parts[-1]
        for t in range(len(parts) - 2, -1, -1):
            found = jnp.where(lanes <= t, parts[t], found)
        return found

    a = pick([p0[here, :]] + [ps[t, here, :] for t in range(ITERS - 1)])
    b = pick([us[t, here, :] for t in range(ITERS)])
    c = pick([ws[t, here, :] for t in range(ITERS)])
    found = roll(rho[here, :], 4 * SKEW)
    found = jnp.where(lanes < 4 * SKEW, roll(stiff[here, :], 3 * SKEW), found)
    found = jnp.where(lanes < 3 * SKEW, roll(c, 2 * SKEW), found)
    found = jnp.where(lanes < 2 * SKEW, roll(b, SKEW), found)
    return jnp.where(lanes < SKEW, a, found)


def packed(p, u, w):
    lanes = lane_ids(p.shape[0])
    found = jnp.where(
        between(lanes, SKEW, SKEW + 2 * WIDTH), roll(u, WIDTH), roll(w, 2 * WIDTH)
    )
    return jnp.where(between(lanes, SKEW, SKEW + WIDTH), p, found)


def finals(stages, here):
    return [stage[ITERS - 1, here, :] for stage in stages]


def first_kernel(n, height, *refs):
    shifts, sources, wavelet, p, u, w, c, rho = refs[:8]
    lows = refs[8:13]
    ahead, low_ahead = refs[13:15], refs[15:17]
    plane, done, slant, to_up, to_down = refs[17:22]
    ax, az, stiff = refs[22:25]
    stages = refs[25:]
    for k, (top, low) in enumerate(zip((p, u, w, c, rho), lows)):
        to_up[pl.ds(k * TILE, TILE), :] = top[pl.ds(0, TILE), :]
        to_down[pl.ds(k * TILE, TILE), :] = low[...]
    to_up[pl.ds(5 * TILE, TILE), :] = jnp.concatenate([ref[...] for ref in ahead], 1)
    to_down[pl.ds(5 * TILE, TILE), :] = jnp.concatenate([ref[...] for ref in low_ahead], 1)
    set_coefs(n, c, rho, ax, az, stiff)
    base = lax.axis_index("depth") * height

    def local_row(row):
        row = row - base
        return row, jnp.logical_and(row >= 0, row < n)

    left_steps(n, (p, u, w), (ax, az, stiff), stages, shifts, sources, wavelet, local_row)

    def finish(r, k):
        fields = finals(stages, pl.ds(r, k))
        there = pl.ds(r - MARGIN, k)
        plane[there, :] = packed(*fields)
        for f in range(3):
            done[f, there, :] = fields[f]
        slant[there, :] = slanted(r, k, p, stages, stiff, rho)

    for_rows(MARGIN, n - MARGIN, finish)


def ghost_rows(up, down, k, last_own):
    place = lax.axis_index("depth")
    at = pl.ds(k * TILE, TILE)
    above, below = up[at, :], down[at, :]
    if k == 4:
        above = jnp.where(place == 0, 1.0, above)
        below = jnp.where(place == lax.axis_size("depth") - 1, last_own, below)
    return above, below


def second_kernel(n, height, n_first, *refs):
    shifts, sources, wavelet = refs[:3]
    tops, lows = refs[3:8], refs[8:13]
    up, down, first_slant = refs[13:16]
    plane, done, slant = refs[16:19]
    ax, az, stiff = refs[19:22]
    stages, inner, full = refs[22:25], refs[25:30], refs[30]
    head = 3 * MARGIN
    split = n_first - 2 * MARGIN
    for k in range(5):
        filler = jnp.full((TILE, LANES), 1.0 if k == 4 else 0.0, jnp.float32)
        last_own = jnp.broadcast_to(lows[k][pl.ds(height - split - 1, 1), :], (TILE, LANES))
        above, below = ghost_rows(up, down, k, last_own)
        inner[k][pl.ds(0, TILE), :] = filler
        inner[k][pl.ds(TILE, TILE), :] = above
        inner[k][pl.ds(2 * TILE, 2 * MARGIN), :] = tops[k][...]

        def bring(r, rows, k=k):
            inner[k][pl.ds(r + head, rows), :] = lows[k][pl.ds(r, rows), :]

        for_rows(0, height - split, bring)
        inner[k][pl.ds(n - 2 * TILE, TILE), :] = below
        inner[k][pl.ds(n - TILE, TILE), :] = filler
    p, u, w, c, rho = inner
    set_coefs(n, c, rho, ax, az, stiff)
    place = lax.axis_index("depth")
    at = pl.ds(TILE, TILE)
    az[at, :] = jnp.where(place == 0, 0.0, az[at, :])
    base = place * height

    def local_row(row):
        row = row - base
        low = jnp.logical_and(row >= -TILE, row < 2 * MARGIN)
        high = jnp.logical_and(row >= split, row < height + TILE)
        return jnp.where(low, row + MARGIN, row - split + head), jnp.logical_or(low, high)

    left_steps(n, (p, u, w), (ax, az, stiff), stages, shifts, sources, wavelet, local_row)

    def finish(shift, r, k):
        fields = finals(stages, pl.ds(r, k))
        there = pl.ds(r - shift, k)
        plane[there, :] = packed(*fields)
        for f in range(3):
            done[f, there, :] = fields[f]

    for_rows(MARGIN, 2 * MARGIN, functools.partial(finish, MARGIN))
    for_rows(head + MARGIN, n - MARGIN, functools.partial(finish, head))

    def lean(shift, r, k):
        full[pl.ds(r + shift, k), :] = slanted(r, k, p, stages, stiff, rho)

    def copy(r, k):
        full[pl.ds(r + 2 * MARGIN, k), :] = first_slant[pl.ds(r, k), :]

    for_rows(TILE, 2 * MARGIN, functools.partial(lean, 0))
    for_rows(head + MARGIN, n - TILE, functools.partial(lean, split + MARGIN - head))
    for_rows(0, n_first - 2 * MARGIN, copy)
    ends = jnp.zeros((TILE, LANES), jnp.float32)
    each = (height + 2 * MARGIN) // GROUPS
    full[pl.ds(0, TILE), :] = ends
    full[pl.ds(height + 2 * MARGIN - TILE, TILE), :] = ends

    def gather(r, k):
        lanes = lane_ids(k)
        found = full[pl.ds(r, k), :]
        for g in range(1, GROUPS):
            part = roll(full[pl.ds(r + g * each, k), :], 5 * SKEW * g)
            found = jnp.where(lanes < 5 * SKEW * g, found, part)
        slant[pl.ds(r, k), :] = found

    for_rows(0, each, gather)


def right_kernel(height, n_first, extra, *refs):
    shifts, sources, wavelet = refs[:3]
    own, ahead = refs[3:8], refs[8:10]
    up, down, slant, first_done, second_done = refs[10:15]
    merged, rest = refs[15:17]
    p, u, w, c, rho, ax, az, al, stiff, gp, gu, gw = refs[17:]
    half = LANES - extra
    n = height + 2 * MARGIN
    place, depth = lax.axis_index("range"), lax.axis_index("depth")
    at_end = place == lax.axis_size("range") - 1
    each = n // GROUPS
    offsets = offsets_of(shifts)
    ghosts = (gp, gu, gw, stiff, rho)

    for g in range(GROUPS):

        def spread(r, k, g=g):
            part = slant[pl.ds(r, k), :]
            for f, ghost in enumerate(ghosts):
                ghost[pl.ds(r + g * each, k), :] = roll(part, half - SKEW * f - 5 * SKEW * g)

        for_rows(0, each, spread)

    def place_rows(e, k, parts, ahead_c, ahead_r):
        here = pl.ds(e, k)
        lanes = lane_ids(k)
        mine = lanes < half
        ghost = jnp.logical_and(between(lanes, half, half + SKEW), jnp.logical_not(at_end))
        blank = jnp.zeros((k, half), jnp.float32)
        for ref, part, source in zip((p, u, w), parts, (gp, gu, gw)):
            other = jnp.where(ghost, source[here, :], 0.0)
            ref[here, :] = jnp.where(mine, roll(part, -half), other)
        ahead_c = jnp.concatenate([blank, ahead_c], 1)
        ahead_r = jnp.concatenate([blank, ahead_r], 1)
        beyond = jnp.where(at_end, ahead_r, 1.0)
        beyond = jnp.where(ghost, rho[here, :], beyond)
        dense = roll(parts[4], -half)
        speed = roll(parts[3], -half)
        rho[here, :] = jnp.where(mine, dense, beyond)
        hard = jnp.where(at_end, TIME_STEP * (ahead_r * ahead_c * ahead_c), 0.0)
        hard = jnp.where(ghost, stiff[here, :], hard)
        stiff[here, :] = jnp.where(mine, TIME_STEP * (dense * speed * speed), hard)

    def middle(r, k):
        here = pl.ds(r, k)
        place_rows(r + MARGIN, k, [ref[here, :] for ref in own], ahead[0][here, :], ahead[1][here, :])

    for_rows(0, height, middle)
    last = pl.ds(height - 1, 1)
    above, below = [], []
    for k in range(5):
        last_own = jnp.broadcast_to(own[k][last, :], (TILE, LANES))
        one, two = ghost_rows(up, down, k, last_own)
        above.append(one)
        below.append(two)
    at = pl.ds(5 * TILE, TILE)
    one, two = up[at, :], down[at, :]
    last_ahead = jnp.broadcast_to(ahead[1][last, :], (TILE, extra))
    one_r = jnp.where(depth == 0, 1.0, one[:, extra:])
    two_r = jnp.where(depth == lax.axis_size("depth") - 1, last_ahead, two[:, extra:])
    place_rows(TILE, TILE, above, one[:, :extra], one_r)
    place_rows(height + MARGIN, TILE, below, two[:, :extra], two_r)
    for e in (0, n - TILE):
        here = pl.ds(e, TILE)
        for ref in (p, u, w, stiff):
            ref[here, :] = jnp.zeros((TILE, LANES), jnp.float32)
        rho[here, :] = jnp.ones((TILE, LANES), jnp.float32)

    def coefs(r, k):
        here = pl.ds(r, k)
        dense = rho[here, :]
        ax[here, :] = (2.0 * TIME_STEP) / (dense + roll(dense, -1))
        az[here, :] = (2.0 * TIME_STEP) / (dense + rho[pl.ds(r + 1, k), :])
        al[here, :] = TIME_STEP / dense

    for_rows(0, n - TILE, coefs)
    at = pl.ds(TILE, TILE)
    az[at, :] = jnp.where(depth == 0, 0.0, az[at, :])
    base = depth * height

    def local_row(row):
        row = row - base
        inside = jnp.logical_and(row >= -TILE, row < height + TILE)
        return row + MARGIN, inside

    for t in range(ITERS):
        edge = jnp.where(at_end, half - 1 + offsets[t], FAR)
        taken = jnp.where(at_end, -1, half + t)

        def speeds(r, k):
            here = pl.ds(r, k)
            lanes = lane_ids(k)
            now = p[here, :]
            dead = lanes > edge
            slope = jnp.where(lanes == edge, al[here, :], ax[here, :])
            slope = jnp.where(dead, 0.0, slope)
            fast = u[here, :] - slope * (roll(now, -1) - now)
            u[here, :] = jnp.where(lanes == taken, gu[here, :], fast)
            slope = jnp.where(dead, 0.0, az[here, :])
            deep = w[here, :] - slope * (p[pl.ds(r + 1, k), :] - now)
            w[here, :] = jnp.where(lanes == taken, gw[here, :], deep)

        def press(r, k):
            here = pl.ds(r, k)
            lanes = lane_ids(k)
            fast = u[here, :]
            down_ = w[here, :] - w[pl.ds(r - 1, k), :]
            hard = jnp.where(lanes > edge, 0.0, stiff[here, :])
            found = p[here, :] - hard * ((fast - roll(fast, 1)) + down_)
            if t < ITERS - 1:
                found = jnp.where(lanes == taken + 1, jnp.where(at_end, found, gp[here, :]), found)
            p[here, :] = found

        for_rows(0, n - TILE, speeds)
        for_rows(TILE, n - TILE, press)
        reach = jnp.where(at_end, LANES - 1, half + t)
        inject(p, sources, wavelet, t, local_row, place * LANES + half, reach)

    n_done = n_first - 2 * MARGIN
    total = offsets[ITERS]

    def merge(shift, source, r, k):
        there = pl.ds(r, k)
        lanes = lane_ids(k)
        from_right = jnp.logical_or(lanes >= half + SKEW, lanes < SKEW)
        from_right = jnp.logical_or(from_right, jnp.logical_and(at_end, lanes < total))
        for f, ref in enumerate((p, u, w)):
            right = roll(ref[pl.ds(r + MARGIN, k), :], half)
            merged[f, there, :] = jnp.where(from_right, right, source[f, pl.ds(r - shift, k), :])

    for_rows(0, MARGIN, functools.partial(merge, 0, second_done))
    for_rows(MARGIN, MARGIN + n_done, functools.partial(merge, MARGIN, first_done))
    for_rows(MARGIN + n_done, height, functools.partial(merge, n_done, second_done))

    more = extra - SKEW - WIDTH
    start = SKEW + WIDTH

    def done_rows(r):
        if r < MARGIN:
            return second_done, 0
        if r < MARGIN + n_done:
            return first_done, MARGIN
        return second_done, n_done

    def join(fields):
        lanes = lane_ids(fields[0].shape[0])
        found = jnp.where(lanes < start + 2 * more, roll(fields[1], more), roll(fields[2], 2 * more))
        return jnp.where(lanes < start + more, fields[0], found)

    def beside(one, one_shift, two, two_shift, r, k):
        lanes = lane_ids(k)
        a = join([one[f, pl.ds(r - one_shift, k), :] for f in range(3)])
        b = join([two[f, pl.ds(r + height // 2 - two_shift, k), :] for f in range(3)])
        rest[pl.ds(r, k), :] = jnp.where(between(lanes, start, start + 3 * more), a, roll(b, LANES // 2))

    cuts = {0, height // 2, MARGIN, MARGIN + n_done, MARGIN - height // 2}
    cuts |= {MARGIN + n_done - height // 2}
    cuts = sorted(x for x in cuts if 0 <= x <= height // 2)
    for low, high in zip(cuts[:-1], cuts[1:]):
        one, one_shift = done_rows(low)
        two, two_shift = done_rows(low + height // 2)
        for_rows(low, high, functools.partial(beside, one, one_shift, two, two_shift))


def last_kernel(height, n_first, extra, shifts, merged, first, second, rest, *outs):
    place = lax.axis_index("range")
    at_end = place == lax.axis_size("range") - 1
    total = offsets_of(shifts)[ITERS]
    n_done = n_first - 2 * MARGIN
    more = extra - SKEW - WIDTH
    start = SKEW + WIDTH
    turn = LANES - total

    def build(source, shift, upper, r, k):
        here = pl.ds(r, k)
        lanes = lane_ids(k)
        near = source[pl.ds(r - shift, k), :]
        far = rest[here, :] if not upper else roll(rest[pl.ds(r - height // 2, k), :], LANES // 2)
        theirs = jnp.logical_and(between(lanes, SKEW, total), jnp.logical_not(at_end))
        for f, out in enumerate(outs):
            got = jnp.where(lanes < start, roll(near, -WIDTH * f), roll(far, -more * f))
            out[here, :] = pltpu.roll(jnp.where(theirs, got, merged[f, here, :]), turn, 1)

    cuts = sorted({0, MARGIN, height // 2, MARGIN + n_done, height})
    for low, high in zip(cuts[:-1], cuts[1:]):
        if low < MARGIN:
            source, shift = second, 0
        elif low < MARGIN + n_done:
            source, shift = first, MARGIN
        else:
            source, shift = second, n_done
        for_rows(low, high, functools.partial(build, source, shift, low >= height // 2))


def moved(x, axis, by):
    size = lax.axis_size(axis)
    return lax.ppermute(x, axis, [(i, i + by) for i in range(size) if 0 <= i + by < size])


def block(rows, at=0, lanes=LANES):
    return pl.BlockSpec((rows, lanes), lambda i: (at, 0))


def whole(x):
    return pl.BlockSpec(x.shape, lambda i: (0,) * len(x.shape))


def scalars(count):
    return [pl.BlockSpec(memory_space=pltpu.SMEM)] * count


def call(kernel, name, ins, specs, outs, scratch):
    return pl.pallas_call(
        kernel,
        name=name,
        grid=(1,),
        in_specs=specs,
        out_specs=[whole(x) for x in outs],
        out_shape=outs,
        scratch_shapes=scratch,
        compiler_params=pltpu.CompilerParams(vmem_limit_bytes=56 * 1024 * 1024),
    )(*ins)


def real(*shape):
    return jax.ShapeDtypeStruct(shape, jnp.float32)


def room(*shape):
    return pltpu.VMEM(shape, jnp.float32)


def shards(
    pressure,
    vel_range,
    vel_depth,
    sound_speed,
    density,
    ahead_speed,
    ahead_density,
    shifts,
    sources,
    wavelet,
):
    height, breadth = pressure.shape
    extra = ahead_speed.shape[1]
    assert breadth == LANES and SKEW + WIDTH < extra < LANES
    assert height % 512 == 0
    own = (pressure, vel_range, vel_depth, sound_speed, density)
    ahead = (ahead_speed, ahead_density)
    small = (shifts, sources, wavelet)

    split = height * 3 // 4
    n_first = split + 2 * MARGIN
    last = height // TILE - 1
    plane_a, done_a, slant_a, to_up, to_down = call(
        functools.partial(first_kernel, n_first, height),
        "first",
        (*small, *own, *own, *ahead, *ahead),
        [
            *scalars(3),
            *[block(n_first)] * 5,
            *[block(TILE, last)] * 5,
            *[block(TILE, 0, extra)] * 2,
            *[block(TILE, last, extra)] * 2,
        ],
        [
            real(split, LANES),
            real(3, split, LANES),
            real(split, LANES),
            real(6 * TILE, LANES),
            real(6 * TILE, LANES),
        ],
        [room(n_first, LANES)] * 3 + [room(ITERS, n_first, LANES)] * 3,
    )
    near = moved(plane_a, "range", -1)
    down = moved(to_up, "depth", -1)
    up = moved(to_down, "depth", 1)

    rest_rows = height - split
    n_second = 3 * MARGIN + rest_rows + MARGIN
    plane_b, done_b, slant = call(
        functools.partial(second_kernel, n_second, height, n_first),
        "second",
        (*small, *own, *own, up, down, slant_a),
        [
            *scalars(3),
            *[block(2 * MARGIN)] * 5,
            *[block(rest_rows, split // rest_rows)] * 5,
            whole(up),
            whole(down),
            whole(slant_a),
        ],
        [
            real(rest_rows, LANES),
            real(3, rest_rows, LANES),
            real((height + 2 * MARGIN) // GROUPS, LANES),
        ],
        [room(n_second, LANES)] * 3
        + [room(ITERS, n_second, LANES)] * 3
        + [room(n_second, LANES)] * 5
        + [room(height + 2 * MARGIN, LANES)],
    )
    slant = moved(slant, "range", -1)
    edge = moved(plane_b, "range", -1)

    merged, rest = call(
        functools.partial(right_kernel, height, n_first, extra),
        "right",
        (*small, *own, *ahead, up, down, slant, done_a, done_b),
        [*scalars(3), *[whole(x) for x in (*own, *ahead, up, down, slant, done_a, done_b)]],
        [real(3, height, LANES), real(height // 2, LANES)],
        [room(height + 2 * MARGIN, LANES)] * 12,
    )
    rest = lax.cond(
        jnp.sum(shifts) > SKEW + WIDTH,
        lambda x: moved(x, "range", -1),
        jnp.zeros_like,
        rest,
    )
    return tuple(
        call(
            functools.partial(last_kernel, height, n_first, extra),
            "last",
            (shifts, merged, near, edge, rest),
            [*scalars(1), *[whole(x) for x in (merged, near, edge, rest)]],
            [real(height, LANES)] * 3,
            [],
        )
    )


def solution(mesh):
    field = P("depth", "range")
    strip = P("depth", None)
    return jax.shard_map(
        shards,
        mesh=mesh,
        in_specs=(field,) * 5 + (strip,) * 2 + (P(),) * 3,
        out_specs=(field,) * 3,
        check_vma=False,
    )
```

```python
import functools

import jax
import jax.numpy as jnp
from jax import lax
from jax.experimental import pallas as pl
from jax.experimental.pallas import tpu as pltpu
from jax.sharding import PartitionSpec as P

ITERS = 4
TIME_STEP = 0.6
LANES = 128
TILE = 8
MARGIN = 16
SKEW = 4
WIDTH = 42
STRIP = 16
BLOCKS = LANES // STRIP
KEPT = LANES - STRIP // 2
BLOCK = 256
FAR = 1 << 20


def lane_ids(rows):
    return lax.broadcasted_iota(jnp.int32, (rows, LANES), 1)


def between(lanes, low, high):
    return jnp.logical_and(lanes >= low, lanes < high)


def roll(x, by):
    return pltpu.roll(x, by % LANES, 1)


def for_rows(start, stop, fn, size=BLOCK):
    whole = (stop - start) // size

    def step(i, carry):
        fn(pl.multiple_of(start + i * size, TILE), size)
        return carry

    if whole > 1:
        lax.fori_loop(0, whole, step, 0)
    elif whole == 1:
        fn(start, size)
    if start + whole * size < stop:
        fn(start + whole * size, stop - start - whole * size)


def offsets_of(shifts):
    found = [jnp.int32(0)]
    for t in range(ITERS):
        found.append(found[-1] + shifts[t])
    return found


def range_ends():
    place = lax.axis_index("range")
    return place == 0, place == lax.axis_size("range") - 1


def depth_ends():
    place = lax.axis_index("depth")
    return place == 0, place == lax.axis_size("depth") - 1


def set_coefs(start, stop, c, rho, ax, az, stiff):
    def coefs(r, k):
        here = pl.ds(r, k)
        dense = rho[here, :]
        ax[here, :] = (2.0 * TIME_STEP) / (dense + roll(dense, -1))
        az[here, :] = (2.0 * TIME_STEP) / (dense + rho[pl.ds(r + 1, k), :])
        if c is not None:
            speed = c[here, :]
            stiff[here, :] = TIME_STEP * (dense * speed * speed)

    for_rows(start, stop, coefs)


class Scalars:
    def __init__(self, remote, local):
        refs, sems = local[:3], local[3]
        pairs = zip(remote, refs)
        self.copies = [
            pltpu.make_async_copy(a, b, sems.at[k]) for k, (a, b) in enumerate(pairs)
        ]
        for copy in self.copies:
            copy.start()
        self.refs = refs

    def wait(self):
        for copy in self.copies:
            copy.wait()
        return self.refs


def find_sources(sources, first_row, places):
    found = []
    for k in range(sources.shape[1]):
        for row, lane, good in places(sources[0, k] - first_row, sources[1, k]):
            good = jnp.logical_and(good, jnp.logical_and(lane >= 0, lane < LANES))
            found.append((k, row, lane, good))
    return found


def inject(field, found, wavelet, t, reach=None):
    here_any = functools.reduce(jnp.logical_or, [good for _, _, _, good in found])

    @pl.when(here_any)
    def _():
        rows = lax.broadcasted_iota(jnp.int32, (TILE, LANES), 0)
        lanes = lane_ids(TILE)
        for k, row, lane, good in found:
            if reach is not None:
                good = jnp.logical_and(good, lane % STRIP <= reach)

            @pl.when(good)
            def _(k=k, row=row, lane=lane):
                at = pl.ds(pl.multiple_of((row // TILE) * TILE, TILE), TILE)
                here = jnp.logical_and(rows == row % TILE, lanes == lane)
                field[at, :] = field[at, :] + jnp.where(here, wavelet[t, k], 0.0)


def left_steps(n, fields, coefs, stages, shifts, found, wavelet):
    ax, az, stiff = coefs
    ps, us, ws = stages
    offsets = offsets_of(shifts)
    at_start, _ = range_ends()
    for t in range(ITERS):
        p, u, w = fields if t == 0 else (ps.at[t - 1], us.at[t - 1], ws.at[t - 1])
        u_new, w_new, p_new = us.at[t], ws.at[t], ps.at[t]
        wall = jnp.where(at_start, offsets[t], -1)

        def speeds(r, k):
            here = pl.ds(r, k)
            now = p[here, :]
            u_new[here, :] = u[here, :] - ax[here, :] * (roll(now, -1) - now)
            w_new[here, :] = w[here, :] - az[here, :] * (p[pl.ds(r + 1, k), :] - now)

        def press(r, k):
            here = pl.ds(r, k)
            fast = u_new[here, :]
            left = jnp.where(lane_ids(k) == wall, 0.0, roll(fast, 1))
            down = w_new[here, :] - w_new[pl.ds(r - 1, k), :]
            p_new[here, :] = p[here, :] - stiff[here, :] * ((fast - left) + down)

        for_rows(0, n - TILE, speeds)
        for_rows(TILE, n - TILE, press)
        inject(p_new, found, wavelet, t)


def slanted(here, p0, stages, stiff):
    ps, us, ws = stages
    lanes = lane_ids(TILE)

    def pick(parts):
        found = parts[-1]
        for t in range(len(parts) - 2, -1, -1):
            found = jnp.where(lanes <= t, parts[t], found)
        return found

    a = pick([p0[here, :]] + [ps[t, here, :] for t in range(ITERS - 1)])
    b = pick([us[t, here, :] for t in range(ITERS)])
    c = pick([ws[t, here, :] for t in range(ITERS)])
    found = jnp.where(lanes < 3 * SKEW, roll(c, 2 * SKEW), roll(stiff, 3 * SKEW))
    found = jnp.where(lanes < 2 * SKEW, roll(b, SKEW), found)
    return jnp.where(lanes < SKEW, a, found)


def packed(p, u, w):
    lanes = lane_ids(p.shape[0])
    found = jnp.where(
        between(lanes, SKEW, SKEW + 2 * WIDTH), roll(u, WIDTH), roll(w, 2 * WIDTH)
    )
    return jnp.where(between(lanes, SKEW, SKEW + WIDTH), p, found)


def finals(stages, here):
    return [stage[ITERS - 1, here, :] for stage in stages]


def own_kernel(height, *refs):
    arrays, ahead = refs[3:8], refs[8:10]
    scalars = Scalars(refs[:3], refs[28:])
    plane, to_up, to_down = refs[10:13]
    own, stages, flag = refs[13:18], refs[18:21], refs[21]
    ax, az, stiff, ends, sems, end_sems = refs[22:28]
    order = (4, 3, 0, 1, 2)
    copies = {k: pltpu.make_async_copy(arrays[k], own[k], sems.at[k]) for k in order}
    for k in order:
        copies[k].start()
    end_copies = []
    for side, start in enumerate((0, height - LANES)):
        for f in range(2):
            copy = pltpu.make_async_copy(
                ahead[f].at[:, pl.ds(start, LANES)],
                ends.at[side, pl.ds(f * LANES // 2, LANES // 2), :],
                end_sems.at[side, f],
            )
            copy.start()
            end_copies.append(copy)
    p, u, w, c, rho = own

    def place(row, col):
        return [(row, col - lax.axis_index("range") * LANES, between(row, 0, height))]

    copies[4].wait()
    copies[3].wait()
    set_coefs(0, height - TILE, c, rho, ax, az, stiff)
    shifts, sources, wavelet = scalars.wait()
    flag[0] = jnp.where(offsets_of(shifts)[ITERS] > SKEW + WIDTH, 1, 0)
    found = find_sources(sources, lax.axis_index("depth") * height, place)
    for k in (0, 1, 2):
        copies[k].wait()
    left_steps(height, (p, u, w), (ax, az, stiff), stages, shifts, found, wavelet)

    def finish(r, k):
        plane[pl.ds(r - MARGIN, k), :] = packed(*finals(stages, pl.ds(r, k)))

    for_rows(MARGIN, height - MARGIN, finish)
    for copy in end_copies:
        copy.wait()
    for k in range(5):
        to_up[pl.ds(k * TILE, TILE), :] = own[k][pl.ds(0, TILE), :]
        to_down[pl.ds(k * TILE, TILE), :] = own[k][pl.ds(height - TILE, TILE), :]
    at = pl.ds(5 * TILE, TILE)
    to_up[at, :] = ends[0].T[:TILE]
    to_down[at, :] = ends[1].T[LANES - TILE :]


def own_stiff(own, here):
    speed = own[3][here, :]
    return TIME_STEP * (own[4][here, :] * speed * speed)


def lean_kernel(height, *refs):
    own, stages, lean = refs[:5], refs[5:8], refs[8]
    each = height // BLOCKS
    tiles = each // TILE + 2

    def tile(i, slot, group):
        lanes = lane_ids(TILE)
        found = rhos = None
        for b in range(BLOCKS):
            row = b * each + i * TILE - TILE
            if not isinstance(i, int):
                row = pl.multiple_of(row, TILE)
            elif row < 0 or row >= height:
                row = 0
            here = pl.ds(row, TILE)
            part = slanted(here, own[0], stages, own_stiff(own, here))
            part = roll(part, STRIP * b) if b else part
            dense = roll(own[4][here, :], 4 * BLOCKS * slot + SKEW * b)
            found = part if b == 0 else jnp.where(lanes < STRIP * b, found, part)
            rhos = dense if b == 0 else jnp.where(lanes < 4 * BLOCKS * slot + SKEW * b, rhos, dense)
        lean[pl.ds(i * TILE, TILE), :] = found
        return rhos

    def group_of(first, count, out):
        lanes = lane_ids(TILE)
        total = None
        for slot in range(count):
            rhos = tile(first + slot, slot, out)
            total = rhos if slot == 0 else jnp.where(lanes < 4 * BLOCKS * slot, total, rhos)
        lean[pl.ds((tiles + out) * TILE, TILE), :] = total

    groups = (tiles - 2) // 4

    def body(m, carry):
        group_of(1 + 4 * m, 4, m)
        return carry

    lax.fori_loop(0, groups, body, 0)
    lanes = lane_ids(TILE)
    total = jnp.where(lanes < 4 * BLOCKS, tile(0, 0, groups), tile(tiles - 1, 1, groups))
    lean[pl.ds((tiles + groups) * TILE, TILE), :] = total


def ghost_rows(up, down, k, last_own):
    at_top, at_bottom = depth_ends()
    at = pl.ds(k * TILE, TILE)
    above, below = up[at, :], down[at, :]
    if k == 4:
        above = jnp.where(at_top, 1.0, above)
        below = jnp.where(at_bottom, last_own, below)
    return above, below


def edge_kernel(height, *refs):
    scalars = Scalars(refs[:3], refs[24:])
    own, up, down, lean = refs[3:8], refs[8], refs[9], refs[10]
    out, done = refs[11:13]
    ax, az, stiff = refs[13:16]
    stages, inner = refs[16:19], refs[19:24]
    seg = 3 * MARGIN
    n = 2 * seg
    low = height - 2 * MARGIN
    for k in range(5):
        filler = jnp.full((TILE, LANES), 1.0 if k == 4 else 0.0, jnp.float32)
        last_own = jnp.broadcast_to(own[k][pl.ds(height - 1, 1), :], (TILE, LANES))
        above, below = ghost_rows(up, down, k, last_own)
        inner[k][pl.ds(0, TILE), :] = filler
        inner[k][pl.ds(TILE, TILE), :] = above
        inner[k][pl.ds(2 * TILE, 2 * MARGIN), :] = own[k][pl.ds(0, 2 * MARGIN), :]
        inner[k][pl.ds(seg, 2 * MARGIN), :] = own[k][pl.ds(low, 2 * MARGIN), :]
        inner[k][pl.ds(n - 2 * TILE, TILE), :] = below
        inner[k][pl.ds(n - TILE, TILE), :] = filler
    p, u, w, c, rho = inner
    set_coefs(0, n - TILE, c, rho, ax, az, stiff)
    at_top, _ = depth_ends()
    at = pl.ds(TILE, TILE)
    az[at, :] = jnp.where(at_top, 0.0, az[at, :])

    def place(row, col):
        upper = between(row, -TILE, 2 * MARGIN)
        lower = between(row, low, height + TILE)
        local = jnp.where(upper, row + MARGIN, row - low + seg)
        lane = col - lax.axis_index("range") * LANES
        return [(local, lane, jnp.logical_or(upper, lower))]

    shifts, sources, wavelet = scalars.wait()
    found = find_sources(sources, lax.axis_index("depth") * height, place)
    left_steps(n, (p, u, w), (ax, az, stiff), stages, shifts, found, wavelet)
    for side, start in enumerate((MARGIN, seg + MARGIN)):
        fields = finals(stages, pl.ds(start, MARGIN))
        there = pl.ds(side * MARGIN, MARGIN)
        out[there, :] = packed(*fields)
        for f in range(3):
            done[f, there, :] = fields[f]
    base = 2 * MARGIN
    rest = lean.shape[0]
    tiles = height // BLOCKS // TILE + 2
    out[pl.ds(base, rest), :] = lean[...]
    lanes = lane_ids(TILE)
    for b, first, start in ((0, 0, TILE), (BLOCKS - 1, tiles - 3, seg + MARGIN)):
        for j in range(3):
            i = first + j
            here = pl.ds(start + j * TILE, TILE)
            part = roll(slanted(here, p, stages, stiff[here, :]), STRIP * b)
            at = pl.ds(base + i * TILE, TILE)
            mine = between(lanes, STRIP * b, STRIP * (b + 1))
            out[at, :] = jnp.where(mine, part, out[at, :])
            group, slot = rho_slot(i, tiles)
            start_lane = 4 * BLOCKS * slot + SKEW * b
            at = pl.ds(base + (tiles + group) * TILE, TILE)
            mine = between(lanes, start_lane, start_lane + SKEW)
            out[at, :] = jnp.where(mine, roll(rho[here, :], start_lane), out[at, :])


def rho_slot(i, tiles):
    if i == 0:
        return (tiles - 2) // 4, 0
    if i == tiles - 1:
        return (tiles - 2) // 4, 1
    return (i - 1) // 4, (i - 1) % 4


def wide_kernel(height, *refs):
    own, ahead, up, down = refs[3:8], refs[8:10], refs[10], refs[11]
    strip, out = refs[12:14]
    p, u, w = out.at[0], out.at[1], out.at[2]
    rho, ax, az, al, stiff, raw, sems = refs[14:21]
    half = LANES // 2
    n = height + 2 * MARGIN
    at_top, at_bottom = depth_ends()
    _, at_end = range_ends()

    @pl.when(jnp.logical_not(at_end))
    def _():
        each = height // BLOCKS
        rows = each + 2 * TILE

        def put(i, k, parts):
            lanes = lane_ids(k)
            for a in range(5):
                found = None
                for b in range(BLOCKS):
                    part = roll(parts[b][a], STRIP * b - KEPT)
                    found = part if b == 0 else jnp.where(lanes < STRIP * b, found, part)
                strip[a, pl.ds(i + TILE, k), :] = found

        def fields(here):
            return [own[0][here, :], own[1][here, :], own[2][here, :], own_stiff(own, here), own[4][here, :]]

        def middle(i, k):
            put(i, k, [fields(pl.ds(b * each - TILE + i, k)) for b in range(BLOCKS)])

        for_rows(TILE, rows - TILE, middle, 32)
        above, below = [], []
        for k in range(5):
            last_own = jnp.broadcast_to(own[k][pl.ds(height - 1, 1), :], (TILE, LANES))
            one, two = ghost_rows(up, down, k, last_own)
            above.append(one)
            below.append(two)
        for parts in (above, below):
            parts[3] = TIME_STEP * (parts[4] * parts[3] * parts[3])
        inner = [fields(pl.ds(b * each - TILE, TILE)) for b in range(1, BLOCKS)]
        put(0, TILE, [above] + inner)
        inner = [fields(pl.ds((b + 1) * each, TILE)) for b in range(BLOCKS - 1)]
        put(rows - TILE, TILE, inner + [below])

    @pl.when(at_end)
    def _():
        scalars = Scalars(refs[:3], refs[21:])
        copies = [pltpu.make_async_copy(ahead[f], raw.at[f], sems.at[f]) for f in range(2)]
        for copy in copies:
            copy.start()
        for copy in copies:
            copy.wait()

        def place_rows(e, k, parts, both):
            here = pl.ds(e, k)
            lanes = lane_ids(k)
            mine = lanes < half
            for ref, part in zip((p, u, w), parts):
                ref[here, :] = jnp.where(mine, roll(part, half), 0.0)
            dense = jnp.where(mine, roll(parts[4], half), both)
            speed = roll(jnp.where(mine, both, parts[3]), half)
            rho[here, :] = dense
            stiff[here, :] = TIME_STEP * (dense * speed * speed)

        for j in range(height // LANES):
            at = pl.ds(j * LANES, LANES)
            both = jnp.concatenate([raw[0, :, at], raw[1, :, at]], 0).T
            place_rows(j * LANES + MARGIN, LANES, [ref[at, :] for ref in own], both)
        above, below = [], []
        for k in range(5):
            last_own = jnp.broadcast_to(own[k][pl.ds(height - 1, 1), :], (TILE, LANES))
            one, two = ghost_rows(up, down, k, last_own)
            above.append(one)
            below.append(two)
        at = pl.ds(5 * TILE, TILE)
        lanes = lane_ids(TILE)
        one, two = up[at, :], down[at, :]
        last = jnp.broadcast_to(rho[pl.ds(height + MARGIN - 1, 1), :], (TILE, LANES))
        one = jnp.where(jnp.logical_and(at_top, lanes >= half), 1.0, one)
        two = jnp.where(jnp.logical_and(at_bottom, lanes >= half), last, two)
        place_rows(TILE, TILE, above, one)
        place_rows(height + MARGIN, TILE, below, two)
        for e in (0, n - TILE):
            here = pl.ds(e, TILE)
            for ref in (p, u, w, stiff):
                ref[here, :] = jnp.zeros((TILE, LANES), jnp.float32)
            rho[here, :] = jnp.ones((TILE, LANES), jnp.float32)
        set_coefs(0, n - TILE, None, rho, ax, az, None)

        def edge_coefs(r, k):
            al[pl.ds(r, k), :] = TIME_STEP / rho[pl.ds(r, k), :]

        for_rows(0, n - TILE, edge_coefs)
        at = pl.ds(TILE, TILE)
        az[at, :] = jnp.where(at_top, 0.0, az[at, :])

        def place(row, col):
            good = between(row, -TILE, height + TILE)
            return [(row + MARGIN, col - lax.axis_index("range") * LANES - half, good)]

        shifts, sources, wavelet = scalars.wait()
        found = find_sources(sources, lax.axis_index("depth") * height, place)
        offsets = offsets_of(shifts)
        for t in range(ITERS):
            edge = half - 1 + offsets[t]

            def speeds(r, k):
                here = pl.ds(r, k)
                lanes = lane_ids(k)
                now = p[here, :]
                slope = jnp.where(lanes == edge, al[here, :], ax[here, :])
                slope = jnp.where(lanes > edge, 0.0, slope)
                u[here, :] = u[here, :] - slope * (roll(now, -1) - now)
                slope = jnp.where(lanes > edge, 0.0, az[here, :])
                w[here, :] = w[here, :] - slope * (p[pl.ds(r + 1, k), :] - now)

            def press(r, k):
                here = pl.ds(r, k)
                fast = u[here, :]
                down_ = w[here, :] - w[pl.ds(r - 1, k), :]
                hard = jnp.where(lane_ids(k) > edge, 0.0, stiff[here, :])
                p[here, :] = p[here, :] - hard * ((fast - roll(fast, 1)) + down_)

            for_rows(0, n - TILE, speeds)
            for_rows(TILE, n - TILE, press)
            inject(p, found, wavelet, t)


def rest_kernel(height, extra, *refs):
    stages, done, out = refs[:3], refs[3], refs[4]
    more = extra - SKEW - WIDTH
    start = SKEW + WIDTH
    half = height // 2

    def read(row, k):
        if isinstance(row, int) and row < MARGIN:
            return [done[f, pl.ds(row, k), :] for f in range(3)]
        if isinstance(row, int) and row >= height - MARGIN:
            return [done[f, pl.ds(row - height + 2 * MARGIN, k), :] for f in range(3)]
        return finals(stages, pl.ds(row, k))

    def join(fields):
        lanes = lane_ids(fields[0].shape[0])
        found = jnp.where(lanes < start + 2 * more, roll(fields[1], more), roll(fields[2], 2 * more))
        return jnp.where(lanes < start + more, fields[0], found)

    def beside(r, k):
        inner = between(lane_ids(k), start, start + 3 * more)
        out[pl.ds(r, k), :] = jnp.where(inner, join(read(r, k)), roll(join(read(r + half, k)), LANES // 2))

    beside(0, MARGIN)
    for_rows(MARGIN, half - MARGIN, beside, 96)
    beside(half - MARGIN, MARGIN)


def last_kernel(height, extra, far_too, *refs):
    stages, done, strip, wide, near, edge = refs[3:6], *refs[6:11]
    rest = refs[11] if far_too else None
    scalars_in, refs = refs[:3], refs[11 + far_too :]
    outs, built = refs[:3], refs[3:6]
    scalars = Scalars(scalars_in, refs[17:])
    p, u, w, rho, ax, az, stiff, gp, gu, gw, sems = refs[6:17]
    at_top, at_bottom = depth_ends()
    at_start, at_end = range_ends()
    each = height // BLOCKS
    tiles = each // TILE + 2
    n = (tiles + 2) * TILE
    half = LANES // 2
    base = 2 * MARGIN
    own_part = STRIP // 2
    shifts, sources, wavelet = scalars.wait()

    @pl.when(jnp.logical_not(at_end))
    def _():
        for i in range(tiles):
            lanes = lane_ids(TILE)
            inner = lanes % STRIP
            here = pl.ds((i + 1) * TILE, TILE)
            pack = edge[pl.ds(base + i * TILE, TILE), :]
            group, slot = rho_slot(i, tiles)
            dense = edge[pl.ds(base + (tiles + group) * TILE, TILE), :]
            theirs = None
            for b in range(BLOCKS):
                part = roll(dense, STRIP * b + own_part - 4 * BLOCKS * slot - SKEW * b)
                theirs = part if b == 0 else jnp.where(lanes < STRIP * b, theirs, part)
            ghosts = [roll(pack, own_part - SKEW * g) for g in range(4)]
            for ref, ghost in zip((gp, gu, gw), ghosts):
                ref[here, :] = ghost
            mine, ghost = inner < own_part, inner < own_part + SKEW
            fill = [0.0, 0.0, 0.0, 0.0, 1.0]
            for a, (ref, part) in enumerate(zip((p, u, w, stiff, rho), (*ghosts, theirs))):
                other = jnp.where(ghost, part, fill[a])
                ref[here, :] = jnp.where(mine, strip[a, here, :], other)
        for e in (0, n - TILE):
            here = pl.ds(e, TILE)
            for ref in (p, u, w, stiff):
                ref[here, :] = jnp.zeros((TILE, LANES), jnp.float32)
            rho[here, :] = jnp.ones((TILE, LANES), jnp.float32)
        set_coefs(TILE, n - TILE, None, rho, ax, az, None)
        at = pl.ds(TILE, TILE)
        az[at, :] = jnp.where(jnp.logical_and(at_top, lane_ids(TILE) < STRIP), 0.0, az[at, :])

        def place(row, col):
            col = col - lax.axis_index("range") * LANES - KEPT
            inside = between(col, 0, STRIP)
            inside = jnp.logical_and(inside, between(row, -TILE, height + TILE))
            b = (row + TILE) // each
            local = row + TILE - b * each
            one = jnp.logical_and(inside, b < BLOCKS)
            two = jnp.logical_and(inside, jnp.logical_and(b > 0, local < 2 * TILE))
            return [
                (local + TILE, STRIP * b + col, one),
                (local + each + TILE, STRIP * (b - 1) + col, two),
            ]

        found = find_sources(sources, lax.axis_index("depth") * height, place)
        for t in range(ITERS):
            taken = own_part + t

            def speeds(r, k):
                here = pl.ds(r, k)
                inner = lane_ids(k) % STRIP
                now = p[here, :]
                fast = u[here, :] - ax[here, :] * (roll(now, -1) - now)
                u[here, :] = jnp.where(inner == taken, gu[here, :], fast)
                deep = w[here, :] - az[here, :] * (p[pl.ds(r + 1, k), :] - now)
                w[here, :] = jnp.where(inner == taken, gw[here, :], deep)

            def press(r, k):
                here = pl.ds(r, k)
                inner = lane_ids(k) % STRIP
                fast = u[here, :]
                down_ = w[here, :] - w[pl.ds(r - 1, k), :]
                new = p[here, :] - stiff[here, :] * ((fast - roll(fast, 1)) + down_)
                if t < ITERS - 1:
                    new = jnp.where(inner == taken + 1, gp[here, :], new)
                p[here, :] = new

            for_rows(TILE, n - TILE, speeds)
            for_rows(TILE, n - TILE, press)
            inject(p, found, wavelet, t, taken)

    total = offsets_of(shifts)[ITERS]
    more = extra - SKEW - WIDTH
    start = SKEW + WIDTH
    turn = LANES - total
    copies = []
    for b in range(BLOCKS):
        first = b * each
        cuts = [first, first + each]
        if b == 0:
            cuts.insert(1, MARGIN)
        if b == BLOCKS - 1:
            cuts.insert(1, height - MARGIN)
        pieces = []
        for low, high in zip(cuts[:-1], cuts[1:]):
            here, k = pl.ds(low, high - low), high - low
            if low < MARGIN or low >= height - MARGIN:
                there = pl.ds(0 if low < MARGIN else MARGIN, MARGIN)
                mine = functools.partial(lambda f, there: done[f, there, :], there=there)
                theirs = functools.partial(lambda there: edge[there, :], there=there)
            else:
                mine = functools.partial(lambda f, here: stages[f][ITERS - 1, here, :], here=here)
                there = pl.ds(low - MARGIN, k)
                theirs = functools.partial(lambda there: near[there, :], there=there)
            pieces.append((low, k, here, mine, theirs))

        @pl.when(jnp.logical_not(at_end))
        def _(pieces=pieces, b=b, first=first):
            for low, k, here, mine, theirs in pieces:
                lanes = lane_ids(k)
                got = theirs()
                if far_too and low < height // 2:
                    far = rest[here, :]
                elif far_too:
                    far = roll(rest[pl.ds(low - height // 2, k), :], half)
                for f, ref in enumerate((p, u, w)):
                    part = roll(ref[pl.ds(low - first + 2 * TILE, k), :], KEPT - STRIP * b)
                    inner = between(lanes, SKEW, KEPT + SKEW)
                    found = jnp.where(inner, mine(f), part)
                    other = roll(got, -WIDTH * f)
                    if far_too:
                        other = jnp.where(lanes < start, other, roll(far, -more * f))
                    found = jnp.where(between(lanes, SKEW, total), other, found)
                    built[f][here, :] = pltpu.roll(found, turn, 1)

        @pl.when(at_end)
        def _(pieces=pieces):
            for low, k, here, mine, theirs in pieces:
                lanes = lane_ids(k)
                inner = jnp.logical_and(lanes >= total, lanes < KEPT + SKEW)
                for f in range(3):
                    part = roll(wide[f, pl.ds(low + MARGIN, k), :], half)
                    built[f][here, :] = pltpu.roll(jnp.where(inner, mine(f), part), turn, 1)

        for f in range(3):
            at = pl.ds(first, each)
            copy = pltpu.make_async_copy(built[f].at[at, :], outs[f].at[at, :], sems.at[f, b])
            copy.start()
            copies.append(copy)
    for copy in copies:
        copy.wait()


def moved(x, axis, by):
    size = lax.axis_size(axis)
    return lax.ppermute(x, axis, [(i, i + by) for i in range(size) if 0 <= i + by < size])


LOCAL = pl.BlockSpec(memory_space=pltpu.VMEM)
REMOTE = pl.BlockSpec(memory_space=pl.ANY)
FLAG = pl.BlockSpec(memory_space=pltpu.SMEM)


def call(kernel, name, ins, outs, scratch=()):
    values, specs = [], []
    for value, space in ins:
        if space is LOCAL:
            value = pltpu.with_memory_space_constraint(value, pltpu.VMEM)
        elif space is REMOTE:
            value = pltpu.with_memory_space_constraint(value, pltpu.HBM)
        values.append(value)
        specs.append(space)
    return pl.pallas_call(
        kernel,
        name=name,
        in_specs=specs,
        out_specs=[space for _, space in outs],
        out_shape=[
            jax.ShapeDtypeStruct((1,), jnp.int32)
            if space is FLAG
            else (pltpu.VMEM if space is LOCAL else jax.ShapeDtypeStruct)(shape, jnp.float32)
            for shape, space in outs
        ],
        scratch_shapes=list(scratch),
        compiler_params=pltpu.CompilerParams(vmem_limit_bytes=8 * 1024 * 1024),
    )(*values)


def room(*shape):
    return pltpu.VMEM(shape, jnp.float32)


def shards(
    pressure,
    vel_range,
    vel_depth,
    sound_speed,
    density,
    ahead_speed,
    ahead_density,
    shifts,
    sources,
    wavelet,
):
    height, breadth = pressure.shape
    extra = ahead_speed.shape[1]
    assert breadth == LANES and 2 * extra == LANES and height % 512 == 0
    arrays = [(x, REMOTE) for x in (pressure, vel_range, vel_depth, sound_speed, density)]
    ahead = [(x.T, REMOTE) for x in (ahead_speed, ahead_density)]
    small = [(shifts, REMOTE), (sources.T, REMOTE), (wavelet.T, REMOTE)]
    sizes = (shifts.shape, sources.shape[::-1], wavelet.shape[::-1])
    kinds = (jnp.int32, jnp.int32, jnp.float32)
    scalars = [pltpu.SMEM(size, kind) for size, kind in zip(sizes, kinds)]
    scalars.append(pltpu.SemaphoreType.DMA((3,)))
    field = (height, LANES)
    dma = pltpu.SemaphoreType.DMA

    found = call(
        functools.partial(own_kernel, height),
        "own",
        small + arrays + ahead,
        [((height - 2 * MARGIN, LANES), LOCAL)]
        + [((6 * TILE, LANES), LOCAL)] * 2
        + [(field, LOCAL)] * 5
        + [((ITERS, *field), LOCAL)] * 3
        + [(None, FLAG)],
        [room(*field)] * 3 + [room(2, LANES, LANES), dma((5,)), dma((2, 2))] + scalars,
    )
    tiles = height // BLOCKS // TILE + 2
    lean_rows = (tiles + (tiles - 2) // 4 + 1) * TILE
    n_edge = 6 * MARGIN
    n_wide = height + 2 * MARGIN
    n_strip = (tiles + 2) * TILE

    def finish(more, shifts, sources, wavelet, ahead, plane, to_up, to_down, *found):
        small = [(x, REMOTE) for x in (shifts, sources, wavelet)]
        ahead = [(x, REMOTE) for x in ahead]
        own = [(x, LOCAL) for x in found[:5]]
        stages = [(x, LOCAL) for x in found[5:8]]
        near = moved(plane, "range", -1)
        down = moved(to_up, "depth", -1)
        up = moved(to_down, "depth", 1)
        (lean,) = call(
            functools.partial(lean_kernel, height),
            "lean",
            own + stages,
            [((lean_rows, LANES), LOCAL)],
        )
        sides = [(up, LOCAL), (down, LOCAL)]
        edge, done = call(
            functools.partial(edge_kernel, height),
            "edge",
            small + own + sides + [(lean, LOCAL)],
            [((2 * MARGIN + lean_rows, LANES), LOCAL), ((3, 2 * MARGIN, LANES), LOCAL)],
            [room(n_edge, LANES)] * 3
            + [room(ITERS, n_edge, LANES)] * 3
            + [room(n_edge, LANES)] * 5
            + scalars,
        )
        edge_near = moved(edge, "range", -1)
        received = [near, edge_near]
        if more:
            (rest,) = call(
                functools.partial(rest_kernel, height, extra),
                "rest",
                stages + [(done, LOCAL)],
                [((height // 2, LANES), LOCAL)],
            )
            received.append(moved(rest, "range", -1))
        strip, wide = call(
            functools.partial(wide_kernel, height),
            "wide",
            small + own + ahead + sides,
            [((5, n_strip, LANES), LOCAL), ((3, n_wide, LANES), LOCAL)],
            [room(n_wide, LANES)] * 5 + [room(2, extra, height), dma((2,))] + scalars,
        )
        mixed = [(x, LOCAL) for x in (done, strip, wide, *received)]
        return tuple(
            call(
                functools.partial(last_kernel, height, extra, more),
                "last",
                small + stages + mixed,
                [(field, REMOTE)] * 3,
                [room(*field)] * 3
                + [room(n_strip, LANES)] * 10
                + [dma((3, BLOCKS))]
                + scalars,
            )
        )

    flag = found[-1].reshape(())
    return lax.cond(
        flag > 0,
        functools.partial(finish, True),
        functools.partial(finish, False),
        *[x for x, _ in small],
        [x for x, _ in ahead],
        *found[:-1],
    )


def solution(mesh):
    field = P("depth", "range")
    strip = P("depth", None)
    return jax.shard_map(
        shards,
        mesh=mesh,
        in_specs=(field,) * 5 + (strip,) * 2 + (P(),) * 3,
        out_specs=(field,) * 3,
        check_vma=False,
    )
```

```python
import functools

import jax
import jax.numpy as jnp
from jax import lax
from jax.experimental import pallas as pl
from jax.experimental.pallas import tpu as pltpu
from jax.sharding import PartitionSpec as P

ITERS = 4
TIME_STEP = 0.6
LANES = 128
TILE = 8
MARGIN = 16
SKEW = 4
WIDTH = 42
STRIP = 16
BLOCKS = LANES // STRIP
KEPT = LANES - STRIP // 2
BLOCK = 1024


def lane_ids(rows):
    return lax.broadcasted_iota(jnp.int32, (rows, LANES), 1)


def between(lanes, low, high):
    return jnp.logical_and(lanes >= low, lanes < high)


def roll(x, by):
    return pltpu.roll(x, by % LANES, 1)


def for_rows(start, stop, fn, size=BLOCK):
    whole = (stop - start) // size

    def step(i, carry):
        fn(pl.multiple_of(start + i * size, TILE), size)
        return carry

    if whole > 1:
        lax.fori_loop(0, whole, step, 0)
    elif whole == 1:
        fn(start, size)
    if start + whole * size < stop:
        fn(start + whole * size, stop - start - whole * size)


def offsets_of(shifts):
    found = [jnp.int32(0)]
    for t in range(ITERS):
        found.append(found[-1] + shifts[t])
    return found


def range_ends():
    place = lax.axis_index("range")
    return place == 0, place == lax.axis_size("range") - 1


def depth_ends():
    place = lax.axis_index("depth")
    return place == 0, place == lax.axis_size("depth") - 1


def set_coefs(start, stop, c, rho, ax, az, stiff):
    def coefs(r, k):
        here = pl.ds(r, k)
        dense = rho[here, :]
        ax[here, :] = (2.0 * TIME_STEP) / (dense + roll(dense, -1))
        az[here, :] = (2.0 * TIME_STEP) / (dense + rho[pl.ds(r + 1, k), :])
        if c is not None:
            speed = c[here, :]
            stiff[here, :] = TIME_STEP * (dense * speed * speed)

    for_rows(start, stop, coefs)


def find_sources(sources, first_row, places):
    found = []
    for k in range(sources.shape[1]):
        for row, lane, good in places(sources[0, k] - first_row, sources[1, k]):
            good = jnp.logical_and(good, jnp.logical_and(lane >= 0, lane < LANES))
            found.append((k, row, lane, good))
    return found


def inject(field, found, wavelet, t, reach=None):
    here_any = functools.reduce(jnp.logical_or, [good for _, _, _, good in found])

    @pl.when(here_any)
    def _():
        rows = lax.broadcasted_iota(jnp.int32, (TILE, LANES), 0)
        lanes = lane_ids(TILE)
        for k, row, lane, good in found:
            if reach is not None:
                good = jnp.logical_and(good, lane % STRIP <= reach)

            @pl.when(good)
            def _(k=k, row=row, lane=lane):
                at = pl.ds(pl.multiple_of((row // TILE) * TILE, TILE), TILE)
                here = jnp.logical_and(rows == row % TILE, lanes == lane)
                field[at, :] = field[at, :] + jnp.where(here, wavelet[t, k], 0.0)


def left_steps(n, fields, coefs, stages, shifts, found, wavelet):
    ax, az, stiff = coefs
    ps, us, ws = stages
    offsets = offsets_of(shifts)
    at_start, _ = range_ends()
    for t in range(ITERS):
        p, u, w = fields if t == 0 else (ps.at[t - 1], us.at[t - 1], ws.at[t - 1])
        u_new, w_new, p_new = us.at[t], ws.at[t], ps.at[t]
        wall = jnp.where(at_start, offsets[t], -1)

        def speeds(r, k):
            here = pl.ds(r, k)
            now = p[here, :]
            u_new[here, :] = u[here, :] - ax[here, :] * (roll(now, -1) - now)
            w_new[here, :] = w[here, :] - az[here, :] * (p[pl.ds(r + 1, k), :] - now)

        def press(r, k):
            here = pl.ds(r, k)
            fast = u_new[here, :]
            left = jnp.where(lane_ids(k) == wall, 0.0, roll(fast, 1))
            down = w_new[here, :] - w_new[pl.ds(r - 1, k), :]
            p_new[here, :] = p[here, :] - stiff[here, :] * ((fast - left) + down)

        for_rows(0, n - TILE, speeds)
        for_rows(TILE, n - TILE, press)
        inject(p_new, found, wavelet, t)


def slanted(here, p0, stages, stiff):
    ps, us, ws = stages
    lanes = lane_ids(TILE)

    def pick(parts):
        found = parts[-1]
        for t in range(len(parts) - 2, -1, -1):
            found = jnp.where(lanes <= t, parts[t], found)
        return found

    a = pick([p0[here, :]] + [ps[t, here, :] for t in range(ITERS - 1)])
    b = pick([us[t, here, :] for t in range(ITERS)])
    c = pick([ws[t, here, :] for t in range(ITERS)])
    found = jnp.where(lanes < 3 * SKEW, roll(c, 2 * SKEW), roll(stiff, 3 * SKEW))
    found = jnp.where(lanes < 2 * SKEW, roll(b, SKEW), found)
    return jnp.where(lanes < SKEW, a, found)


def packed(p, u, w):
    lanes = lane_ids(p.shape[0])
    found = jnp.where(
        between(lanes, SKEW, SKEW + 2 * WIDTH), roll(u, WIDTH), roll(w, 2 * WIDTH)
    )
    return jnp.where(between(lanes, SKEW, SKEW + WIDTH), p, found)


def finals(stages, here):
    return [stage[ITERS - 1, here, :] for stage in stages]


def own_kernel(height, *refs):
    arrays, ahead = refs[3:8], refs[8:10]
    plane, to_up, to_down = refs[10:13]
    own, stages, scalars, flag = refs[13:18], refs[18:21], refs[21:24], refs[24]
    ax, az, stiff, ends, sems, end_sems, scalar_sems = refs[25:]
    shifts, sources, wavelet = scalars
    order = (4, 3, 0, 1, 2)
    copies = {k: pltpu.make_async_copy(arrays[k], own[k], sems.at[k]) for k in order}
    for k in order:
        copies[k].start()
    scalar_copies = [
        pltpu.make_async_copy(refs[k], scalars[k], scalar_sems.at[k]) for k in range(3)
    ]
    for copy in scalar_copies:
        copy.start()
    end_copies = []
    for side, start in enumerate((0, height - LANES)):
        for f in range(2):
            copy = pltpu.make_async_copy(
                ahead[f].at[:, pl.ds(start, LANES)],
                ends.at[side, pl.ds(f * LANES // 2, LANES // 2), :],
                end_sems.at[side, f],
            )
            copy.start()
            end_copies.append(copy)
    p, u, w, c, rho = own

    def place(row, col):
        return [(row, col - lax.axis_index("range") * LANES, between(row, 0, height))]

    copies[4].wait()
    copies[3].wait()
    set_coefs(0, height - TILE, c, rho, ax, az, stiff)
    for copy in scalar_copies:
        copy.wait()
    flag[0] = jnp.where(offsets_of(shifts)[ITERS] > SKEW + WIDTH, 1, 0)
    found = find_sources(sources, lax.axis_index("depth") * height, place)
    for k in (0, 1, 2):
        copies[k].wait()
    left_steps(height, (p, u, w), (ax, az, stiff), stages, shifts, found, wavelet)

    def finish(r, k):
        plane[pl.ds(r - MARGIN, k), :] = packed(*finals(stages, pl.ds(r, k)))

    for_rows(MARGIN, height - MARGIN, finish)
    for copy in end_copies:
        copy.wait()
    for k in range(5):
        to_up[pl.ds(k * TILE, TILE), :] = own[k][pl.ds(0, TILE), :]
        to_down[pl.ds(k * TILE, TILE), :] = own[k][pl.ds(height - TILE, TILE), :]
    at = pl.ds(5 * TILE, TILE)
    to_up[at, :] = ends[0].T[:TILE]
    to_down[at, :] = ends[1].T[LANES - TILE :]


def own_stiff(own, here):
    speed = own[3][here, :]
    return TIME_STEP * (own[4][here, :] * speed * speed)


def lean_kernel(height, *refs):
    own, stages, lean = refs[:5], refs[5:8], refs[8]
    each = height // BLOCKS
    tiles = each // TILE + 2

    def tile(i, slot):
        lanes = lane_ids(TILE)
        found = rhos = None
        for b in range(BLOCKS):
            row = b * each + i * TILE - TILE
            if not isinstance(i, int):
                row = pl.multiple_of(row, TILE)
            elif row < 0 or row >= height:
                row = 0
            here = pl.ds(row, TILE)
            part = slanted(here, own[0], stages, own_stiff(own, here))
            part = roll(part, STRIP * b) if b else part
            dense = roll(own[4][here, :], 4 * BLOCKS * slot + SKEW * b)
            found = part if b == 0 else jnp.where(lanes < STRIP * b, found, part)
            rhos = dense if b == 0 else jnp.where(lanes < 4 * BLOCKS * slot + SKEW * b, rhos, dense)
        lean[pl.ds(i * TILE, TILE), :] = found
        return rhos

    def group_of(first, count, out):
        lanes = lane_ids(TILE)
        total = None
        for slot in range(count):
            rhos = tile(first + slot, slot)
            total = rhos if slot == 0 else jnp.where(lanes < 4 * BLOCKS * slot, total, rhos)
        lean[pl.ds((tiles + out) * TILE, TILE), :] = total

    groups = (tiles - 2) // 4

    def body(m, carry):
        group_of(1 + 4 * m, 4, m)
        return carry

    lax.fori_loop(0, groups, body, 0)
    lanes = lane_ids(TILE)
    total = jnp.where(lanes < 4 * BLOCKS, tile(0, 0), tile(tiles - 1, 1))
    lean[pl.ds((tiles + groups) * TILE, TILE), :] = total


def ghost_rows(up, down, k, last_own):
    at_top, at_bottom = depth_ends()
    at = pl.ds(k * TILE, TILE)
    above, below = up[at, :], down[at, :]
    if k == 4:
        above = jnp.where(at_top, 1.0, above)
        below = jnp.where(at_bottom, last_own, below)
    return above, below


def edge_kernel(height, *refs):
    shifts, sources, wavelet = refs[:3]
    own, up, down = refs[3:8], refs[8], refs[9]
    out, done = refs[10:12]
    ax, az, stiff = refs[12:15]
    stages, inner = refs[15:18], refs[18:23]
    seg = 3 * MARGIN
    n = 2 * seg
    low = height - 2 * MARGIN
    for k in range(5):
        filler = jnp.full((TILE, LANES), 1.0 if k == 4 else 0.0, jnp.float32)
        last_own = jnp.broadcast_to(own[k][pl.ds(height - 1, 1), :], (TILE, LANES))
        above, below = ghost_rows(up, down, k, last_own)
        inner[k][pl.ds(0, TILE), :] = filler
        inner[k][pl.ds(TILE, TILE), :] = above
        inner[k][pl.ds(2 * TILE, 2 * MARGIN), :] = own[k][pl.ds(0, 2 * MARGIN), :]
        inner[k][pl.ds(seg, 2 * MARGIN), :] = own[k][pl.ds(low, 2 * MARGIN), :]
        inner[k][pl.ds(n - 2 * TILE, TILE), :] = below
        inner[k][pl.ds(n - TILE, TILE), :] = filler
    p, u, w, c, rho = inner
    set_coefs(0, n - TILE, c, rho, ax, az, stiff)
    at_top, _ = depth_ends()
    at = pl.ds(TILE, TILE)
    az[at, :] = jnp.where(at_top, 0.0, az[at, :])

    def place(row, col):
        upper = between(row, -TILE, 2 * MARGIN)
        lower = between(row, low, height + TILE)
        local = jnp.where(upper, row + MARGIN, row - low + seg)
        lane = col - lax.axis_index("range") * LANES
        return [(local, lane, jnp.logical_or(upper, lower))]

    found = find_sources(sources, lax.axis_index("depth") * height, place)
    left_steps(n, (p, u, w), (ax, az, stiff), stages, shifts, found, wavelet)
    for side, start in enumerate((MARGIN, seg + MARGIN)):
        fields = finals(stages, pl.ds(start, MARGIN))
        there = pl.ds(side * MARGIN, MARGIN)
        out[there, :] = packed(*fields)
        for f in range(3):
            done[f, there, :] = fields[f]
    lanes = lane_ids(TILE)
    found = None
    for side, start in enumerate((TILE, seg + MARGIN)):
        for j in range(3):
            here = pl.ds(start + j * TILE, TILE)
            part = jnp.where(
                lanes < 4 * SKEW,
                slanted(here, p, stages, stiff[here, :]),
                roll(rho[here, :], 4 * SKEW),
            )
            lane = 5 * SKEW * (3 * side + j)
            part = roll(part, lane) if lane else part
            found = part if lane == 0 else jnp.where(lanes < lane, found, part)
    out[pl.ds(2 * MARGIN, TILE), :] = found


def rho_slot(i, tiles):
    if i == 0:
        return (tiles - 2) // 4, 0
    if i == tiles - 1:
        return (tiles - 2) // 4, 1
    return (i - 1) // 4, (i - 1) % 4


def wide_kernel(height, *refs):
    shifts, sources, wavelet = refs[:3]
    own, ahead, up, down = refs[3:8], refs[8:10], refs[10], refs[11]
    strip, out = refs[12:14]
    p, u, w = out.at[0], out.at[1], out.at[2]
    rho, ax, az, al, stiff, raw, sems = refs[14:]
    half = LANES // 2
    n = height + 2 * MARGIN
    at_top, at_bottom = depth_ends()
    _, at_end = range_ends()

    @pl.when(jnp.logical_not(at_end))
    def _():
        each = height // BLOCKS
        rows = each + 2 * TILE

        def put(i, k, parts):
            lanes = lane_ids(k)
            for a in range(5):
                found = None
                for b in range(BLOCKS):
                    part = roll(parts[b][a], STRIP * b - KEPT)
                    found = part if b == 0 else jnp.where(lanes < STRIP * b, found, part)
                strip[a, pl.ds(i + TILE, k), :] = found

        def fields(here):
            return [own[0][here, :], own[1][here, :], own[2][here, :], own_stiff(own, here), own[4][here, :]]

        def middle(i, k):
            put(i, k, [fields(pl.ds(b * each - TILE + i, k)) for b in range(BLOCKS)])

        for_rows(TILE, rows - TILE, middle, 32)
        above, below = [], []
        for k in range(5):
            last_own = jnp.broadcast_to(own[k][pl.ds(height - 1, 1), :], (TILE, LANES))
            one, two = ghost_rows(up, down, k, last_own)
            above.append(one)
            below.append(two)
        for parts in (above, below):
            parts[3] = TIME_STEP * (parts[4] * parts[3] * parts[3])
        inner = [fields(pl.ds(b * each - TILE, TILE)) for b in range(1, BLOCKS)]
        put(0, TILE, [above] + inner)
        inner = [fields(pl.ds((b + 1) * each, TILE)) for b in range(BLOCKS - 1)]
        put(rows - TILE, TILE, inner + [below])

    @pl.when(at_end)
    def _():
        copies = [pltpu.make_async_copy(ahead[f], raw.at[f], sems.at[f]) for f in range(2)]
        for copy in copies:
            copy.start()
        for copy in copies:
            copy.wait()

        def place_rows(e, k, parts, both):
            here = pl.ds(e, k)
            lanes = lane_ids(k)
            mine = lanes < half
            for ref, part in zip((p, u, w), parts):
                ref[here, :] = jnp.where(mine, roll(part, half), 0.0)
            dense = jnp.where(mine, roll(parts[4], half), both)
            speed = roll(jnp.where(mine, both, parts[3]), half)
            rho[here, :] = dense
            stiff[here, :] = TIME_STEP * (dense * speed * speed)

        for j in range(height // LANES):
            at = pl.ds(j * LANES, LANES)
            both = jnp.concatenate([raw[0, :, at], raw[1, :, at]], 0).T
            place_rows(j * LANES + MARGIN, LANES, [ref[at, :] for ref in own], both)
        above, below = [], []
        for k in range(5):
            last_own = jnp.broadcast_to(own[k][pl.ds(height - 1, 1), :], (TILE, LANES))
            one, two = ghost_rows(up, down, k, last_own)
            above.append(one)
            below.append(two)
        at = pl.ds(5 * TILE, TILE)
        lanes = lane_ids(TILE)
        one, two = up[at, :], down[at, :]
        last = jnp.broadcast_to(rho[pl.ds(height + MARGIN - 1, 1), :], (TILE, LANES))
        one = jnp.where(jnp.logical_and(at_top, lanes >= half), 1.0, one)
        two = jnp.where(jnp.logical_and(at_bottom, lanes >= half), last, two)
        place_rows(TILE, TILE, above, one)
        place_rows(height + MARGIN, TILE, below, two)
        for e in (0, n - TILE):
            here = pl.ds(e, TILE)
            for ref in (p, u, w, stiff):
                ref[here, :] = jnp.zeros((TILE, LANES), jnp.float32)
            rho[here, :] = jnp.ones((TILE, LANES), jnp.float32)
        set_coefs(0, n - TILE, None, rho, ax, az, None)

        def edge_coefs(r, k):
            al[pl.ds(r, k), :] = TIME_STEP / rho[pl.ds(r, k), :]

        for_rows(0, n - TILE, edge_coefs)
        at = pl.ds(TILE, TILE)
        az[at, :] = jnp.where(at_top, 0.0, az[at, :])

        def place(row, col):
            good = between(row, -TILE, height + TILE)
            return [(row + MARGIN, col - lax.axis_index("range") * LANES - half, good)]

        found = find_sources(sources, lax.axis_index("depth") * height, place)
        offsets = offsets_of(shifts)
        for t in range(ITERS):
            edge = half - 1 + offsets[t]

            def speeds(r, k):
                here = pl.ds(r, k)
                lanes = lane_ids(k)
                now = p[here, :]
                slope = jnp.where(lanes == edge, al[here, :], ax[here, :])
                slope = jnp.where(lanes > edge, 0.0, slope)
                u[here, :] = u[here, :] - slope * (roll(now, -1) - now)
                slope = jnp.where(lanes > edge, 0.0, az[here, :])
                w[here, :] = w[here, :] - slope * (p[pl.ds(r + 1, k), :] - now)

            def press(r, k):
                here = pl.ds(r, k)
                fast = u[here, :]
                down_ = w[here, :] - w[pl.ds(r - 1, k), :]
                hard = jnp.where(lane_ids(k) > edge, 0.0, stiff[here, :])
                p[here, :] = p[here, :] - hard * ((fast - roll(fast, 1)) + down_)

            for_rows(0, n - TILE, speeds)
            for_rows(TILE, n - TILE, press)
            inject(p, found, wavelet, t)


def rest_kernel(height, extra, *refs):
    stages, done, out = refs[:3], refs[3], refs[4]
    more = extra - SKEW - WIDTH
    start = SKEW + WIDTH
    half = height // 2

    def read(row, k):
        if isinstance(row, int) and row < MARGIN:
            return [done[f, pl.ds(row, k), :] for f in range(3)]
        if isinstance(row, int) and row >= height - MARGIN:
            return [done[f, pl.ds(row - height + 2 * MARGIN, k), :] for f in range(3)]
        return finals(stages, pl.ds(row, k))

    def join(fields):
        lanes = lane_ids(fields[0].shape[0])
        found = jnp.where(lanes < start + 2 * more, roll(fields[1], more), roll(fields[2], 2 * more))
        return jnp.where(lanes < start + more, fields[0], found)

    def beside(r, k):
        inner = between(lane_ids(k), start, start + 3 * more)
        out[pl.ds(r, k), :] = jnp.where(inner, join(read(r, k)), roll(join(read(r + half, k)), LANES // 2))

    beside(0, MARGIN)
    for_rows(MARGIN, half - MARGIN, beside, 96)
    beside(half - MARGIN, MARGIN)


def mid_kernel(height, *refs):
    shifts, stages, done, wide, near = refs[0], refs[1:4], refs[4], refs[5], refs[6]
    built = refs[7:]
    _, at_end = range_ends()
    total = offsets_of(shifts)[ITERS]
    turn = LANES - total
    inside = (MARGIN, height - MARGIN)

    @pl.when(jnp.logical_not(at_end))
    def _():
        def build(r, k):
            got = near[pl.ds(r - MARGIN, k), :]
            theirs = between(lane_ids(k), SKEW, total)
            for f in range(3):
                mine = stages[f][ITERS - 1, pl.ds(r, k), :]
                other = roll(got, -WIDTH * f) if f else got
                built[f][pl.ds(r, k), :] = pltpu.roll(jnp.where(theirs, other, mine), turn, 1)

        for_rows(*inside, build)

    @pl.when(at_end)
    def _():
        def build(r, k):
            lanes = lane_ids(k)
            inner = jnp.logical_and(lanes >= total, lanes < KEPT + SKEW)
            for f in range(3):
                part = roll(wide[f, pl.ds(r + MARGIN, k), :], LANES // 2)
                if inside[0] <= r < inside[1]:
                    mine = stages[f][ITERS - 1, pl.ds(r, k), :]
                else:
                    mine = done[f, pl.ds(0 if r < MARGIN else MARGIN, k), :]
                built[f][pl.ds(r, k), :] = pltpu.roll(jnp.where(inner, mine, part), turn, 1)

        build(0, MARGIN)
        build(MARGIN, height - 2 * MARGIN)
        build(height - MARGIN, MARGIN)


def last_kernel(height, extra, far_too, *refs):
    shifts, sources, wavelet = refs[:3]
    done, strip, lean, edge = refs[3:7]
    drafts = refs[7:10]
    rest = refs[10] if far_too else None
    refs = refs[10 + far_too :]
    outs, built = refs[:3], refs[3:6]
    p, u, w, rho, ax, az, stiff, gp, gu, gw, sems = refs[6:]
    at_top, _ = depth_ends()
    _, at_end = range_ends()
    each = height // BLOCKS
    tiles = each // TILE + 2
    n = (tiles + 2) * TILE
    half = LANES // 2
    own_part = STRIP // 2
    total = offsets_of(shifts)[ITERS]
    more = extra - SKEW - WIDTH
    start = SKEW + WIDTH
    turn = LANES - total

    @pl.when(at_end)
    def _():
        copies = [pltpu.make_async_copy(drafts[f], outs[f], sems.at[f, 0]) for f in range(3)]
        for copy in copies:
            copy.start()
        for copy in copies:
            copy.wait()

    @pl.when(jnp.logical_not(at_end))
    def _():
        lanes = lane_ids(TILE)
        inner = lanes % STRIP
        mine, ghost = inner < own_part, inner < own_part + SKEW
        fill = [0.0, 0.0, 0.0, 0.0, 1.0]
        six = edge[pl.ds(2 * MARGIN, TILE), :]
        for i in range(tiles):
            here = pl.ds((i + 1) * TILE, TILE)
            pack = lean[pl.ds(i * TILE, TILE), :]
            group, slot = rho_slot(i, tiles)
            dense = lean[pl.ds((tiles + group) * TILE, TILE), :]
            origin = 4 * BLOCKS * slot + SKEW * (lanes // STRIP) + inner - own_part
            theirs = jnp.take_along_axis(dense, jnp.clip(origin, 0, LANES - 1), 1)
            parts = [roll(pack, own_part - SKEW * g) if g != 2 else pack for g in range(4)]
            parts.append(theirs)
            late = None
            if i < 3:
                late, lane, b = 5 * SKEW * i, own_part, 0
            elif i >= tiles - 3:
                late, lane, b = 5 * SKEW * (i - tiles + 6), STRIP * (BLOCKS - 1) + own_part, BLOCKS - 1
            if late is not None:
                block = between(lanes, STRIP * b, STRIP * (b + 1))
                parts = [
                    jnp.where(block, roll(six, lane - late - SKEW * g), part)
                    for g, part in enumerate(parts)
                ]
            for ref, part in zip((gp, gu, gw), parts):
                ref[here, :] = part
            for a, (ref, part) in enumerate(zip((p, u, w, stiff, rho), parts)):
                other = jnp.where(ghost, part, fill[a])
                ref[here, :] = jnp.where(mine, strip[a, here, :], other)
        for e in (0, n - TILE):
            here = pl.ds(e, TILE)
            for ref in (p, u, w, stiff):
                ref[here, :] = jnp.zeros((TILE, LANES), jnp.float32)
            rho[here, :] = jnp.ones((TILE, LANES), jnp.float32)
        set_coefs(TILE, n - TILE, None, rho, ax, az, None)
        at = pl.ds(TILE, TILE)
        az[at, :] = jnp.where(jnp.logical_and(at_top, lane_ids(TILE) < STRIP), 0.0, az[at, :])

        def place(row, col):
            col = col - lax.axis_index("range") * LANES - KEPT
            inside = between(col, 0, STRIP)
            inside = jnp.logical_and(inside, between(row, -TILE, height + TILE))
            b = (row + TILE) // each
            local = row + TILE - b * each
            one = jnp.logical_and(inside, b < BLOCKS)
            two = jnp.logical_and(inside, jnp.logical_and(b > 0, local < 2 * TILE))
            return [
                (local + TILE, STRIP * b + col, one),
                (local + each + TILE, STRIP * (b - 1) + col, two),
            ]

        found = find_sources(sources, lax.axis_index("depth") * height, place)
        for t in range(ITERS):
            taken = own_part + t

            def speeds(r, k):
                here = pl.ds(r, k)
                inner = lane_ids(k) % STRIP
                now = p[here, :]
                fast = u[here, :] - ax[here, :] * (roll(now, -1) - now)
                u[here, :] = jnp.where(inner == taken, gu[here, :], fast)
                deep = w[here, :] - az[here, :] * (p[pl.ds(r + 1, k), :] - now)
                w[here, :] = jnp.where(inner == taken, gw[here, :], deep)

            def press(r, k):
                here = pl.ds(r, k)
                inner = lane_ids(k) % STRIP
                fast = u[here, :]
                down_ = w[here, :] - w[pl.ds(r - 1, k), :]
                new = p[here, :] - stiff[here, :] * ((fast - roll(fast, 1)) + down_)
                if t < ITERS - 1:
                    new = jnp.where(inner == taken + 1, gp[here, :], new)
                p[here, :] = new

            for_rows(TILE, n - TILE, speeds)
            for_rows(TILE, n - TILE, press)
            inject(p, found, wavelet, t, taken)

        copies = []
        for b in range(BLOCKS):
            first = b * each
            low, high = first, first + each
            edges = []
            if b == 0:
                low = MARGIN
                edges = [(0, 0)]
            if b == BLOCKS - 1:
                high = height - MARGIN
                edges = [(high, MARGIN)]

            def far_values(row, k):
                if row < height // 2:
                    return rest[pl.ds(row, k), :]
                return roll(rest[pl.ds(row - height // 2, k), :], half)

            for row, side in edges:
                here, there = pl.ds(row, MARGIN), pl.ds(side, MARGIN)
                lanes = lane_ids(MARGIN)
                for f, ref in enumerate((p, u, w)):
                    part = roll(ref[pl.ds(row - first + 2 * TILE, MARGIN), :], KEPT - STRIP * b)
                    kept = jnp.where(between(lanes, SKEW, KEPT + SKEW), done[f, there, :], part)
                    other = edge[there, :]
                    other = roll(other, -WIDTH * f) if f else other
                    if far_too:
                        far = far_values(row, MARGIN)
                        far = roll(far, -more * f) if f else far
                        other = jnp.where(lanes < start, other, far)
                    kept = jnp.where(between(lanes, SKEW, total), other, kept)
                    built[f][here, :] = pltpu.roll(kept, turn, 1)
            here, k = pl.ds(low, high - low), high - low
            natural = (lane_ids(k) + total) % LANES
            ready = between(natural, SKEW, KEPT + SKEW)
            shift = (KEPT - STRIP * b + LANES + turn) % LANES
            for f, ref in enumerate((p, u, w)):
                part = pltpu.roll(ref[pl.ds(low - first + 2 * TILE, k), :], shift, 1)
                kept = jnp.where(ready, drafts[f][here, :], part)
                if far_too:
                    far = pltpu.roll(far_values(low, k), (turn + LANES - more * f) % LANES, 1)
                    kept = jnp.where(between(natural, start, total), far, kept)
                built[f][here, :] = kept
            for f in range(3):
                at = pl.ds(first, each)
                copy = pltpu.make_async_copy(built[f].at[at, :], outs[f].at[at, :], sems.at[f, b])
                copy.start()
                copies.append(copy)
        for copy in copies:
            copy.wait()


def moved(x, axis, by):
    size = lax.axis_size(axis)
    pairs = [(i, i + by) for i in range(size) if 0 <= i + by < size]
    return lax.ppermute(x, axis, pairs)


LOCAL = pl.BlockSpec(memory_space=pltpu.VMEM)
REMOTE = pl.BlockSpec(memory_space=pl.ANY)
SCALAR = pl.BlockSpec(memory_space=pltpu.SMEM)


def shaped(shape, space):
    if space is SCALAR:
        return pltpu.SMEM(*shape)
    if space is LOCAL:
        return pltpu.VMEM(shape, jnp.float32)
    return jax.ShapeDtypeStruct(shape, jnp.float32)


def call(kernel, ins, outs, scratch=()):
    values, specs = [], []
    for value, space in ins:
        if space is LOCAL:
            value = pltpu.with_memory_space_constraint(value, pltpu.VMEM)
        elif space is SCALAR:
            value = pltpu.with_memory_space_constraint(value, pltpu.SMEM)
        elif space is REMOTE:
            value = pltpu.with_memory_space_constraint(value, pltpu.HBM)
        values.append(value)
        specs.append(space)
    return pl.pallas_call(
        kernel,
        in_specs=specs,
        out_specs=[space for _, space in outs],
        out_shape=[shaped(*pair) for pair in outs],
        scratch_shapes=list(scratch),
        compiler_params=pltpu.CompilerParams(vmem_limit_bytes=8 * 1024 * 1024),
    )(*values)


def room(*shape):
    return pltpu.VMEM(shape, jnp.float32)


def shards(
    pressure,
    vel_range,
    vel_depth,
    sound_speed,
    density,
    ahead_speed,
    ahead_density,
    shifts,
    sources,
    wavelet,
):
    height, breadth = pressure.shape
    extra = ahead_speed.shape[1]
    assert breadth == LANES and 2 * extra == LANES and height % 512 == 0
    arrays = [(x, REMOTE) for x in (pressure, vel_range, vel_depth, sound_speed, density)]
    ahead = [(x.T, REMOTE) for x in (ahead_speed, ahead_density)]
    small = [(shifts, REMOTE), (sources.T, REMOTE), (wavelet.T, REMOTE)]
    sizes = (shifts.shape, sources.shape[::-1], wavelet.shape[::-1])
    kinds = (jnp.int32, jnp.int32, jnp.float32)
    scalars = [(pair, SCALAR) for pair in zip(sizes, kinds)]
    field = (height, LANES)
    dma = pltpu.SemaphoreType.DMA

    found = call(
        functools.partial(own_kernel, height),
        small + arrays + ahead,
        [((height - 2 * MARGIN, LANES), LOCAL)]
        + [((6 * TILE, LANES), LOCAL)] * 2
        + [(field, LOCAL)] * 5
        + [((ITERS, *field), LOCAL)] * 3
        + scalars
        + [(((1,), jnp.int32), SCALAR)],
        [room(*field)] * 3 + [room(2, LANES, LANES), dma((5,)), dma((2, 2)), dma((3,))],
    )
    tiles = height // BLOCKS // TILE + 2
    lean_rows = (tiles + (tiles - 2) // 4 + 1) * TILE
    n_edge = 6 * MARGIN
    n_wide = height + 2 * MARGIN
    n_strip = (tiles + 2) * TILE

    def finish(more, ahead, plane, to_up, to_down, *found):
        ahead = [(x, REMOTE) for x in ahead]
        own = [(x, LOCAL) for x in found[:5]]
        stages = [(x, LOCAL) for x in found[5:8]]
        small = [(x, SCALAR) for x in found[8:]]
        near = moved(plane, "range", -1)
        down = moved(to_up, "depth", -1)
        up = moved(to_down, "depth", 1)
        (lean,) = call(
            functools.partial(lean_kernel, height), own + stages, [((lean_rows, LANES), LOCAL)]
        )
        lean_near = moved(lean, "range", -1)
        sides = [(up, LOCAL), (down, LOCAL)]
        edge, done = call(
            functools.partial(edge_kernel, height),
            small + own + sides,
            [((2 * MARGIN + TILE, LANES), LOCAL), ((3, 2 * MARGIN, LANES), LOCAL)],
            [room(n_edge, LANES)] * 3
            + [room(ITERS, n_edge, LANES)] * 3
            + [room(n_edge, LANES)] * 5,
        )
        edge_near = moved(edge, "range", -1)
        received = []
        if more:
            (rest,) = call(
                functools.partial(rest_kernel, height, extra),
                stages + [(done, LOCAL)],
                [((height // 2, LANES), LOCAL)],
            )
            received = [(moved(rest, "range", -1), LOCAL)]
        strip, wide = call(
            functools.partial(wide_kernel, height),
            small + own + ahead + sides,
            [((5, n_strip, LANES), LOCAL), ((3, n_wide, LANES), LOCAL)],
            [room(n_wide, LANES)] * 5 + [room(2, extra, height), dma((2,))],
        )
        drafts = call(
            functools.partial(mid_kernel, height),
            small[:1] + stages + [(x, LOCAL) for x in (done, wide, near)],
            [(field, LOCAL)] * 3,
        )
        mixed = [(x, LOCAL) for x in (done, strip, lean_near, edge_near, *drafts)]
        return tuple(
            call(
                functools.partial(last_kernel, height, extra, more),
                small + mixed + received,
                [(field, REMOTE)] * 3,
                [room(*field)] * 3 + [room(n_strip, LANES)] * 10 + [dma((3, BLOCKS))],
            )
        )

    return lax.cond(
        found[-1].reshape(()) > 0,
        functools.partial(finish, True),
        functools.partial(finish, False),
        [x for x, _ in ahead],
        *found[:-1],
    )


def solution(mesh):
    field = P("depth", "range")
    strip = P("depth", None)
    return jax.shard_map(
        shards,
        mesh=mesh,
        in_specs=(field,) * 5 + (strip,) * 2 + (P(),) * 3,
        out_specs=(field,) * 3,
        check_vma=False,
    )
```

```python
import functools

import jax
import jax.numpy as jnp
from jax import lax
from jax.experimental import pallas as pl
from jax.experimental.pallas import tpu as pltpu
from jax.sharding import PartitionSpec as P

ITERS = 4
TIME_STEP = 0.6
LANES = 128
TILE = 8
MARGIN = 16
SKEW = 4
WIDTH = 42
STRIP = 16
BLOCKS = LANES // STRIP
KEPT = LANES - STRIP // 2
BLOCK = 1024


def lane_ids(rows):
    return lax.broadcasted_iota(jnp.int32, (rows, LANES), 1)


def between(lanes, low, high):
    return jnp.logical_and(lanes >= low, lanes < high)


def roll(x, by):
    return pltpu.roll(x, by % LANES, 1)


def for_rows(start, stop, fn, size=BLOCK):
    whole = (stop - start) // size

    def step(i, carry):
        fn(pl.multiple_of(start + i * size, TILE), size)
        return carry

    if whole > 1:
        lax.fori_loop(0, whole, step, 0)
    elif whole == 1:
        fn(start, size)
    if start + whole * size < stop:
        fn(start + whole * size, stop - start - whole * size)


def offsets_of(shifts):
    found = [jnp.int32(0)]
    for t in range(ITERS):
        found.append(found[-1] + shifts[t])
    return found


def range_ends():
    place = lax.axis_index("range")
    return place == 0, place == lax.axis_size("range") - 1


def depth_ends():
    place = lax.axis_index("depth")
    return place == 0, place == lax.axis_size("depth") - 1


def set_coefs(start, stop, c, rho, ax, az, stiff):
    def coefs(r, k):
        here = pl.ds(r, k)
        dense = rho[here, :]
        ax[here, :] = (2.0 * TIME_STEP) / (dense + roll(dense, -1))
        az[here, :] = (2.0 * TIME_STEP) / (dense + rho[pl.ds(r + 1, k), :])
        if c is not None:
            speed = c[here, :]
            stiff[here, :] = TIME_STEP * (dense * speed * speed)

    for_rows(start, stop, coefs)


def find_sources(sources, first_row, places):
    found = []
    for k in range(sources.shape[1]):
        for row, lane, good in places(sources[0, k] - first_row, sources[1, k]):
            good = jnp.logical_and(good, jnp.logical_and(lane >= 0, lane < LANES))
            found.append((k, row, lane, good))
    return found


def inject(field, found, wavelet, t, reach=None):
    here_any = functools.reduce(jnp.logical_or, [good for _, _, _, good in found])

    @pl.when(here_any)
    def _():
        rows = lax.broadcasted_iota(jnp.int32, (TILE, LANES), 0)
        lanes = lane_ids(TILE)
        for k, row, lane, good in found:
            if reach is not None:
                good = jnp.logical_and(good, lane % STRIP <= reach)

            @pl.when(good)
            def _(k=k, row=row, lane=lane):
                at = pl.ds(pl.multiple_of((row // TILE) * TILE, TILE), TILE)
                here = jnp.logical_and(rows == row % TILE, lanes == lane)
                field[at, :] = field[at, :] + jnp.where(here, wavelet[t, k], 0.0)


def left_steps(n, fields, coefs, stages, shifts, found, wavelet):
    ax, az, stiff = coefs
    ps, us, ws = stages
    offsets = offsets_of(shifts)
    at_start, _ = range_ends()
    for t in range(ITERS):
        p, u, w = fields if t == 0 else (ps.at[t - 1], us.at[t - 1], ws.at[t - 1])
        u_new, w_new, p_new = us.at[t], ws.at[t], ps.at[t]
        wall = jnp.where(at_start, offsets[t], -1)

        def speeds(r, k):
            here = pl.ds(r, k)
            now = p[here, :]
            u_new[here, :] = u[here, :] - ax[here, :] * (roll(now, -1) - now)
            w_new[here, :] = w[here, :] - az[here, :] * (p[pl.ds(r + 1, k), :] - now)

        def press(r, k):
            here = pl.ds(r, k)
            fast = u_new[here, :]
            left = jnp.where(lane_ids(k) == wall, 0.0, roll(fast, 1))
            down = w_new[here, :] - w_new[pl.ds(r - 1, k), :]
            p_new[here, :] = p[here, :] - stiff[here, :] * ((fast - left) + down)

        for_rows(0, n - TILE, speeds)
        for_rows(TILE, n - TILE, press)
        inject(p_new, found, wavelet, t)


def slanted(here, p0, stages, stiff):
    ps, us, ws = stages
    lanes = lane_ids(TILE)

    def pick(parts):
        found = parts[-1]
        for t in range(len(parts) - 2, -1, -1):
            found = jnp.where(lanes <= t, parts[t], found)
        return found

    a = pick([p0[here, :]] + [ps[t, here, :] for t in range(ITERS - 1)])
    b = pick([us[t, here, :] for t in range(ITERS)])
    c = pick([ws[t, here, :] for t in range(ITERS)])
    found = jnp.where(lanes < 3 * SKEW, roll(c, 2 * SKEW), roll(stiff, 3 * SKEW))
    found = jnp.where(lanes < 2 * SKEW, roll(b, SKEW), found)
    return jnp.where(lanes < SKEW, a, found)


def packed(p, u, w):
    lanes = lane_ids(p.shape[0])
    found = jnp.where(
        between(lanes, SKEW, SKEW + 2 * WIDTH), roll(u, WIDTH), roll(w, 2 * WIDTH)
    )
    return jnp.where(between(lanes, SKEW, SKEW + WIDTH), p, found)


def finals(stages, here):
    return [stage[ITERS - 1, here, :] for stage in stages]


def own_kernel(height, *refs):
    arrays, ahead = refs[3:8], refs[8:10]
    plane, swap_one, swap_two = refs[10:13]
    own, stages, scalars, flag = refs[13:18], refs[18:21], refs[21:24], refs[24]
    ax, az, stiff, ends, sems, end_sems, scalar_sems = refs[25:]
    shifts, sources, wavelet = scalars
    order = (4, 3, 0, 1, 2)
    copies = {k: pltpu.make_async_copy(arrays[k], own[k], sems.at[k]) for k in order}
    for k in order:
        copies[k].start()
    scalar_copies = [
        pltpu.make_async_copy(refs[k], scalars[k], scalar_sems.at[k]) for k in range(3)
    ]
    for copy in scalar_copies:
        copy.start()
    end_copies = []
    for side, start in enumerate((0, height - LANES)):
        for f in range(2):
            copy = pltpu.make_async_copy(
                ahead[f].at[:, pl.ds(start, LANES)],
                ends.at[side, pl.ds(f * LANES // 2, LANES // 2), :],
                end_sems.at[side, f],
            )
            copy.start()
            end_copies.append(copy)
    p, u, w, c, rho = own

    def place(row, col):
        return [(row, col - lax.axis_index("range") * LANES, between(row, 0, height))]

    copies[4].wait()
    copies[3].wait()
    set_coefs(0, height - TILE, c, rho, ax, az, stiff)
    for copy in scalar_copies:
        copy.wait()
    flag[0] = jnp.where(offsets_of(shifts)[ITERS] > SKEW + WIDTH, 1, 0)
    found = find_sources(sources, lax.axis_index("depth") * height, place)
    for k in (0, 1, 2):
        copies[k].wait()
    left_steps(height, (p, u, w), (ax, az, stiff), stages, shifts, found, wavelet)

    def finish(r, k):
        plane[pl.ds(r - MARGIN, k), :] = packed(*finals(stages, pl.ds(r, k)))

    for_rows(MARGIN, height - MARGIN, finish)
    for copy in end_copies:
        copy.wait()
    even = lax.axis_index("depth") % 2 == 0
    tops = [own[k][pl.ds(0, TILE), :] for k in range(5)] + [ends[0].T[:TILE]]
    lows = [own[k][pl.ds(height - TILE, TILE), :] for k in range(5)] + [ends[1].T[LANES - TILE :]]
    for k, (top, low) in enumerate(zip(tops, lows)):
        at = pl.ds(k * TILE, TILE)
        swap_one[at, :] = jnp.where(even, low, top)
        swap_two[at, :] = jnp.where(even, top, low)


def own_stiff(own, here):
    speed = own[3][here, :]
    return TIME_STEP * (own[4][here, :] * speed * speed)


def lean_kernel(height, *refs):
    own, stages, lean = refs[:5], refs[5:8], refs[8]
    each = height // BLOCKS
    tiles = each // TILE + 2

    def tile(i, slot):
        lanes = lane_ids(TILE)
        found = rhos = None
        for b in range(BLOCKS):
            row = b * each + i * TILE - TILE
            if not isinstance(i, int):
                row = pl.multiple_of(row, TILE)
            elif row < 0 or row >= height:
                row = 0
            here = pl.ds(row, TILE)
            part = slanted(here, own[0], stages, own_stiff(own, here))
            part = roll(part, STRIP * b) if b else part
            dense = roll(own[4][here, :], 4 * BLOCKS * slot + SKEW * b)
            found = part if b == 0 else jnp.where(lanes < STRIP * b, found, part)
            rhos = dense if b == 0 else jnp.where(lanes < 4 * BLOCKS * slot + SKEW * b, rhos, dense)
        lean[pl.ds(i * TILE, TILE), :] = found
        return rhos

    def group_of(first, count, out):
        lanes = lane_ids(TILE)
        total = None
        for slot in range(count):
            rhos = tile(first + slot, slot)
            total = rhos if slot == 0 else jnp.where(lanes < 4 * BLOCKS * slot, total, rhos)
        lean[pl.ds((tiles + out) * TILE, TILE), :] = total

    groups = (tiles - 2) // 4

    def body(m, carry):
        group_of(1 + 4 * m, 4, m)
        return carry

    lax.fori_loop(0, groups, body, 0)
    lanes = lane_ids(TILE)
    total = jnp.where(lanes < 4 * BLOCKS, tile(0, 0), tile(tiles - 1, 1))
    lean[pl.ds((tiles + groups) * TILE, TILE), :] = total


def swapped_rows(one, two, k):
    at = pl.ds(k * TILE, TILE)
    even = lax.axis_index("depth") % 2 == 0
    first, second = one[at, :], two[at, :]
    return jnp.where(even, second, first), jnp.where(even, first, second)


def ghost_rows(one, two, k, last_own):
    at_top, at_bottom = depth_ends()
    above, below = swapped_rows(one, two, k)
    if k == 4:
        above = jnp.where(at_top, 1.0, above)
        below = jnp.where(at_bottom, last_own, below)
    return above, below


def edge_kernel(height, *refs):
    shifts, sources, wavelet = refs[:3]
    own, swap_one, swap_two, lean = refs[3:8], refs[8], refs[9], refs[10]
    out, done = refs[11:13]
    ax, az, stiff = refs[13:16]
    stages, inner = refs[16:19], refs[19:24]
    seg = 3 * MARGIN
    n = 2 * seg
    low = height - 2 * MARGIN
    for k in range(5):
        filler = jnp.full((TILE, LANES), 1.0 if k == 4 else 0.0, jnp.float32)
        last_own = jnp.broadcast_to(own[k][pl.ds(height - 1, 1), :], (TILE, LANES))
        above, below = ghost_rows(swap_one, swap_two, k, last_own)
        inner[k][pl.ds(0, TILE), :] = filler
        inner[k][pl.ds(TILE, TILE), :] = above
        inner[k][pl.ds(2 * TILE, 2 * MARGIN), :] = own[k][pl.ds(0, 2 * MARGIN), :]
        inner[k][pl.ds(seg, 2 * MARGIN), :] = own[k][pl.ds(low, 2 * MARGIN), :]
        inner[k][pl.ds(n - 2 * TILE, TILE), :] = below
        inner[k][pl.ds(n - TILE, TILE), :] = filler
    p, u, w, c, rho = inner
    set_coefs(0, n - TILE, c, rho, ax, az, stiff)
    at_top, _ = depth_ends()
    at = pl.ds(TILE, TILE)
    az[at, :] = jnp.where(at_top, 0.0, az[at, :])

    def place(row, col):
        upper = between(row, -TILE, 2 * MARGIN)
        lower = between(row, low, height + TILE)
        local = jnp.where(upper, row + MARGIN, row - low + seg)
        lane = col - lax.axis_index("range") * LANES
        return [(local, lane, jnp.logical_or(upper, lower))]

    found = find_sources(sources, lax.axis_index("depth") * height, place)
    left_steps(n, (p, u, w), (ax, az, stiff), stages, shifts, found, wavelet)
    for side, start in enumerate((MARGIN, seg + MARGIN)):
        fields = finals(stages, pl.ds(start, MARGIN))
        there = pl.ds(side * MARGIN, MARGIN)
        out[there, :] = packed(*fields)
        for f in range(3):
            done[f, there, :] = fields[f]
    lanes = lane_ids(TILE)
    found = None
    for side, start in enumerate((TILE, seg + MARGIN)):
        for j in range(3):
            here = pl.ds(start + j * TILE, TILE)
            part = jnp.where(
                lanes < 4 * SKEW,
                slanted(here, p, stages, stiff[here, :]),
                roll(rho[here, :], 4 * SKEW),
            )
            lane = 5 * SKEW * (3 * side + j)
            part = roll(part, lane) if lane else part
            found = part if lane == 0 else jnp.where(lanes < lane, found, part)
    out[pl.ds(2 * MARGIN, TILE), :] = found
    out[pl.ds(2 * MARGIN + TILE, lean.shape[0]), :] = lean[...]


def rho_slot(i, tiles):
    if i == 0:
        return (tiles - 2) // 4, 0
    if i == tiles - 1:
        return (tiles - 2) // 4, 1
    return (i - 1) // 4, (i - 1) % 4


def wide_kernel(height, *refs):
    shifts, sources, wavelet = refs[:3]
    own, ahead, swap_one, swap_two = refs[3:8], refs[8:10], refs[10], refs[11]
    strip, out = refs[12:14]
    p, u, w = out.at[0], out.at[1], out.at[2]
    rho, ax, az, al, stiff, raw, sems = refs[14:]
    half = LANES // 2
    n = height + 2 * MARGIN
    at_top, at_bottom = depth_ends()
    _, at_end = range_ends()

    @pl.when(jnp.logical_not(at_end))
    def _():
        each = height // BLOCKS
        rows = each + 2 * TILE

        def put(i, k, parts):
            lanes = lane_ids(k)
            for a in range(5):
                found = None
                for b in range(BLOCKS):
                    part = roll(parts[b][a], STRIP * b - KEPT)
                    found = part if b == 0 else jnp.where(lanes < STRIP * b, found, part)
                strip[a, pl.ds(i + TILE, k), :] = found

        def fields(here):
            return [own[0][here, :], own[1][here, :], own[2][here, :], own_stiff(own, here), own[4][here, :]]

        def middle(i, k):
            put(i, k, [fields(pl.ds(b * each - TILE + i, k)) for b in range(BLOCKS)])

        for_rows(TILE, rows - TILE, middle, 32)
        above, below = [], []
        for k in range(5):
            last_own = jnp.broadcast_to(own[k][pl.ds(height - 1, 1), :], (TILE, LANES))
            one, two = ghost_rows(swap_one, swap_two, k, last_own)
            above.append(one)
            below.append(two)
        for parts in (above, below):
            parts[3] = TIME_STEP * (parts[4] * parts[3] * parts[3])
        inner = [fields(pl.ds(b * each - TILE, TILE)) for b in range(1, BLOCKS)]
        put(0, TILE, [above] + inner)
        inner = [fields(pl.ds((b + 1) * each, TILE)) for b in range(BLOCKS - 1)]
        put(rows - TILE, TILE, inner + [below])

    @pl.when(at_end)
    def _():
        copies = [pltpu.make_async_copy(ahead[f], raw.at[f], sems.at[f]) for f in range(2)]
        for copy in copies:
            copy.start()
        for copy in copies:
            copy.wait()

        def place_rows(e, k, parts, both):
            here = pl.ds(e, k)
            lanes = lane_ids(k)
            mine = lanes < half
            for ref, part in zip((p, u, w), parts):
                ref[here, :] = jnp.where(mine, roll(part, half), 0.0)
            dense = jnp.where(mine, roll(parts[4], half), both)
            speed = roll(jnp.where(mine, both, parts[3]), half)
            rho[here, :] = dense
            stiff[here, :] = TIME_STEP * (dense * speed * speed)

        for j in range(height // LANES):
            at = pl.ds(j * LANES, LANES)
            both = jnp.concatenate([raw[0, :, at], raw[1, :, at]], 0).T
            place_rows(j * LANES + MARGIN, LANES, [ref[at, :] for ref in own], both)
        above, below = [], []
        for k in range(5):
            last_own = jnp.broadcast_to(own[k][pl.ds(height - 1, 1), :], (TILE, LANES))
            one, two = ghost_rows(swap_one, swap_two, k, last_own)
            above.append(one)
            below.append(two)
        lanes = lane_ids(TILE)
        one, two = swapped_rows(swap_one, swap_two, 5)
        last = jnp.broadcast_to(rho[pl.ds(height + MARGIN - 1, 1), :], (TILE, LANES))
        one = jnp.where(jnp.logical_and(at_top, lanes >= half), 1.0, one)
        two = jnp.where(jnp.logical_and(at_bottom, lanes >= half), last, two)
        place_rows(TILE, TILE, above, one)
        place_rows(height + MARGIN, TILE, below, two)
        for e in (0, n - TILE):
            here = pl.ds(e, TILE)
            for ref in (p, u, w, stiff):
                ref[here, :] = jnp.zeros((TILE, LANES), jnp.float32)
            rho[here, :] = jnp.ones((TILE, LANES), jnp.float32)
        set_coefs(0, n - TILE, None, rho, ax, az, None)

        def edge_coefs(r, k):
            al[pl.ds(r, k), :] = TIME_STEP / rho[pl.ds(r, k), :]

        for_rows(0, n - TILE, edge_coefs)
        at = pl.ds(TILE, TILE)
        az[at, :] = jnp.where(at_top, 0.0, az[at, :])

        def place(row, col):
            good = between(row, -TILE, height + TILE)
            return [(row + MARGIN, col - lax.axis_index("range") * LANES - half, good)]

        found = find_sources(sources, lax.axis_index("depth") * height, place)
        offsets = offsets_of(shifts)
        for t in range(ITERS):
            edge = half - 1 + offsets[t]

            def speeds(r, k):
                here = pl.ds(r, k)
                lanes = lane_ids(k)
                now = p[here, :]
                slope = jnp.where(lanes == edge, al[here, :], ax[here, :])
                slope = jnp.where(lanes > edge, 0.0, slope)
                u[here, :] = u[here, :] - slope * (roll(now, -1) - now)
                slope = jnp.where(lanes > edge, 0.0, az[here, :])
                w[here, :] = w[here, :] - slope * (p[pl.ds(r + 1, k), :] - now)

            def press(r, k):
                here = pl.ds(r, k)
                fast = u[here, :]
                down_ = w[here, :] - w[pl.ds(r - 1, k), :]
                hard = jnp.where(lane_ids(k) > edge, 0.0, stiff[here, :])
                p[here, :] = p[here, :] - hard * ((fast - roll(fast, 1)) + down_)

            for_rows(0, n - TILE, speeds)
            for_rows(TILE, n - TILE, press)
            inject(p, found, wavelet, t)


def rest_kernel(height, extra, *refs):
    stages, done, out = refs[:3], refs[3], refs[4]
    more = extra - SKEW - WIDTH
    start = SKEW + WIDTH
    half = height // 2

    def read(row, k):
        if isinstance(row, int) and row < MARGIN:
            return [done[f, pl.ds(row, k), :] for f in range(3)]
        if isinstance(row, int) and row >= height - MARGIN:
            return [done[f, pl.ds(row - height + 2 * MARGIN, k), :] for f in range(3)]
        return finals(stages, pl.ds(row, k))

    def join(fields):
        lanes = lane_ids(fields[0].shape[0])
        found = jnp.where(lanes < start + 2 * more, roll(fields[1], more), roll(fields[2], 2 * more))
        return jnp.where(lanes < start + more, fields[0], found)

    def beside(r, k):
        inner = between(lane_ids(k), start, start + 3 * more)
        out[pl.ds(r, k), :] = jnp.where(inner, join(read(r, k)), roll(join(read(r + half, k)), LANES // 2))

    beside(0, MARGIN)
    for_rows(MARGIN, half - MARGIN, beside, 96)
    beside(half - MARGIN, MARGIN)


def mid_kernel(height, *refs):
    shifts, stages, done, wide, near = refs[0], refs[1:4], refs[4], refs[5], refs[6]
    built = refs[7:]
    _, at_end = range_ends()
    total = offsets_of(shifts)[ITERS]
    turn = LANES - total
    inside = (MARGIN, height - MARGIN)

    @pl.when(jnp.logical_not(at_end))
    def _():
        def build(r, k):
            got = near[pl.ds(r - MARGIN, k), :]
            theirs = between(lane_ids(k), SKEW, total)
            for f in range(3):
                mine = stages[f][ITERS - 1, pl.ds(r, k), :]
                other = roll(got, -WIDTH * f) if f else got
                built[f][pl.ds(r, k), :] = pltpu.roll(jnp.where(theirs, other, mine), turn, 1)

        for_rows(*inside, build)

    @pl.when(at_end)
    def _():
        def build(r, k):
            lanes = lane_ids(k)
            inner = jnp.logical_and(lanes >= total, lanes < KEPT + SKEW)
            for f in range(3):
                part = roll(wide[f, pl.ds(r + MARGIN, k), :], LANES // 2)
                if inside[0] <= r < inside[1]:
                    mine = stages[f][ITERS - 1, pl.ds(r, k), :]
                else:
                    mine = done[f, pl.ds(0 if r < MARGIN else MARGIN, k), :]
                built[f][pl.ds(r, k), :] = pltpu.roll(jnp.where(inner, mine, part), turn, 1)

        build(0, MARGIN)
        build(MARGIN, height - 2 * MARGIN)
        build(height - MARGIN, MARGIN)


def last_kernel(height, extra, far_too, *refs):
    shifts, sources, wavelet = refs[:3]
    done, strip, edge = refs[3:6]
    lean = edge.at[pl.ds(2 * MARGIN + TILE, edge.shape[0] - 2 * MARGIN - TILE)]
    drafts = refs[6:9]
    rest = refs[9] if far_too else None
    refs = refs[9 + far_too :]
    outs, built = refs[:3], refs[3:6]
    p, u, w, rho, ax, az, stiff, gp, gu, gw, sems = refs[6:]
    at_top, _ = depth_ends()
    _, at_end = range_ends()
    each = height // BLOCKS
    tiles = each // TILE + 2
    n = (tiles + 2) * TILE
    half = LANES // 2
    own_part = STRIP // 2
    total = offsets_of(shifts)[ITERS]
    more = extra - SKEW - WIDTH
    start = SKEW + WIDTH
    turn = LANES - total

    @pl.when(at_end)
    def _():
        copies = [pltpu.make_async_copy(drafts[f], outs[f], sems.at[f, 0]) for f in range(3)]
        for copy in copies:
            copy.start()
        for copy in copies:
            copy.wait()

    @pl.when(jnp.logical_not(at_end))
    def _():
        lanes = lane_ids(TILE)
        inner = lanes % STRIP
        mine, ghost = inner < own_part, inner < own_part + SKEW
        fill = [0.0, 0.0, 0.0, 0.0, 1.0]
        six = edge[pl.ds(2 * MARGIN, TILE), :]
        for i in range(tiles):
            here = pl.ds((i + 1) * TILE, TILE)
            pack = lean[pl.ds(i * TILE, TILE), :]
            group, slot = rho_slot(i, tiles)
            dense = lean[pl.ds((tiles + group) * TILE, TILE), :]
            origin = 4 * BLOCKS * slot + SKEW * (lanes // STRIP) + inner - own_part
            theirs = jnp.take_along_axis(dense, jnp.clip(origin, 0, LANES - 1), 1)
            parts = [roll(pack, own_part - SKEW * g) if g != 2 else pack for g in range(4)]
            parts.append(theirs)
            late = None
            if i < 3:
                late, lane, b = 5 * SKEW * i, own_part, 0
            elif i >= tiles - 3:
                late, lane, b = 5 * SKEW * (i - tiles + 6), STRIP * (BLOCKS - 1) + own_part, BLOCKS - 1
            if late is not None:
                block = between(lanes, STRIP * b, STRIP * (b + 1))
                parts = [
                    jnp.where(block, roll(six, lane - late - SKEW * g), part)
                    for g, part in enumerate(parts)
                ]
            for ref, part in zip((gp, gu, gw), parts):
                ref[here, :] = part
            for a, (ref, part) in enumerate(zip((p, u, w, stiff, rho), parts)):
                other = jnp.where(ghost, part, fill[a])
                ref[here, :] = jnp.where(mine, strip[a, here, :], other)
        for e in (0, n - TILE):
            here = pl.ds(e, TILE)
            for ref in (p, u, w, stiff):
                ref[here, :] = jnp.zeros((TILE, LANES), jnp.float32)
            rho[here, :] = jnp.ones((TILE, LANES), jnp.float32)
        set_coefs(TILE, n - TILE, None, rho, ax, az, None)
        at = pl.ds(TILE, TILE)
        az[at, :] = jnp.where(jnp.logical_and(at_top, lane_ids(TILE) < STRIP), 0.0, az[at, :])

        def place(row, col):
            col = col - lax.axis_index("range") * LANES - KEPT
            inside = between(col, 0, STRIP)
            inside = jnp.logical_and(inside, between(row, -TILE, height + TILE))
            b = (row + TILE) // each
            local = row + TILE - b * each
            one = jnp.logical_and(inside, b < BLOCKS)
            two = jnp.logical_and(inside, jnp.logical_and(b > 0, local < 2 * TILE))
            return [
                (local + TILE, STRIP * b + col, one),
                (local + each + TILE, STRIP * (b - 1) + col, two),
            ]

        found = find_sources(sources, lax.axis_index("depth") * height, place)
        for t in range(ITERS):
            taken = own_part + t

            def speeds(r, k):
                here = pl.ds(r, k)
                inner = lane_ids(k) % STRIP
                now = p[here, :]
                fast = u[here, :] - ax[here, :] * (roll(now, -1) - now)
                u[here, :] = jnp.where(inner == taken, gu[here, :], fast)
                deep = w[here, :] - az[here, :] * (p[pl.ds(r + 1, k), :] - now)
                w[here, :] = jnp.where(inner == taken, gw[here, :], deep)

            def press(r, k):
                here = pl.ds(r, k)
                inner = lane_ids(k) % STRIP
                fast = u[here, :]
                down_ = w[here, :] - w[pl.ds(r - 1, k), :]
                new = p[here, :] - stiff[here, :] * ((fast - roll(fast, 1)) + down_)
                if t < ITERS - 1:
                    new = jnp.where(inner == taken + 1, gp[here, :], new)
                p[here, :] = new

            for_rows(TILE, n - TILE, speeds)
            for_rows(TILE, n - TILE, press)
            inject(p, found, wavelet, t, taken)

        copies = []
        for b in range(BLOCKS):
            first = b * each
            low, high = first, first + each
            edges = []
            if b == 0:
                low = MARGIN
                edges = [(0, 0)]
            if b == BLOCKS - 1:
                high = height - MARGIN
                edges = [(high, MARGIN)]

            def far_values(row, k):
                if row < height // 2:
                    return rest[pl.ds(row, k), :]
                return roll(rest[pl.ds(row - height // 2, k), :], half)

            for row, side in edges:
                here, there = pl.ds(row, MARGIN), pl.ds(side, MARGIN)
                lanes = lane_ids(MARGIN)
                for f, ref in enumerate((p, u, w)):
                    part = roll(ref[pl.ds(row - first + 2 * TILE, MARGIN), :], KEPT - STRIP * b)
                    kept = jnp.where(between(lanes, SKEW, KEPT + SKEW), done[f, there, :], part)
                    other = edge[there, :]
                    other = roll(other, -WIDTH * f) if f else other
                    if far_too:
                        far = far_values(row, MARGIN)
                        far = roll(far, -more * f) if f else far
                        other = jnp.where(lanes < start, other, far)
                    kept = jnp.where(between(lanes, SKEW, total), other, kept)
                    built[f][here, :] = pltpu.roll(kept, turn, 1)
            here, k = pl.ds(low, high - low), high - low
            natural = (lane_ids(k) + total) % LANES
            ready = between(natural, SKEW, KEPT + SKEW)
            shift = (KEPT - STRIP * b + LANES + turn) % LANES
            for f, ref in enumerate((p, u, w)):
                part = pltpu.roll(ref[pl.ds(low - first + 2 * TILE, k), :], shift, 1)
                kept = jnp.where(ready, drafts[f][here, :], part)
                if far_too:
                    far = pltpu.roll(far_values(low, k), (turn + LANES - more * f) % LANES, 1)
                    kept = jnp.where(between(natural, start, total), far, kept)
                built[f][here, :] = kept
            for f in range(3):
                at = pl.ds(first, each)
                copy = pltpu.make_async_copy(built[f].at[at, :], outs[f].at[at, :], sems.at[f, b])
                copy.start()
                copies.append(copy)
        for copy in copies:
            copy.wait()


def moved(x):
    return lax.ppermute(x, "range", [(i + 1, i) for i in range(lax.axis_size("range") - 1)])


def swapped(x, first):
    pairs = [(i, i + 1) for i in range(first, lax.axis_size("depth") - 1, 2)]
    return lax.ppermute(x, "depth", pairs + [(j, i) for i, j in pairs])


LOCAL = pl.BlockSpec(memory_space=pltpu.VMEM)
REMOTE = pl.BlockSpec(memory_space=pl.ANY)
SCALAR = pl.BlockSpec(memory_space=pltpu.SMEM)


def shaped(shape, space):
    if space is SCALAR:
        return pltpu.SMEM(*shape)
    if space is LOCAL:
        return pltpu.VMEM(shape, jnp.float32)
    return jax.ShapeDtypeStruct(shape, jnp.float32)


def call(kernel, ins, outs, scratch=()):
    values, specs = [], []
    for value, space in ins:
        if space is LOCAL:
            value = pltpu.with_memory_space_constraint(value, pltpu.VMEM)
        elif space is SCALAR:
            value = pltpu.with_memory_space_constraint(value, pltpu.SMEM)
        elif space is REMOTE:
            value = pltpu.with_memory_space_constraint(value, pltpu.HBM)
        values.append(value)
        specs.append(space)
    return pl.pallas_call(
        kernel,
        in_specs=specs,
        out_specs=[space for _, space in outs],
        out_shape=[shaped(*pair) for pair in outs],
        scratch_shapes=list(scratch),
        compiler_params=pltpu.CompilerParams(vmem_limit_bytes=8 * 1024 * 1024),
    )(*values)


def room(*shape):
    return pltpu.VMEM(shape, jnp.float32)


def shards(
    pressure,
    vel_range,
    vel_depth,
    sound_speed,
    density,
    ahead_speed,
    ahead_density,
    shifts,
    sources,
    wavelet,
):
    height, breadth = pressure.shape
    extra = ahead_speed.shape[1]
    assert breadth == LANES and 2 * extra == LANES and height % 512 == 0
    arrays = [(x, REMOTE) for x in (pressure, vel_range, vel_depth, sound_speed, density)]
    ahead = [(x.T, REMOTE) for x in (ahead_speed, ahead_density)]
    small = [(shifts, REMOTE), (sources.T, REMOTE), (wavelet.T, REMOTE)]
    sizes = (shifts.shape, sources.shape[::-1], wavelet.shape[::-1])
    kinds = (jnp.int32, jnp.int32, jnp.float32)
    scalars = [(pair, SCALAR) for pair in zip(sizes, kinds)]
    field = (height, LANES)
    dma = pltpu.SemaphoreType.DMA

    found = call(
        functools.partial(own_kernel, height),
        small + arrays + ahead,
        [((height - 2 * MARGIN, LANES), LOCAL)]
        + [((6 * TILE, LANES), LOCAL)] * 2
        + [(field, LOCAL)] * 5
        + [((ITERS, *field), LOCAL)] * 3
        + scalars
        + [(((1,), jnp.int32), SCALAR)],
        [room(*field)] * 3 + [room(2, LANES, LANES), dma((5,)), dma((2, 2)), dma((3,))],
    )
    tiles = height // BLOCKS // TILE + 2
    lean_rows = (tiles + (tiles - 2) // 4 + 1) * TILE
    n_edge = 6 * MARGIN
    n_wide = height + 2 * MARGIN
    n_strip = (tiles + 2) * TILE

    def finish(more, ahead, plane, swap_one, swap_two, *found):
        ahead = [(x, REMOTE) for x in ahead]
        own = [(x, LOCAL) for x in found[:5]]
        stages = [(x, LOCAL) for x in found[5:8]]
        small = [(x, SCALAR) for x in found[8:]]
        near = moved(plane)
        sides = [(swapped(swap_one, 0), LOCAL), (swapped(swap_two, 1), LOCAL)]
        (lean,) = call(
            functools.partial(lean_kernel, height), own + stages, [((lean_rows, LANES), LOCAL)]
        )
        edge, done = call(
            functools.partial(edge_kernel, height),
            small + own + sides + [(lean, LOCAL)],
            [((2 * MARGIN + TILE + lean_rows, LANES), LOCAL), ((3, 2 * MARGIN, LANES), LOCAL)],
            [room(n_edge, LANES)] * 3
            + [room(ITERS, n_edge, LANES)] * 3
            + [room(n_edge, LANES)] * 5,
        )
        edge_near = moved(edge)
        received = []
        if more:
            (rest,) = call(
                functools.partial(rest_kernel, height, extra),
                stages + [(done, LOCAL)],
                [((height // 2, LANES), LOCAL)],
            )
            received = [(moved(rest), LOCAL)]
        strip, wide = call(
            functools.partial(wide_kernel, height),
            small + own + ahead + sides,
            [((5, n_strip, LANES), LOCAL), ((3, n_wide, LANES), LOCAL)],
            [room(n_wide, LANES)] * 5 + [room(2, extra, height), dma((2,))],
        )
        drafts = call(
            functools.partial(mid_kernel, height),
            small[:1] + stages + [(x, LOCAL) for x in (done, wide, near)],
            [(field, LOCAL)] * 3,
        )
        mixed = [(x, LOCAL) for x in (done, strip, edge_near, *drafts)]
        return tuple(
            call(
                functools.partial(last_kernel, height, extra, more),
                small + mixed + received,
                [(field, REMOTE)] * 3,
                [room(*field)] * 3 + [room(n_strip, LANES)] * 10 + [dma((3, BLOCKS))],
            )
        )

    return lax.cond(
        found[-1].reshape(()) > 0,
        functools.partial(finish, True),
        functools.partial(finish, False),
        [x for x, _ in ahead],
        *found[:-1],
    )


def solution(mesh):
    field = P("depth", "range")
    strip = P("depth", None)
    return jax.shard_map(
        shards,
        mesh=mesh,
        in_specs=(field,) * 5 + (strip,) * 2 + (P(),) * 3,
        out_specs=(field,) * 3,
        check_vma=False,
    )
```

```python
import functools

import jax
import jax.numpy as jnp
from jax import lax
from jax.experimental import pallas as pl
from jax.experimental.pallas import tpu as pltpu
from jax.sharding import PartitionSpec as P

ITERS = 4
TIME_STEP = 0.6
LANES = 128
TILE = 8
MARGIN = 16
SKEW = 4
WIDTH = 42
NARROW = 32
START = SKEW + WIDTH
MORE = ((NARROW + SKEW, 0, 0), (START, 0, 0), (START + 10, 10, 4), (1 << 20, 18, 2))
STRIP = 16
BLOCKS = LANES // STRIP
KEPT = LANES - STRIP // 2
BLOCK = 1024


def lane_ids(rows):
    return lax.broadcasted_iota(jnp.int32, (rows, LANES), 1)


def between(lanes, low, high):
    return jnp.logical_and(lanes >= low, lanes < high)


def roll(x, by):
    return pltpu.roll(x, by % LANES, 1)


def for_rows(start, stop, fn, size=BLOCK):
    whole = (stop - start) // size

    def step(i, carry):
        fn(pl.multiple_of(start + i * size, TILE), size)
        return carry

    if whole > 1:
        lax.fori_loop(0, whole, step, 0)
    elif whole == 1:
        fn(start, size)
    if start + whole * size < stop:
        fn(start + whole * size, stop - start - whole * size)


def offsets_of(shifts):
    found = [jnp.int32(0)]
    for t in range(ITERS):
        found.append(found[-1] + shifts[t])
    return found


def range_ends():
    place = lax.axis_index("range")
    return place == 0, place == lax.axis_size("range") - 1


def depth_ends():
    place = lax.axis_index("depth")
    return place == 0, place == lax.axis_size("depth") - 1


def set_coefs(start, stop, c, rho, ax, az, stiff):
    def coefs(r, k):
        here = pl.ds(r, k)
        dense = rho[here, :]
        ax[here, :] = (2.0 * TIME_STEP) / (dense + roll(dense, -1))
        az[here, :] = (2.0 * TIME_STEP) / (dense + rho[pl.ds(r + 1, k), :])
        if c is not None:
            speed = c[here, :]
            stiff[here, :] = TIME_STEP * (dense * speed * speed)

    for_rows(start, stop, coefs)


def find_sources(sources, first_row, places):
    def candidates(k):
        found = []
        for row, lane, good in places(sources[0, k] - first_row, sources[1, k]):
            good = jnp.logical_and(good, between(lane, 0, LANES))
            found.append((row, lane, good))
        return found

    def look(k, seen):
        for _, _, good in candidates(k):
            seen = jnp.logical_or(seen, good)
        return seen

    return candidates, lax.fori_loop(0, sources.shape[1], look, jnp.bool_(False))


def inject(field, found, wavelet, t, reach=None):
    candidates, seen = found

    @pl.when(seen)
    def _():
        rows = lax.broadcasted_iota(jnp.int32, (TILE, LANES), 0)
        lanes = lane_ids(TILE)

        def add(k, carry):
            for row, lane, good in candidates(k):
                if reach is not None:
                    good = jnp.logical_and(good, lane % STRIP <= reach)

                @pl.when(good)
                def _(row=row, lane=lane):
                    at = pl.ds(pl.multiple_of((row // TILE) * TILE, TILE), TILE)
                    here = jnp.logical_and(rows == row % TILE, lanes == lane)
                    field[at, :] = field[at, :] + jnp.where(here, wavelet[t, k], 0.0)

            return carry

        lax.fori_loop(0, wavelet.shape[1], add, 0)


def left_steps(n, fields, coefs, stages, shifts, found, wavelet):
    ax, az, stiff = coefs
    ps, us, ws = stages
    offsets = offsets_of(shifts)
    at_start, _ = range_ends()
    for t in range(ITERS):
        p, u, w = fields if t == 0 else (ps[t - 1], us[t - 1], ws[t - 1])
        u_new, w_new, p_new = us[t], ws[t], ps[t]
        wall = jnp.where(at_start, offsets[t], -1)

        def speeds(r, k):
            here = pl.ds(r, k)
            now = p[here, :]
            u_new[here, :] = u[here, :] - ax[here, :] * (roll(now, -1) - now)
            w_new[here, :] = w[here, :] - az[here, :] * (p[pl.ds(r + 1, k), :] - now)

        def press(r, k):
            here = pl.ds(r, k)
            fast = u_new[here, :]
            left = jnp.where(lane_ids(k) == wall, 0.0, roll(fast, 1))
            down = w_new[here, :] - w_new[pl.ds(r - 1, k), :]
            p_new[here, :] = p[here, :] - stiff[here, :] * ((fast - left) + down)

        for_rows(0, n - TILE, speeds)
        for_rows(TILE, n - TILE, press)
        inject(p_new, found, wavelet, t)


def slanted(here, p0, stages, stiff):
    ps, us, ws = stages
    lanes = lane_ids(TILE)

    def pick(parts):
        found = parts[-1]
        for t in range(len(parts) - 2, -1, -1):
            found = jnp.where(lanes <= t, parts[t], found)
        return found

    a = pick([p0[here, :]] + [ps[t][here, :] for t in range(ITERS - 1)])
    b = pick([us[t][here, :] for t in range(ITERS)])
    c = pick([ws[t][here, :] for t in range(ITERS)])
    found = jnp.where(lanes < 3 * SKEW, roll(c, 2 * SKEW), roll(stiff, 3 * SKEW))
    found = jnp.where(lanes < 2 * SKEW, roll(b, SKEW), found)
    return jnp.where(lanes < SKEW, a, found)


def packed(p, u, w, width=WIDTH):
    lanes = lane_ids(p.shape[0])
    found = jnp.where(
        between(lanes, SKEW, SKEW + 2 * width), roll(u, width), roll(w, 2 * width)
    )
    return jnp.where(between(lanes, SKEW, SKEW + width), p, found)


def finals(stages, here):
    return [stage[-1][here, :] for stage in stages]


def staged(early, final):
    return [[a.at[t] for t in range(ITERS - 1)] + [b] for a, b in zip(early, final)]


def own_kernel(height, *refs):
    arrays, ahead = refs[3:8], refs[8:10]
    swap_one, swap_two = refs[10:12]
    own, stages, scalars = refs[12:17], staged(refs[17:20], refs[20:23]), refs[23:26]
    flag, ax, az, stiff, ends, sems, end_sems, scalar_sems = refs[26:]
    shifts, sources, wavelet = scalars
    order = (4, 3, 0, 1, 2)
    copies = {k: pltpu.make_async_copy(arrays[k], own[k], sems.at[k]) for k in order}
    for k in order:
        copies[k].start()
    scalar_copies = [
        pltpu.make_async_copy(refs[k], scalars[k], scalar_sems.at[k]) for k in range(3)
    ]
    for copy in scalar_copies:
        copy.start()
    end_copies = []
    for side, start in enumerate((0, height - LANES)):
        for f in range(2):
            copy = pltpu.make_async_copy(
                ahead[f].at[:, pl.ds(start, LANES)],
                ends.at[side, pl.ds(f * LANES // 2, LANES // 2), :],
                end_sems.at[side, f],
            )
            copy.start()
            end_copies.append(copy)
    p, u, w, c, rho = own

    def place(row, col):
        return [(row, col - lax.axis_index("range") * LANES, between(row, 0, height))]

    copies[4].wait()
    copies[3].wait()
    set_coefs(0, height - TILE, c, rho, ax, az, stiff)
    for copy in scalar_copies:
        copy.wait()
    total = offsets_of(shifts)[ITERS]
    kind = jnp.int32(0)
    for limit, _, _ in MORE[:-1]:
        kind = kind + jnp.where(total > limit, 1, 0)
    flag[0] = kind
    found = find_sources(sources, lax.axis_index("depth") * height, place)
    for k in (0, 1, 2):
        copies[k].wait()
    left_steps(height, (p, u, w), (ax, az, stiff), stages, shifts, found, wavelet)

    for copy in end_copies:
        copy.wait()
    even = lax.axis_index("depth") % 2 == 0
    tops = [own[k][pl.ds(0, TILE), :] for k in range(5)] + [ends[0].T[:TILE]]
    lows = [own[k][pl.ds(height - TILE, TILE), :] for k in range(5)] + [ends[1].T[LANES - TILE :]]
    for k, (top, low) in enumerate(zip(tops, lows)):
        at = pl.ds(k * TILE, TILE)
        swap_one[at, :] = jnp.where(even, low, top)
        swap_two[at, :] = jnp.where(even, top, low)


def pack_kernel(height, low, *refs):
    stages, plane = [[ref] for ref in refs[:3]], refs[3]
    if not low:

        def finish(r, k):
            plane[pl.ds(r - MARGIN, k), :] = packed(*finals(stages, pl.ds(r, k)))

        for_rows(MARGIN, height - MARGIN, finish)
        return
    each = (height - 2 * MARGIN) // 4
    inner = between(lane_ids(each), SKEW, SKEW + 3 * NARROW)
    spread = finals(stages, pl.ds(MARGIN + 3 * each, each))
    for b in range(3):
        part = packed(*finals(stages, pl.ds(MARGIN + b * each, each)), NARROW)
        plane[pl.ds(b * each, each), :] = jnp.where(inner, part, roll(spread[b], 3 * NARROW))


def own_stiff(own, here):
    speed = own[3][here, :]
    return TIME_STEP * (own[4][here, :] * speed * speed)


def lean_kernel(height, *refs):
    own, stages, lean = refs[:5], staged(refs[5:8], refs[8:11]), refs[11]
    each = height // BLOCKS
    tiles = each // TILE + 2

    def tile(i, slot):
        lanes = lane_ids(TILE)
        found = rhos = None
        for b in range(BLOCKS):
            row = b * each + i * TILE - TILE
            if not isinstance(i, int):
                row = pl.multiple_of(row, TILE)
            elif row < 0 or row >= height:
                row = 0
            here = pl.ds(row, TILE)
            part = slanted(here, own[0], stages, own_stiff(own, here))
            part = roll(part, STRIP * b) if b else part
            dense = roll(own[4][here, :], 4 * BLOCKS * slot + SKEW * b)
            found = part if b == 0 else jnp.where(lanes < STRIP * b, found, part)
            rhos = dense if b == 0 else jnp.where(lanes < 4 * BLOCKS * slot + SKEW * b, rhos, dense)
        lean[pl.ds(i * TILE, TILE), :] = found
        return rhos

    def group_of(first, count, out):
        lanes = lane_ids(TILE)
        total = None
        for slot in range(count):
            rhos = tile(first + slot, slot)
            total = rhos if slot == 0 else jnp.where(lanes < 4 * BLOCKS * slot, total, rhos)
        lean[pl.ds((tiles + out) * TILE, TILE), :] = total

    groups = (tiles - 2) // 4

    def body(m, carry):
        group_of(1 + 4 * m, 4, m)
        return carry

    lax.fori_loop(0, groups, body, 0)
    lanes = lane_ids(TILE)
    total = jnp.where(lanes < 4 * BLOCKS, tile(0, 0), tile(tiles - 1, 1))
    lean[pl.ds((tiles + groups) * TILE, TILE), :] = total


def swapped_rows(one, two, k):
    at = pl.ds(k * TILE, TILE)
    even = lax.axis_index("depth") % 2 == 0
    first, second = one[at, :], two[at, :]
    return jnp.where(even, second, first), jnp.where(even, first, second)


def ghost_rows(one, two, k, last_own):
    at_top, at_bottom = depth_ends()
    above, below = swapped_rows(one, two, k)
    if k == 4:
        above = jnp.where(at_top, 1.0, above)
        below = jnp.where(at_bottom, last_own, below)
    return above, below


def edge_kernel(height, *refs):
    shifts, sources, wavelet = refs[:3]
    own, swap_one, swap_two, lean = refs[3:8], refs[8], refs[9], refs[10]
    out, done = refs[11:13]
    ax, az, stiff = refs[13:16]
    stages, inner = staged(refs[16:19], refs[19:22]), refs[22:27]
    seg = 3 * MARGIN
    n = 2 * seg
    low = height - 2 * MARGIN
    for k in range(5):
        filler = jnp.full((TILE, LANES), 1.0 if k == 4 else 0.0, jnp.float32)
        last_own = jnp.broadcast_to(own[k][pl.ds(height - 1, 1), :], (TILE, LANES))
        above, below = ghost_rows(swap_one, swap_two, k, last_own)
        inner[k][pl.ds(0, TILE), :] = filler
        inner[k][pl.ds(TILE, TILE), :] = above
        inner[k][pl.ds(2 * TILE, 2 * MARGIN), :] = own[k][pl.ds(0, 2 * MARGIN), :]
        inner[k][pl.ds(seg, 2 * MARGIN), :] = own[k][pl.ds(low, 2 * MARGIN), :]
        inner[k][pl.ds(n - 2 * TILE, TILE), :] = below
        inner[k][pl.ds(n - TILE, TILE), :] = filler
    p, u, w, c, rho = inner
    set_coefs(0, n - TILE, c, rho, ax, az, stiff)
    at_top, _ = depth_ends()
    at = pl.ds(TILE, TILE)
    az[at, :] = jnp.where(at_top, 0.0, az[at, :])

    def place(row, col):
        upper = between(row, -TILE, 2 * MARGIN)
        lower = between(row, low, height + TILE)
        local = jnp.where(upper, row + MARGIN, row - low + seg)
        lane = col - lax.axis_index("range") * LANES
        return [(local, lane, jnp.logical_or(upper, lower))]

    found = find_sources(sources, lax.axis_index("depth") * height, place)
    left_steps(n, (p, u, w), (ax, az, stiff), stages, shifts, found, wavelet)
    for side, start in enumerate((MARGIN, seg + MARGIN)):
        fields = finals(stages, pl.ds(start, MARGIN))
        there = pl.ds(side * MARGIN, MARGIN)
        out[there, :] = packed(*fields)
        for f in range(3):
            done[f, there, :] = fields[f]
    lanes = lane_ids(TILE)
    found = None
    for side, start in enumerate((TILE, seg + MARGIN)):
        for j in range(3):
            here = pl.ds(start + j * TILE, TILE)
            part = jnp.where(
                lanes < 4 * SKEW,
                slanted(here, p, stages, stiff[here, :]),
                roll(rho[here, :], 4 * SKEW),
            )
            lane = 5 * SKEW * (3 * side + j)
            part = roll(part, lane) if lane else part
            found = part if lane == 0 else jnp.where(lanes < lane, found, part)
    out[pl.ds(2 * MARGIN, TILE), :] = found
    out[pl.ds(2 * MARGIN + TILE, lean.shape[0]), :] = lean[...]


def rho_slot(i, tiles):
    if i == 0:
        return (tiles - 2) // 4, 0
    if i == tiles - 1:
        return (tiles - 2) // 4, 1
    return (i - 1) // 4, (i - 1) % 4


def wide_kernel(height, *refs):
    shifts, sources, wavelet = refs[:3]
    own, ahead, swap_one, swap_two = refs[3:8], refs[8:10], refs[10], refs[11]
    strip, out = refs[12:14]
    p, u, w = out.at[0], out.at[1], out.at[2]
    rho, ax, az, al, stiff, raw, sems = refs[14:]
    half = LANES // 2
    n = height + 2 * MARGIN
    at_top, at_bottom = depth_ends()
    _, at_end = range_ends()

    @pl.when(jnp.logical_not(at_end))
    def _():
        each = height // BLOCKS
        rows = each + 2 * TILE

        def put(i, k, parts):
            lanes = lane_ids(k)
            for a in range(5):
                found = None
                for b in range(BLOCKS):
                    part = roll(parts[b][a], STRIP * b - KEPT)
                    found = part if b == 0 else jnp.where(lanes < STRIP * b, found, part)
                strip[a, pl.ds(i + TILE, k), :] = found

        def fields(here):
            return [own[0][here, :], own[1][here, :], own[2][here, :], own_stiff(own, here), own[4][here, :]]

        def middle(i, k):
            put(i, k, [fields(pl.ds(b * each - TILE + i, k)) for b in range(BLOCKS)])

        for_rows(TILE, rows - TILE, middle, 32)
        above, below = [], []
        for k in range(5):
            last_own = jnp.broadcast_to(own[k][pl.ds(height - 1, 1), :], (TILE, LANES))
            one, two = ghost_rows(swap_one, swap_two, k, last_own)
            above.append(one)
            below.append(two)
        for parts in (above, below):
            parts[3] = TIME_STEP * (parts[4] * parts[3] * parts[3])
        inner = [fields(pl.ds(b * each - TILE, TILE)) for b in range(1, BLOCKS)]
        put(0, TILE, [above] + inner)
        inner = [fields(pl.ds((b + 1) * each, TILE)) for b in range(BLOCKS - 1)]
        put(rows - TILE, TILE, inner + [below])

    @pl.when(at_end)
    def _():
        copies = [pltpu.make_async_copy(ahead[f], raw.at[f], sems.at[f]) for f in range(2)]
        for copy in copies:
            copy.start()
        for copy in copies:
            copy.wait()

        def place_rows(e, k, parts, both):
            here = pl.ds(e, k)
            lanes = lane_ids(k)
            mine = lanes < half
            for ref, part in zip((p, u, w), parts):
                ref[here, :] = jnp.where(mine, roll(part, half), 0.0)
            dense = jnp.where(mine, roll(parts[4], half), both)
            speed = roll(jnp.where(mine, both, parts[3]), half)
            rho[here, :] = dense
            stiff[here, :] = TIME_STEP * (dense * speed * speed)

        for j in range(height // LANES):
            at = pl.ds(j * LANES, LANES)
            both = jnp.concatenate([raw[0, :, at], raw[1, :, at]], 0).T
            place_rows(j * LANES + MARGIN, LANES, [ref[at, :] for ref in own], both)
        above, below = [], []
        for k in range(5):
            last_own = jnp.broadcast_to(own[k][pl.ds(height - 1, 1), :], (TILE, LANES))
            one, two = ghost_rows(swap_one, swap_two, k, last_own)
            above.append(one)
            below.append(two)
        lanes = lane_ids(TILE)
        one, two = swapped_rows(swap_one, swap_two, 5)
        last = jnp.broadcast_to(rho[pl.ds(height + MARGIN - 1, 1), :], (TILE, LANES))
        one = jnp.where(jnp.logical_and(at_top, lanes >= half), 1.0, one)
        two = jnp.where(jnp.logical_and(at_bottom, lanes >= half), last, two)
        place_rows(TILE, TILE, above, one)
        place_rows(height + MARGIN, TILE, below, two)
        for e in (0, n - TILE):
            here = pl.ds(e, TILE)
            for ref in (p, u, w, stiff):
                ref[here, :] = jnp.zeros((TILE, LANES), jnp.float32)
            rho[here, :] = jnp.ones((TILE, LANES), jnp.float32)
        set_coefs(0, n - TILE, None, rho, ax, az, None)

        def edge_coefs(r, k):
            al[pl.ds(r, k), :] = TIME_STEP / rho[pl.ds(r, k), :]

        for_rows(0, n - TILE, edge_coefs)
        at = pl.ds(TILE, TILE)
        az[at, :] = jnp.where(at_top, 0.0, az[at, :])

        def place(row, col):
            good = between(row, -TILE, height + TILE)
            return [(row + MARGIN, col - lax.axis_index("range") * LANES - half, good)]

        found = find_sources(sources, lax.axis_index("depth") * height, place)
        offsets = offsets_of(shifts)
        for t in range(ITERS):
            edge = half - 1 + offsets[t]

            def speeds(r, k):
                here = pl.ds(r, k)
                lanes = lane_ids(k)
                now = p[here, :]
                slope = jnp.where(lanes == edge, al[here, :], ax[here, :])
                slope = jnp.where(lanes > edge, 0.0, slope)
                u[here, :] = u[here, :] - slope * (roll(now, -1) - now)
                slope = jnp.where(lanes > edge, 0.0, az[here, :])
                w[here, :] = w[here, :] - slope * (p[pl.ds(r + 1, k), :] - now)

            def press(r, k):
                here = pl.ds(r, k)
                fast = u[here, :]
                down_ = w[here, :] - w[pl.ds(r - 1, k), :]
                hard = jnp.where(lane_ids(k) > edge, 0.0, stiff[here, :])
                p[here, :] = p[here, :] - hard * ((fast - roll(fast, 1)) + down_)

            for_rows(0, n - TILE, speeds)
            for_rows(TILE, n - TILE, press)
            inject(p, found, wavelet, t)


def rest_kernel(height, more, blocks, *refs):
    stages, done, out = [[ref] for ref in refs[:3]], refs[3], refs[4]
    each = height // blocks

    def read(b, side, r, k):
        if b == 0 and side < 0:
            return [done[f, pl.ds(0, k), :] for f in range(3)]
        if b == blocks - 1 and side > 0:
            return [done[f, pl.ds(MARGIN, k), :] for f in range(3)]
        return finals(stages, pl.ds(r + b * each, k))

    def join(fields):
        lanes = lane_ids(fields[0].shape[0])
        found = jnp.where(lanes < START + 2 * more, roll(fields[1], more), roll(fields[2], 2 * more))
        return jnp.where(lanes < START + more, fields[0], found)

    for side, (low, high) in zip((-1, 0, 1), ((0, MARGIN), (MARGIN, each - MARGIN), (each - MARGIN, each))):

        def beside(r, k, side=side):
            lanes = lane_ids(k)
            found = join(read(0, side, r, k))
            for b in range(1, blocks):
                part = roll(join(read(b, side, r, k)), LANES // blocks * b)
                start = START + LANES // blocks * b
                mine = between(lanes, start, start + 3 * more)
                if start + 3 * more > LANES:
                    mine = jnp.logical_or(lanes >= start, lanes < start + 3 * more - LANES)
                    if start >= LANES:
                        mine = between(lanes, start - LANES, start + 3 * more - LANES)
                found = jnp.where(mine, part, found)
            out[pl.ds(r, k), :] = found

        for_rows(low, high, beside)


def mid_kernel(height, low, *refs):
    shifts, stages, done, wide, near = refs[0], refs[1:4], refs[4], refs[5], refs[6]
    built = refs[-3:]
    _, at_end = range_ends()
    total = offsets_of(shifts)[ITERS]
    turn = LANES - total
    inside = (MARGIN, height - MARGIN)

    @pl.when(jnp.logical_not(at_end))
    def _():
        def build(r, k):
            theirs = between(lane_ids(k), SKEW, total)
            for f in range(3):
                mine = stages[f][pl.ds(r, k), :]
                at, back = r - MARGIN, (NARROW if low else WIDTH) * f
                if low and at >= 3 * each:
                    at, back = f * each, 3 * NARROW
                other = near[pl.ds(at, k), :]
                other = roll(other, -back) if back else other
                built[f][pl.ds(r, k), :] = pltpu.roll(jnp.where(theirs, other, mine), turn, 1)

        each = (inside[1] - inside[0]) // 4
        for start in range(*inside, each):
            build(start, each)

    @pl.when(at_end)
    def _():
        def build(r, k):
            lanes = lane_ids(k)
            inner = jnp.logical_and(lanes >= total, lanes < KEPT + SKEW)
            for f in range(3):
                part = roll(wide[f, pl.ds(r + MARGIN, k), :], LANES // 2)
                if inside[0] <= r < inside[1]:
                    mine = stages[f][pl.ds(r, k), :]
                else:
                    mine = done[f, pl.ds(0 if r < MARGIN else MARGIN, k), :]
                built[f][pl.ds(r, k), :] = pltpu.roll(jnp.where(inner, mine, part), turn, 1)

        build(0, MARGIN)
        build(MARGIN, height - 2 * MARGIN)
        build(height - MARGIN, MARGIN)


def last_kernel(height, more, blocks, *refs):
    far_too = more > 0
    shifts, sources, wavelet = refs[:3]
    done, strip, edge = refs[3:6]
    lean = edge.at[pl.ds(2 * MARGIN + TILE, edge.shape[0] - 2 * MARGIN - TILE)]
    drafts = refs[6:9]
    rest = refs[9] if far_too else None
    refs = refs[9 + far_too :]
    outs, built = refs[:3], refs[3:6]
    p, u, w, rho, ax, az, stiff, gp, gu, gw, sems = refs[6:]
    at_top, _ = depth_ends()
    _, at_end = range_ends()
    each = height // BLOCKS
    tiles = each // TILE + 2
    n = (tiles + 2) * TILE
    own_part = STRIP // 2
    total = offsets_of(shifts)[ITERS]
    start = START
    turn = LANES - total

    @pl.when(at_end)
    def _():
        copies = [pltpu.make_async_copy(drafts[f], outs[f], sems.at[f, 0]) for f in range(3)]
        for copy in copies:
            copy.start()
        for copy in copies:
            copy.wait()

    @pl.when(jnp.logical_not(at_end))
    def _():
        lanes = lane_ids(TILE)
        inner = lanes % STRIP
        mine = inner < own_part
        six = edge[pl.ds(2 * MARGIN, TILE), :]
        for i in range(tiles):
            here = pl.ds((i + 1) * TILE, TILE)
            pack = lean[pl.ds(i * TILE, TILE), :]
            group, slot = rho_slot(i, tiles)
            dense = lean[pl.ds((tiles + group) * TILE, TILE), :]
            origin = 4 * BLOCKS * slot + SKEW * (lanes // STRIP) + inner - own_part
            theirs = jnp.take_along_axis(dense, jnp.clip(origin, 0, LANES - 1), 1)
            parts = [roll(pack, own_part - SKEW * g) if g != 2 else pack for g in range(4)]
            parts.append(theirs)
            late = None
            if i < 3:
                late, lane, b = 5 * SKEW * i, own_part, 0
            elif i >= tiles - 3:
                late, lane, b = 5 * SKEW * (i - tiles + 6), STRIP * (BLOCKS - 1) + own_part, BLOCKS - 1
            if late is not None:
                block = between(lanes, STRIP * b, STRIP * (b + 1))
                parts = [
                    jnp.where(block, roll(six, lane - late - SKEW * g), part)
                    for g, part in enumerate(parts)
                ]
            for ref, part in zip((gp, gu, gw), parts):
                ref[here, :] = part
            for a, (ref, part) in enumerate(zip((p, u, w, stiff, rho), parts)):
                ref[here, :] = jnp.where(mine, strip[a, here, :], part)
        for e in (0, n - TILE):
            here = pl.ds(e, TILE)
            for ref in (p, u, w, stiff):
                ref[here, :] = jnp.zeros((TILE, LANES), jnp.float32)
            rho[here, :] = jnp.ones((TILE, LANES), jnp.float32)
        set_coefs(TILE, n - TILE, None, rho, ax, az, None)
        at = pl.ds(TILE, TILE)
        az[at, :] = jnp.where(jnp.logical_and(at_top, lane_ids(TILE) < STRIP), 0.0, az[at, :])

        def place(row, col):
            col = col - lax.axis_index("range") * LANES - KEPT
            inside = between(col, 0, STRIP)
            inside = jnp.logical_and(inside, between(row, -TILE, height + TILE))
            b = (row + TILE) // each
            local = row + TILE - b * each
            one = jnp.logical_and(inside, b < BLOCKS)
            two = jnp.logical_and(inside, jnp.logical_and(b > 0, local < 2 * TILE))
            return [
                (local + TILE, STRIP * b + col, one),
                (local + each + TILE, STRIP * (b - 1) + col, two),
            ]

        found = find_sources(sources, lax.axis_index("depth") * height, place)
        for t in range(ITERS):
            taken = own_part + t

            def speeds(r, k):
                here = pl.ds(r, k)
                inner = lane_ids(k) % STRIP
                now = p[here, :]
                fast = u[here, :] - ax[here, :] * (roll(now, -1) - now)
                u[here, :] = jnp.where(inner == taken, gu[here, :], fast)
                deep = w[here, :] - az[here, :] * (p[pl.ds(r + 1, k), :] - now)
                w[here, :] = jnp.where(inner == taken, gw[here, :], deep)

            def press(r, k):
                here = pl.ds(r, k)
                inner = lane_ids(k) % STRIP
                fast = u[here, :]
                down_ = w[here, :] - w[pl.ds(r - 1, k), :]
                new = p[here, :] - stiff[here, :] * ((fast - roll(fast, 1)) + down_)
                if t < ITERS - 1:
                    new = jnp.where(inner == taken + 1, gp[here, :], new)
                p[here, :] = new

            for_rows(TILE, n - TILE, speeds)
            for_rows(TILE, n - TILE, press)
            inject(p, found, wavelet, t, taken)

        copies = []
        for b in range(BLOCKS):
            first = b * each
            low, high = first, first + each
            edges = []
            if b == 0:
                low = MARGIN
                edges = [(0, 0)]
            if b == BLOCKS - 1:
                high = height - MARGIN
                edges = [(high, MARGIN)]

            def far_values(row, k):
                b = row // (height // blocks)
                found = rest[pl.ds(row - b * (height // blocks), k), :]
                return roll(found, -LANES // blocks * b) if b else found

            for row, side in edges:
                here, there = pl.ds(row, MARGIN), pl.ds(side, MARGIN)
                lanes = lane_ids(MARGIN)
                for f, ref in enumerate((p, u, w)):
                    part = roll(ref[pl.ds(row - first + 2 * TILE, MARGIN), :], KEPT - STRIP * b)
                    kept = jnp.where(between(lanes, SKEW, KEPT + SKEW), done[f, there, :], part)
                    other = edge[there, :]
                    other = roll(other, -WIDTH * f) if f else other
                    if far_too:
                        far = far_values(row, MARGIN)
                        far = roll(far, -more * f) if f else far
                        other = jnp.where(lanes < start, other, far)
                    kept = jnp.where(between(lanes, SKEW, total), other, kept)
                    built[f][here, :] = pltpu.roll(kept, turn, 1)
            here, k = pl.ds(low, high - low), high - low
            natural = (lane_ids(k) + total) % LANES
            ready = between(natural, SKEW, KEPT + SKEW)
            shift = (KEPT - STRIP * b + LANES + turn) % LANES
            for f, ref in enumerate((p, u, w)):
                part = pltpu.roll(ref[pl.ds(low - first + 2 * TILE, k), :], shift, 1)
                kept = jnp.where(ready, drafts[f][here, :], part)
                if far_too:
                    far = pltpu.roll(far_values(low, k), (turn + LANES - more * f) % LANES, 1)
                    kept = jnp.where(between(natural, start, total), far, kept)
                built[f][here, :] = kept
            for f in range(3):
                at = pl.ds(first, each)
                copy = pltpu.make_async_copy(built[f].at[at, :], outs[f].at[at, :], sems.at[f, b])
                copy.start()
                copies.append(copy)
        for copy in copies:
            copy.wait()


def moved(x):
    return lax.ppermute(x, "range", [(i + 1, i) for i in range(lax.axis_size("range") - 1)])


def swapped(x, first):
    pairs = [(i, i + 1) for i in range(first, lax.axis_size("depth") - 1, 2)]
    return lax.ppermute(x, "depth", pairs + [(j, i) for i, j in pairs])


LOCAL = pl.BlockSpec(memory_space=pltpu.VMEM)
REMOTE = pl.BlockSpec(memory_space=pl.ANY)
SCALAR = pl.BlockSpec(memory_space=pltpu.SMEM)


def shaped(shape, space):
    if space is SCALAR:
        return pltpu.SMEM(*shape)
    if space is LOCAL:
        return pltpu.VMEM(shape, jnp.float32)
    return jax.ShapeDtypeStruct(shape, jnp.float32)


def call(kernel, ins, outs, scratch=()):
    values, specs = [], []
    for value, space in ins:
        if space is LOCAL:
            value = pltpu.with_memory_space_constraint(value, pltpu.VMEM)
        elif space is SCALAR:
            value = pltpu.with_memory_space_constraint(value, pltpu.SMEM)
        elif space is REMOTE:
            value = pltpu.with_memory_space_constraint(value, pltpu.HBM)
        values.append(value)
        specs.append(space)
    return pl.pallas_call(
        kernel,
        in_specs=specs,
        out_specs=[space for _, space in outs],
        out_shape=[shaped(*pair) for pair in outs],
        scratch_shapes=list(scratch),
        compiler_params=pltpu.CompilerParams(vmem_limit_bytes=8 * 1024 * 1024),
    )(*values)


def room(*shape):
    return pltpu.VMEM(shape, jnp.float32)


def shards(
    pressure,
    vel_range,
    vel_depth,
    sound_speed,
    density,
    ahead_speed,
    ahead_density,
    shifts,
    sources,
    wavelet,
):
    height, breadth = pressure.shape
    extra = ahead_speed.shape[1]
    assert breadth == LANES and 2 * extra == LANES and height % 512 == 0
    assert START + MORE[-1][1] == extra
    arrays = [(x, REMOTE) for x in (pressure, vel_range, vel_depth, sound_speed, density)]
    ahead = [(x.T, REMOTE) for x in (ahead_speed, ahead_density)]
    small = [(shifts, REMOTE), (sources.T, REMOTE), (wavelet.T, REMOTE)]
    sizes = (shifts.shape, sources.shape[::-1], wavelet.shape[::-1])
    kinds = (jnp.int32, jnp.int32, jnp.float32)
    scalars = [(pair, SCALAR) for pair in zip(sizes, kinds)]
    field = (height, LANES)
    dma = pltpu.SemaphoreType.DMA

    found = call(
        functools.partial(own_kernel, height),
        small + arrays + ahead,
        [((6 * TILE, LANES), LOCAL)] * 2
        + [(field, LOCAL)] * 5
        + [((ITERS - 1, *field), LOCAL)] * 3
        + [(field, LOCAL)] * 3
        + scalars
        + [(((1,), jnp.int32), SCALAR)],
        [room(*field)] * 3 + [room(2, LANES, LANES), dma((5,)), dma((2, 2)), dma((3,))],
    )
    tiles = height // BLOCKS // TILE + 2
    lean_rows = (tiles + (tiles - 2) // 4 + 1) * TILE
    n_edge = 6 * MARGIN
    n_wide = height + 2 * MARGIN
    n_strip = (tiles + 2) * TILE

    def finish(kind, ahead, swap_one, swap_two, *found):
        _, more, blocks = MORE[kind]
        ahead = [(x, REMOTE) for x in ahead]
        own = [(x, LOCAL) for x in found[:5]]
        stages = [(x, LOCAL) for x in found[5:11]]
        last = stages[3:]
        small = [(x, SCALAR) for x in found[11:]]
        (plane,) = call(
            functools.partial(pack_kernel, height, kind == 0),
            last,
            [(((4 if kind else 3) * (height - 2 * MARGIN) // 4, LANES), LOCAL)],
        )
        near = [(moved(plane), LOCAL)]
        sides = [(swapped(swap_one, 0), LOCAL), (swapped(swap_two, 1), LOCAL)]
        (lean,) = call(
            functools.partial(lean_kernel, height), own + stages, [((lean_rows, LANES), LOCAL)]
        )
        edge, done = call(
            functools.partial(edge_kernel, height),
            small + own + sides + [(lean, LOCAL)],
            [((2 * MARGIN + TILE + lean_rows, LANES), LOCAL), ((3, 2 * MARGIN, LANES), LOCAL)],
            [room(n_edge, LANES)] * 3
            + [room(ITERS - 1, n_edge, LANES)] * 3
            + [room(n_edge, LANES)] * 8,
        )
        edge_near = moved(edge)
        received = []
        if more:
            (rest,) = call(
                functools.partial(rest_kernel, height, more, blocks),
                last + [(done, LOCAL)],
                [((height // blocks, LANES), LOCAL)],
            )
            received = [(moved(rest), LOCAL)]
        strip, wide = call(
            functools.partial(wide_kernel, height),
            small + own + ahead + sides,
            [((5, n_strip, LANES), LOCAL), ((3, n_wide, LANES), LOCAL)],
            [room(n_wide, LANES)] * 5 + [room(2, extra, height), dma((2,))],
        )
        drafts = call(
            functools.partial(mid_kernel, height, kind == 0),
            small[:1] + last + [(done, LOCAL), (wide, LOCAL)] + near,
            [(field, LOCAL)] * 3,
        )
        mixed = [(x, LOCAL) for x in (done, strip, edge_near, *drafts)]
        return tuple(
            call(
                functools.partial(last_kernel, height, more, blocks),
                small + mixed + received,
                [(field, REMOTE)] * 3,
                [room(*field)] * 3 + [room(n_strip, LANES)] * 10 + [dma((3, BLOCKS))],
            )
        )

    return lax.switch(
        found[-1].reshape(()),
        [functools.partial(finish, kind) for kind in range(len(MORE))],
        [x for x, _ in ahead],
        *found[:-1],
    )


def solution(mesh):
    field = P("depth", "range")
    strip = P("depth", None)
    return jax.shard_map(
        shards,
        mesh=mesh,
        in_specs=(field,) * 5 + (strip,) * 2 + (P(),) * 3,
        out_specs=(field,) * 3,
        check_vma=False,
    )
```

```python
import functools

import jax
import jax.numpy as jnp
from jax import lax
from jax.experimental import pallas as pl
from jax.experimental.pallas import tpu as pltpu
from jax.sharding import PartitionSpec as P

ITERS = 4
TIME_STEP = 0.6
LANES = 128
TILE = 8
MARGIN = 16
SKEW = 4
WIDTH = 42
NARROW = 32
START = SKEW + WIDTH
MORE = ((NARROW + SKEW, 0, 0), (START, 0, 0), (START + 10, 10, 4), (1 << 20, 18, 2))
STRIP = 16
BLOCKS = LANES // STRIP
KEPT = LANES - STRIP // 2
BLOCK = 1024


def lane_ids(rows):
    return lax.broadcasted_iota(jnp.int32, (rows, LANES), 1)


def between(lanes, low, high):
    return jnp.logical_and(lanes >= low, lanes < high)


def roll(x, by):
    return pltpu.roll(x, by % LANES, 1)


def for_rows(start, stop, fn, size=BLOCK):
    whole = (stop - start) // size

    def step(i, carry):
        fn(pl.multiple_of(start + i * size, TILE), size)
        return carry

    if whole > 1:
        lax.fori_loop(0, whole, step, 0)
    elif whole == 1:
        fn(start, size)
    if start + whole * size < stop:
        fn(start + whole * size, stop - start - whole * size)


def offsets_of(shifts):
    found = [jnp.int32(0)]
    for t in range(ITERS):
        found.append(found[-1] + shifts[t])
    return found


def range_ends():
    place = lax.axis_index("range")
    return place == 0, place == lax.axis_size("range") - 1


def depth_ends():
    place = lax.axis_index("depth")
    return place == 0, place == lax.axis_size("depth") - 1


def set_coefs(start, stop, c, rho, ax, az, stiff):
    def coefs(r, k):
        here = pl.ds(r, k)
        dense = rho[here, :]
        ax[here, :] = (2.0 * TIME_STEP) / (dense + roll(dense, -1))
        az[here, :] = (2.0 * TIME_STEP) / (dense + rho[pl.ds(r + 1, k), :])
        if c is not None:
            speed = c[here, :]
            stiff[here, :] = TIME_STEP * (dense * speed * speed)

    for_rows(start, stop, coefs)


def find_sources(sources, height, places, seen=None):
    def candidates(k):
        found = []
        for row, lane, good in places(height, sources[0, k] - lax.axis_index("depth") * height, sources[1, k]):
            good = jnp.logical_and(good, between(lane, 0, LANES))
            found.append((row, lane, good))
        return found

    def look(k, seen):
        for _, _, good in candidates(k):
            seen = jnp.logical_or(seen, good)
        return seen

    if seen is None:
        seen = lax.fori_loop(0, sources.shape[1], look, jnp.bool_(False))
    return candidates, seen


def own_place(height, row, col):
    return [(row, col - lax.axis_index("range") * LANES, between(row, 0, height))]


def edge_place(height, row, col):
    low, seg = height - 2 * MARGIN, 3 * MARGIN
    upper = between(row, -TILE, 2 * MARGIN)
    lower = between(row, low, height + TILE)
    local = jnp.where(upper, row + MARGIN, row - low + seg)
    lane = col - lax.axis_index("range") * LANES
    return [(local, lane, jnp.logical_or(upper, lower))]


def wide_place(height, row, col):
    good = between(row, -TILE, height + TILE)
    return [(row + MARGIN, col - lax.axis_index("range") * LANES - LANES // 2, good)]


def strip_place(height, row, col):
    each = height // BLOCKS
    col = col - lax.axis_index("range") * LANES - KEPT
    inside = between(col, 0, STRIP)
    inside = jnp.logical_and(inside, between(row, -TILE, height + TILE))
    b = (row + TILE) // each
    local = row + TILE - b * each
    one = jnp.logical_and(inside, b < BLOCKS)
    two = jnp.logical_and(inside, jnp.logical_and(b > 0, local < 2 * TILE))
    return [
        (local + TILE, STRIP * b + col, one),
        (local + each + TILE, STRIP * (b - 1) + col, two),
    ]


def inject(field, found, wavelet, t, reach=None):
    candidates, seen = found

    @pl.when(seen)
    def _():
        rows = lax.broadcasted_iota(jnp.int32, (TILE, LANES), 0)
        lanes = lane_ids(TILE)

        def add(k, carry):
            for row, lane, good in candidates(k):
                if reach is not None:
                    good = jnp.logical_and(good, lane % STRIP <= reach)

                @pl.when(good)
                def _(row=row, lane=lane):
                    at = pl.ds(pl.multiple_of((row // TILE) * TILE, TILE), TILE)
                    here = jnp.logical_and(rows == row % TILE, lanes == lane)
                    field[at, :] = field[at, :] + jnp.where(here, wavelet[t, k], 0.0)

            return carry

        lax.fori_loop(0, wavelet.shape[1], add, 0)


def left_steps(n, fields, coefs, stages, shifts, found, wavelet):
    ax, az, stiff = coefs
    ps, us, ws = stages
    offsets = offsets_of(shifts)
    at_start, _ = range_ends()
    for t in range(ITERS):
        p, u, w = fields if t == 0 else (ps[t - 1], us[t - 1], ws[t - 1])
        u_new, w_new, p_new = us[t], ws[t], ps[t]
        wall = jnp.where(at_start, offsets[t], -1)

        def speeds(r, k):
            here = pl.ds(r, k)
            now = p[here, :]
            u_new[here, :] = u[here, :] - ax[here, :] * (roll(now, -1) - now)
            w_new[here, :] = w[here, :] - az[here, :] * (p[pl.ds(r + 1, k), :] - now)

        def press(r, k):
            here = pl.ds(r, k)
            fast = u_new[here, :]
            left = jnp.where(lane_ids(k) == wall, 0.0, roll(fast, 1))
            down = w_new[here, :] - w_new[pl.ds(r - 1, k), :]
            p_new[here, :] = p[here, :] - stiff[here, :] * ((fast - left) + down)

        for_rows(0, n - TILE, speeds)
        for_rows(TILE, n - TILE, press)
        inject(p_new, found, wavelet, t)


def slanted(here, p0, stages, stiff):
    ps, us, ws = stages
    lanes = lane_ids(TILE)

    def pick(parts):
        found = parts[-1]
        for t in range(len(parts) - 2, -1, -1):
            found = jnp.where(lanes <= t, parts[t], found)
        return found

    a = pick([p0[here, :]] + [ps[t][here, :] for t in range(ITERS - 1)])
    b = pick([us[t][here, :] for t in range(ITERS)])
    c = pick([ws[t][here, :] for t in range(ITERS)])
    found = jnp.where(lanes < 3 * SKEW, roll(c, 2 * SKEW), roll(stiff, 3 * SKEW))
    found = jnp.where(lanes < 2 * SKEW, roll(b, SKEW), found)
    return jnp.where(lanes < SKEW, a, found)


def packed(p, u, w, width=WIDTH):
    lanes = lane_ids(p.shape[0])
    found = jnp.where(
        between(lanes, SKEW, SKEW + 2 * width), roll(u, width), roll(w, 2 * width)
    )
    return jnp.where(between(lanes, SKEW, SKEW + width), p, found)


def finals(stages, here):
    return [stage[-1][here, :] for stage in stages]


def staged(early, final):
    return [[a.at[t] for t in range(ITERS - 1)] + [b] for a, b in zip(early, final)]


def own_kernel(height, *refs):
    arrays, ahead = refs[3:8], refs[8:10]
    swap_one, swap_two = refs[10:12]
    own, stages, scalars = refs[12:17], staged(refs[17:20], refs[20:23]), refs[23:26]
    seen, flag, ax, az, stiff, ends, sems, end_sems, scalar_sems = refs[26:]
    shifts, sources, wavelet = scalars
    order = (4, 3, 0, 1, 2)
    copies = {k: pltpu.make_async_copy(arrays[k], own[k], sems.at[k]) for k in order}
    scalar_copies = [
        pltpu.make_async_copy(refs[k], scalars[k], scalar_sems.at[k]) for k in range(3)
    ]
    for copy in scalar_copies:
        copy.start()
    for k in order:
        copies[k].start()
    end_copies = []
    for side, start in enumerate((0, height - LANES)):
        for f in range(2):
            copy = pltpu.make_async_copy(
                ahead[f].at[:, pl.ds(start, LANES)],
                ends.at[side, pl.ds(f * LANES // 2, LANES // 2), :],
                end_sems.at[side, f],
            )
            copy.start()
            end_copies.append(copy)
    p, u, w, c, rho = own

    for copy in scalar_copies:
        copy.wait()
    total = offsets_of(shifts)[ITERS]
    kind = jnp.int32(0)
    for limit, _, _ in MORE[:-1]:
        kind = kind + jnp.where(total > limit, 1, 0)
    flag[0] = kind
    for j, places in enumerate((edge_place, wide_place, strip_place)):
        seen[j] = jnp.where(find_sources(sources, height, places)[1], 1, 0)
    found = find_sources(sources, height, own_place)
    copies[4].wait()
    copies[3].wait()
    set_coefs(0, height - TILE, c, rho, ax, az, stiff)
    for k in (0, 1, 2):
        copies[k].wait()
    left_steps(height, (p, u, w), (ax, az, stiff), stages, shifts, found, wavelet)

    for copy in end_copies:
        copy.wait()
    even = lax.axis_index("depth") % 2 == 0
    tops = [own[k][pl.ds(0, TILE), :] for k in range(5)] + [ends[0].T[:TILE]]
    lows = [own[k][pl.ds(height - TILE, TILE), :] for k in range(5)] + [ends[1].T[LANES - TILE :]]
    for k, (top, low) in enumerate(zip(tops, lows)):
        at = pl.ds(k * TILE, TILE)
        swap_one[at, :] = jnp.where(even, low, top)
        swap_two[at, :] = jnp.where(even, top, low)


def pack_kernel(height, low, *refs):
    stages, plane = [[ref] for ref in refs[:3]], refs[3]
    if not low:

        def finish(r, k):
            plane[pl.ds(r - MARGIN, k), :] = packed(*finals(stages, pl.ds(r, k)))

        for_rows(MARGIN, height - MARGIN, finish)
        return
    each = (height - 2 * MARGIN) // 4
    inner = between(lane_ids(each), SKEW, SKEW + 3 * NARROW)
    spread = finals(stages, pl.ds(MARGIN + 3 * each, each))
    for b in range(3):
        part = packed(*finals(stages, pl.ds(MARGIN + b * each, each)), NARROW)
        plane[pl.ds(b * each, each), :] = jnp.where(inner, part, roll(spread[b], 3 * NARROW))


def own_stiff(own, here):
    speed = own[3][here, :]
    return TIME_STEP * (own[4][here, :] * speed * speed)


def lean_kernel(height, *refs):
    own, stages, lean = refs[:5], staged(refs[5:8], refs[8:11]), refs[11]
    each = height // BLOCKS
    tiles = each // TILE + 2

    def tile(i, slot):
        lanes = lane_ids(TILE)
        found = rhos = None
        for b in range(BLOCKS):
            row = b * each + i * TILE - TILE
            if not isinstance(i, int):
                row = pl.multiple_of(row, TILE)
            elif row < 0 or row >= height:
                row = 0
            here = pl.ds(row, TILE)
            part = slanted(here, own[0], stages, own_stiff(own, here))
            part = roll(part, STRIP * b) if b else part
            dense = roll(own[4][here, :], 4 * BLOCKS * slot + SKEW * b)
            found = part if b == 0 else jnp.where(lanes < STRIP * b, found, part)
            rhos = dense if b == 0 else jnp.where(lanes < 4 * BLOCKS * slot + SKEW * b, rhos, dense)
        lean[pl.ds(i * TILE, TILE), :] = found
        return rhos

    def group_of(first, count, out):
        lanes = lane_ids(TILE)
        total = None
        for slot in range(count):
            rhos = tile(first + slot, slot)
            total = rhos if slot == 0 else jnp.where(lanes < 4 * BLOCKS * slot, total, rhos)
        lean[pl.ds((tiles + out) * TILE, TILE), :] = total

    groups = (tiles - 2) // 4

    def body(m, carry):
        group_of(1 + 4 * m, 4, m)
        return carry

    lax.fori_loop(0, groups, body, 0)
    lanes = lane_ids(TILE)
    total = jnp.where(lanes < 4 * BLOCKS, tile(0, 0), tile(tiles - 1, 1))
    lean[pl.ds((tiles + groups) * TILE, TILE), :] = total


def swapped_rows(one, two, k):
    at = pl.ds(k * TILE, TILE)
    even = lax.axis_index("depth") % 2 == 0
    first, second = one[at, :], two[at, :]
    return jnp.where(even, second, first), jnp.where(even, first, second)


def ghost_rows(one, two, k, last_own):
    at_top, at_bottom = depth_ends()
    above, below = swapped_rows(one, two, k)
    if k == 4:
        above = jnp.where(at_top, 1.0, above)
        below = jnp.where(at_bottom, last_own, below)
    return above, below


def edge_kernel(height, *refs):
    shifts, sources, wavelet, seen = refs[:4]
    refs = refs[1:]
    own, swap_one, swap_two, lean = refs[3:8], refs[8], refs[9], refs[10]
    out, done = refs[11:13]
    ax, az, stiff = refs[13:16]
    stages, inner = staged(refs[16:19], refs[19:22]), refs[22:27]
    seg = 3 * MARGIN
    n = 2 * seg
    low = height - 2 * MARGIN
    for k in range(5):
        filler = jnp.full((TILE, LANES), 1.0 if k == 4 else 0.0, jnp.float32)
        last_own = jnp.broadcast_to(own[k][pl.ds(height - 1, 1), :], (TILE, LANES))
        above, below = ghost_rows(swap_one, swap_two, k, last_own)
        inner[k][pl.ds(0, TILE), :] = filler
        inner[k][pl.ds(TILE, TILE), :] = above
        inner[k][pl.ds(2 * TILE, 2 * MARGIN), :] = own[k][pl.ds(0, 2 * MARGIN), :]
        inner[k][pl.ds(seg, 2 * MARGIN), :] = own[k][pl.ds(low, 2 * MARGIN), :]
        inner[k][pl.ds(n - 2 * TILE, TILE), :] = below
        inner[k][pl.ds(n - TILE, TILE), :] = filler
    p, u, w, c, rho = inner
    set_coefs(0, n - TILE, c, rho, ax, az, stiff)
    at_top, _ = depth_ends()
    at = pl.ds(TILE, TILE)
    az[at, :] = jnp.where(at_top, 0.0, az[at, :])

    found = find_sources(sources, height, edge_place, seen[0] > 0)
    left_steps(n, (p, u, w), (ax, az, stiff), stages, shifts, found, wavelet)
    for side, start in enumerate((MARGIN, seg + MARGIN)):
        fields = finals(stages, pl.ds(start, MARGIN))
        there = pl.ds(side * MARGIN, MARGIN)
        out[there, :] = packed(*fields)
        for f in range(3):
            done[f, there, :] = fields[f]
    lanes = lane_ids(TILE)
    found = None
    for side, start in enumerate((TILE, seg + MARGIN)):
        for j in range(3):
            here = pl.ds(start + j * TILE, TILE)
            part = jnp.where(
                lanes < 4 * SKEW,
                slanted(here, p, stages, stiff[here, :]),
                roll(rho[here, :], 4 * SKEW),
            )
            lane = 5 * SKEW * (3 * side + j)
            part = roll(part, lane) if lane else part
            found = part if lane == 0 else jnp.where(lanes < lane, found, part)
    out[pl.ds(2 * MARGIN, TILE), :] = found
    out[pl.ds(2 * MARGIN + TILE, lean.shape[0]), :] = lean[...]


def rho_slot(i, tiles):
    if i == 0:
        return (tiles - 2) // 4, 0
    if i == tiles - 1:
        return (tiles - 2) // 4, 1
    return (i - 1) // 4, (i - 1) % 4


def wide_kernel(height, *refs):
    shifts, sources, wavelet, seen = refs[:4]
    refs = refs[1:]
    own, ahead, swap_one, swap_two = refs[3:8], refs[8:10], refs[10], refs[11]
    strip, out = refs[12:14]
    p, u, w = out.at[0], out.at[1], out.at[2]
    rho, ax, az, al, stiff, raw, sems = refs[14:]
    half = LANES // 2
    n = height + 2 * MARGIN
    at_top, at_bottom = depth_ends()
    _, at_end = range_ends()

    @pl.when(jnp.logical_not(at_end))
    def _():
        each = height // BLOCKS
        rows = each + 2 * TILE

        def put(i, k, parts):
            lanes = lane_ids(k)
            for a in range(5):
                found = None
                for b in range(BLOCKS):
                    part = roll(parts[b][a], STRIP * b - KEPT)
                    found = part if b == 0 else jnp.where(lanes < STRIP * b, found, part)
                strip[a, pl.ds(i + TILE, k), :] = found

        def fields(here):
            return [own[0][here, :], own[1][here, :], own[2][here, :], own_stiff(own, here), own[4][here, :]]

        def middle(i, k):
            put(i, k, [fields(pl.ds(b * each - TILE + i, k)) for b in range(BLOCKS)])

        for_rows(TILE, rows - TILE, middle, 32)
        above, below = [], []
        for k in range(5):
            last_own = jnp.broadcast_to(own[k][pl.ds(height - 1, 1), :], (TILE, LANES))
            one, two = ghost_rows(swap_one, swap_two, k, last_own)
            above.append(one)
            below.append(two)
        for parts in (above, below):
            parts[3] = TIME_STEP * (parts[4] * parts[3] * parts[3])
        inner = [fields(pl.ds(b * each - TILE, TILE)) for b in range(1, BLOCKS)]
        put(0, TILE, [above] + inner)
        inner = [fields(pl.ds((b + 1) * each, TILE)) for b in range(BLOCKS - 1)]
        put(rows - TILE, TILE, inner + [below])

    @pl.when(at_end)
    def _():
        copies = [pltpu.make_async_copy(ahead[f], raw.at[f], sems.at[f]) for f in range(2)]
        for copy in copies:
            copy.start()
        for copy in copies:
            copy.wait()

        def place_rows(e, k, parts, both):
            here = pl.ds(e, k)
            lanes = lane_ids(k)
            mine = lanes < half
            for ref, part in zip((p, u, w), parts):
                ref[here, :] = jnp.where(mine, roll(part, half), 0.0)
            dense = jnp.where(mine, roll(parts[4], half), both)
            speed = roll(jnp.where(mine, both, parts[3]), half)
            rho[here, :] = dense
            stiff[here, :] = TIME_STEP * (dense * speed * speed)

        for j in range(height // LANES):
            at = pl.ds(j * LANES, LANES)
            both = jnp.concatenate([raw[0, :, at], raw[1, :, at]], 0).T
            place_rows(j * LANES + MARGIN, LANES, [ref[at, :] for ref in own], both)
        above, below = [], []
        for k in range(5):
            last_own = jnp.broadcast_to(own[k][pl.ds(height - 1, 1), :], (TILE, LANES))
            one, two = ghost_rows(swap_one, swap_two, k, last_own)
            above.append(one)
            below.append(two)
        lanes = lane_ids(TILE)
        one, two = swapped_rows(swap_one, swap_two, 5)
        last = jnp.broadcast_to(rho[pl.ds(height + MARGIN - 1, 1), :], (TILE, LANES))
        one = jnp.where(jnp.logical_and(at_top, lanes >= half), 1.0, one)
        two = jnp.where(jnp.logical_and(at_bottom, lanes >= half), last, two)
        place_rows(TILE, TILE, above, one)
        place_rows(height + MARGIN, TILE, below, two)
        for e in (0, n - TILE):
            here = pl.ds(e, TILE)
            for ref in (p, u, w, stiff):
                ref[here, :] = jnp.zeros((TILE, LANES), jnp.float32)
            rho[here, :] = jnp.ones((TILE, LANES), jnp.float32)
        set_coefs(0, n - TILE, None, rho, ax, az, None)

        def edge_coefs(r, k):
            al[pl.ds(r, k), :] = TIME_STEP / rho[pl.ds(r, k), :]

        for_rows(0, n - TILE, edge_coefs)
        at = pl.ds(TILE, TILE)
        az[at, :] = jnp.where(at_top, 0.0, az[at, :])

        found = find_sources(sources, height, wide_place, seen[1] > 0)
        offsets = offsets_of(shifts)
        for t in range(ITERS):
            edge = half - 1 + offsets[t]

            def speeds(r, k):
                here = pl.ds(r, k)
                lanes = lane_ids(k)
                now = p[here, :]
                slope = jnp.where(lanes == edge, al[here, :], ax[here, :])
                slope = jnp.where(lanes > edge, 0.0, slope)
                u[here, :] = u[here, :] - slope * (roll(now, -1) - now)
                slope = jnp.where(lanes > edge, 0.0, az[here, :])
                w[here, :] = w[here, :] - slope * (p[pl.ds(r + 1, k), :] - now)

            def press(r, k):
                here = pl.ds(r, k)
                fast = u[here, :]
                down_ = w[here, :] - w[pl.ds(r - 1, k), :]
                hard = jnp.where(lane_ids(k) > edge, 0.0, stiff[here, :])
                p[here, :] = p[here, :] - hard * ((fast - roll(fast, 1)) + down_)

            for_rows(0, n - TILE, speeds)
            for_rows(TILE, n - TILE, press)
            inject(p, found, wavelet, t)


def rest_kernel(height, more, blocks, *refs):
    stages, done, out = [[ref] for ref in refs[:3]], refs[3], refs[4]
    each = height // blocks

    def read(b, side, r, k):
        if b == 0 and side < 0:
            return [done[f, pl.ds(0, k), :] for f in range(3)]
        if b == blocks - 1 and side > 0:
            return [done[f, pl.ds(MARGIN, k), :] for f in range(3)]
        return finals(stages, pl.ds(r + b * each, k))

    def join(fields):
        lanes = lane_ids(fields[0].shape[0])
        found = jnp.where(lanes < START + 2 * more, roll(fields[1], more), roll(fields[2], 2 * more))
        return jnp.where(lanes < START + more, fields[0], found)

    for side, (low, high) in zip((-1, 0, 1), ((0, MARGIN), (MARGIN, each - MARGIN), (each - MARGIN, each))):

        def beside(r, k, side=side):
            lanes = lane_ids(k)
            found = join(read(0, side, r, k))
            for b in range(1, blocks):
                part = roll(join(read(b, side, r, k)), LANES // blocks * b)
                start = START + LANES // blocks * b
                mine = between(lanes, start, start + 3 * more)
                if start + 3 * more > LANES:
                    mine = jnp.logical_or(lanes >= start, lanes < start + 3 * more - LANES)
                    if start >= LANES:
                        mine = between(lanes, start - LANES, start + 3 * more - LANES)
                found = jnp.where(mine, part, found)
            out[pl.ds(r, k), :] = found

        for_rows(low, high, beside)


def mid_kernel(height, low, *refs):
    shifts, stages, done, wide, near = refs[0], refs[1:4], refs[4], refs[5], refs[6]
    built = refs[-3:]
    _, at_end = range_ends()
    total = offsets_of(shifts)[ITERS]
    turn = LANES - total
    inside = (MARGIN, height - MARGIN)

    @pl.when(jnp.logical_not(at_end))
    def _():
        def build(r, k):
            theirs = between(lane_ids(k), SKEW, total)
            for f in range(3):
                mine = stages[f][pl.ds(r, k), :]
                at, back = r - MARGIN, (NARROW if low else WIDTH) * f
                if low and at >= 3 * each:
                    at, back = f * each, 3 * NARROW
                other = near[pl.ds(at, k), :]
                other = roll(other, -back) if back else other
                built[f][pl.ds(r, k), :] = pltpu.roll(jnp.where(theirs, other, mine), turn, 1)

        each = (inside[1] - inside[0]) // 4
        for start in range(*inside, each):
            build(start, each)

    @pl.when(at_end)
    def _():
        def build(r, k):
            lanes = lane_ids(k)
            inner = jnp.logical_and(lanes >= total, lanes < KEPT + SKEW)
            for f in range(3):
                part = roll(wide[f, pl.ds(r + MARGIN, k), :], LANES // 2)
                if inside[0] <= r < inside[1]:
                    mine = stages[f][pl.ds(r, k), :]
                else:
                    mine = done[f, pl.ds(0 if r < MARGIN else MARGIN, k), :]
                built[f][pl.ds(r, k), :] = pltpu.roll(jnp.where(inner, mine, part), turn, 1)

        build(0, MARGIN)
        build(MARGIN, height - 2 * MARGIN)
        build(height - MARGIN, MARGIN)


def last_kernel(height, more, blocks, *refs):
    far_too = more > 0
    shifts, sources, wavelet, seen = refs[:4]
    refs = refs[1:]
    done, strip, edge = refs[3:6]
    lean = edge.at[pl.ds(2 * MARGIN + TILE, edge.shape[0] - 2 * MARGIN - TILE)]
    drafts = refs[6:9]
    rest = refs[9] if far_too else None
    refs = refs[9 + far_too :]
    outs, built = refs[:3], refs[3:6]
    p, u, w, rho, ax, az, stiff, gp, gu, gw, sems = refs[6:]
    at_top, _ = depth_ends()
    _, at_end = range_ends()
    each = height // BLOCKS
    tiles = each // TILE + 2
    n = (tiles + 2) * TILE
    own_part = STRIP // 2
    total = offsets_of(shifts)[ITERS]
    start = START
    turn = LANES - total

    @pl.when(at_end)
    def _():
        copies = [pltpu.make_async_copy(drafts[f], outs[f], sems.at[f, 0]) for f in range(3)]
        for copy in copies:
            copy.start()
        for copy in copies:
            copy.wait()

    @pl.when(jnp.logical_not(at_end))
    def _():
        lanes = lane_ids(TILE)
        inner = lanes % STRIP
        mine = inner < own_part
        six = edge[pl.ds(2 * MARGIN, TILE), :]
        for i in range(tiles):
            here = pl.ds((i + 1) * TILE, TILE)
            pack = lean[pl.ds(i * TILE, TILE), :]
            group, slot = rho_slot(i, tiles)
            dense = lean[pl.ds((tiles + group) * TILE, TILE), :]
            origin = 4 * BLOCKS * slot + SKEW * (lanes // STRIP) + inner - own_part
            theirs = jnp.take_along_axis(dense, jnp.clip(origin, 0, LANES - 1), 1)
            parts = [roll(pack, own_part - SKEW * g) if g != 2 else pack for g in range(4)]
            parts.append(theirs)
            late = None
            if i < 3:
                late, lane, b = 5 * SKEW * i, own_part, 0
            elif i >= tiles - 3:
                late, lane, b = 5 * SKEW * (i - tiles + 6), STRIP * (BLOCKS - 1) + own_part, BLOCKS - 1
            if late is not None:
                block = between(lanes, STRIP * b, STRIP * (b + 1))
                parts = [
                    jnp.where(block, roll(six, lane - late - SKEW * g), part)
                    for g, part in enumerate(parts)
                ]
            for ref, part in zip((gp, gu, gw), parts):
                ref[here, :] = part
            for a, (ref, part) in enumerate(zip((p, u, w, stiff, rho), parts)):
                ref[here, :] = jnp.where(mine, strip[a, here, :], part)
        for e in (0, n - TILE):
            here = pl.ds(e, TILE)
            for ref in (p, u, w, stiff):
                ref[here, :] = jnp.zeros((TILE, LANES), jnp.float32)
            rho[here, :] = jnp.ones((TILE, LANES), jnp.float32)
        set_coefs(TILE, n - TILE, None, rho, ax, az, None)
        at = pl.ds(TILE, TILE)
        az[at, :] = jnp.where(jnp.logical_and(at_top, lane_ids(TILE) < STRIP), 0.0, az[at, :])

        found = find_sources(sources, height, strip_place, seen[2] > 0)
        for t in range(ITERS):
            taken = own_part + t

            def speeds(r, k):
                here = pl.ds(r, k)
                inner = lane_ids(k) % STRIP
                now = p[here, :]
                fast = u[here, :] - ax[here, :] * (roll(now, -1) - now)
                u[here, :] = jnp.where(inner == taken, gu[here, :], fast)
                deep = w[here, :] - az[here, :] * (p[pl.ds(r + 1, k), :] - now)
                w[here, :] = jnp.where(inner == taken, gw[here, :], deep)

            def press(r, k):
                here = pl.ds(r, k)
                inner = lane_ids(k) % STRIP
                fast = u[here, :]
                down_ = w[here, :] - w[pl.ds(r - 1, k), :]
                new = p[here, :] - stiff[here, :] * ((fast - roll(fast, 1)) + down_)
                if t < ITERS - 1:
                    new = jnp.where(inner == taken + 1, gp[here, :], new)
                p[here, :] = new

            for_rows(TILE, n - TILE, speeds)
            for_rows(TILE, n - TILE, press)
            inject(p, found, wavelet, t, taken)

        copies = []
        for b in range(BLOCKS):
            first = b * each
            low, high = first, first + each
            edges = []
            if b == 0:
                low = MARGIN
                edges = [(0, 0)]
            if b == BLOCKS - 1:
                high = height - MARGIN
                edges = [(high, MARGIN)]

            def far_values(row, k):
                b = row // (height // blocks)
                found = rest[pl.ds(row - b * (height // blocks), k), :]
                return roll(found, -LANES // blocks * b) if b else found

            for row, side in edges:
                here, there = pl.ds(row, MARGIN), pl.ds(side, MARGIN)
                lanes = lane_ids(MARGIN)
                for f, ref in enumerate((p, u, w)):
                    part = roll(ref[pl.ds(row - first + 2 * TILE, MARGIN), :], KEPT - STRIP * b)
                    kept = jnp.where(between(lanes, SKEW, KEPT + SKEW), done[f, there, :], part)
                    other = edge[there, :]
                    other = roll(other, -WIDTH * f) if f else other
                    if far_too:
                        far = far_values(row, MARGIN)
                        far = roll(far, -more * f) if f else far
                        other = jnp.where(lanes < start, other, far)
                    kept = jnp.where(between(lanes, SKEW, total), other, kept)
                    built[f][here, :] = pltpu.roll(kept, turn, 1)
            here, k = pl.ds(low, high - low), high - low
            natural = (lane_ids(k) + total) % LANES
            ready = between(natural, SKEW, KEPT + SKEW)
            shift = (KEPT - STRIP * b + LANES + turn) % LANES
            for f, ref in enumerate((p, u, w)):
                part = pltpu.roll(ref[pl.ds(low - first + 2 * TILE, k), :], shift, 1)
                kept = jnp.where(ready, drafts[f][here, :], part)
                if far_too:
                    far = pltpu.roll(far_values(low, k), (turn + LANES - more * f) % LANES, 1)
                    kept = jnp.where(between(natural, start, total), far, kept)
                built[f][here, :] = kept
            for f in range(3):
                at = pl.ds(first, each)
                copy = pltpu.make_async_copy(built[f].at[at, :], outs[f].at[at, :], sems.at[f, b])
                copy.start()
                copies.append(copy)
        for copy in copies:
            copy.wait()


def moved(x):
    return lax.ppermute(x, "range", [(i + 1, i) for i in range(lax.axis_size("range") - 1)])


def swapped(x, first):
    pairs = [(i, i + 1) for i in range(first, lax.axis_size("depth") - 1, 2)]
    return lax.ppermute(x, "depth", pairs + [(j, i) for i, j in pairs])


LOCAL = pl.BlockSpec(memory_space=pltpu.VMEM)
REMOTE = pl.BlockSpec(memory_space=pl.ANY)
SCALAR = pl.BlockSpec(memory_space=pltpu.SMEM)


def shaped(shape, space):
    if space is SCALAR:
        return pltpu.SMEM(*shape)
    if space is LOCAL:
        return pltpu.VMEM(shape, jnp.float32)
    return jax.ShapeDtypeStruct(shape, jnp.float32)


def call(kernel, ins, outs, scratch=()):
    values, specs = [], []
    for value, space in ins:
        if space is LOCAL:
            value = pltpu.with_memory_space_constraint(value, pltpu.VMEM)
        elif space is SCALAR:
            value = pltpu.with_memory_space_constraint(value, pltpu.SMEM)
        elif space is REMOTE:
            value = pltpu.with_memory_space_constraint(value, pltpu.HBM)
        values.append(value)
        specs.append(space)
    return pl.pallas_call(
        kernel,
        in_specs=specs,
        out_specs=[space for _, space in outs],
        out_shape=[shaped(*pair) for pair in outs],
        scratch_shapes=list(scratch),
        compiler_params=pltpu.CompilerParams(vmem_limit_bytes=8 * 1024 * 1024),
    )(*values)


def room(*shape):
    return pltpu.VMEM(shape, jnp.float32)


def shards(
    pressure,
    vel_range,
    vel_depth,
    sound_speed,
    density,
    ahead_speed,
    ahead_density,
    shifts,
    sources,
    wavelet,
):
    height, breadth = pressure.shape
    extra = ahead_speed.shape[1]
    assert breadth == LANES and 2 * extra == LANES and height % 512 == 0
    assert START + MORE[-1][1] == extra
    arrays = [(x, REMOTE) for x in (pressure, vel_range, vel_depth, sound_speed, density)]
    ahead = [(x.T, REMOTE) for x in (ahead_speed, ahead_density)]
    small = [(shifts, REMOTE), (sources.T, REMOTE), (wavelet.T, REMOTE)]
    sizes = (shifts.shape, sources.shape[::-1], wavelet.shape[::-1])
    kinds = (jnp.int32, jnp.int32, jnp.float32)
    scalars = [(pair, SCALAR) for pair in zip(sizes, kinds)]
    field = (height, LANES)
    dma = pltpu.SemaphoreType.DMA

    found = call(
        functools.partial(own_kernel, height),
        small + arrays + ahead,
        [((6 * TILE, LANES), LOCAL)] * 2
        + [(field, LOCAL)] * 5
        + [((ITERS - 1, *field), LOCAL)] * 3
        + [(field, LOCAL)] * 3
        + scalars
        + [(((3,), jnp.int32), SCALAR), (((1,), jnp.int32), SCALAR)],
        [room(*field)] * 3 + [room(2, LANES, LANES), dma((5,)), dma((2, 2)), dma((3,))],
    )
    tiles = height // BLOCKS // TILE + 2
    lean_rows = (tiles + (tiles - 2) // 4 + 1) * TILE
    n_edge = 6 * MARGIN
    n_wide = height + 2 * MARGIN
    n_strip = (tiles + 2) * TILE

    def finish(kind, ahead, swap_one, swap_two, *found):
        _, more, blocks = MORE[kind]
        ahead = [(x, REMOTE) for x in ahead]
        own = [(x, LOCAL) for x in found[:5]]
        stages = [(x, LOCAL) for x in found[5:11]]
        last = stages[3:]
        small = [(x, SCALAR) for x in found[11:]]
        (plane,) = call(
            functools.partial(pack_kernel, height, kind == 0),
            last,
            [(((4 if kind else 3) * (height - 2 * MARGIN) // 4, LANES), LOCAL)],
        )
        near = [(moved(plane), LOCAL)]
        sides = [(swapped(swap_one, 0), LOCAL), (swapped(swap_two, 1), LOCAL)]
        (lean,) = call(
            functools.partial(lean_kernel, height), own + stages, [((lean_rows, LANES), LOCAL)]
        )
        edge, done = call(
            functools.partial(edge_kernel, height),
            small + own + sides + [(lean, LOCAL)],
            [((2 * MARGIN + TILE + lean_rows, LANES), LOCAL), ((3, 2 * MARGIN, LANES), LOCAL)],
            [room(n_edge, LANES)] * 3
            + [room(ITERS - 1, n_edge, LANES)] * 3
            + [room(n_edge, LANES)] * 8,
        )
        edge_near = moved(edge)
        received = []
        if more:
            (rest,) = call(
                functools.partial(rest_kernel, height, more, blocks),
                last + [(done, LOCAL)],
                [((height // blocks, LANES), LOCAL)],
            )
            received = [(moved(rest), LOCAL)]
        strip, wide = call(
            functools.partial(wide_kernel, height),
            small + own + ahead + sides,
            [((5, n_strip, LANES), LOCAL), ((3, n_wide, LANES), LOCAL)],
            [room(n_wide, LANES)] * 5 + [room(2, extra, height), dma((2,))],
        )
        drafts = call(
            functools.partial(mid_kernel, height, kind == 0),
            small[:1] + last + [(done, LOCAL), (wide, LOCAL)] + near,
            [(field, LOCAL)] * 3,
        )
        mixed = [(x, LOCAL) for x in (done, strip, edge_near, *drafts)]
        return tuple(
            call(
                functools.partial(last_kernel, height, more, blocks),
                small + mixed + received,
                [(field, REMOTE)] * 3,
                [room(*field)] * 3 + [room(n_strip, LANES)] * 10 + [dma((3, BLOCKS))],
            )
        )

    return lax.switch(
        found[-1].reshape(()),
        [functools.partial(finish, kind) for kind in range(len(MORE))],
        [x for x, _ in ahead],
        *found[:-1],
    )


def solution(mesh):
    field = P("depth", "range")
    strip = P("depth", None)
    return jax.shard_map(
        shards,
        mesh=mesh,
        in_specs=(field,) * 5 + (strip,) * 2 + (P(),) * 3,
        out_specs=(field,) * 3,
        check_vma=False,
    )
```
